128 devices in a mesh: dp: 2 (over core), cp: 64 (over z, y, x).
Axes of the slice: x: 4, y: 4, z: 4, core: 2. Of those that a mesh axis runs over, the one named last changes fastest.
Arguments:
- inputs: bfloat16 [8, 16384, 322], P('dp', 'cp')
- latents: float32 [2048, 512], replicated
- x_gain: float32 [322], replicated
- x_shift: float32 [322], replicated
- z_gain: float32 [512], replicated
- z_shift: float32 [512], replicated
- w_query: bfloat16 [512, 512], replicated
- w_key: bfloat16 [322, 512], replicated
- w_value: bfloat16 [322, 512], replicated
- w_out: bfloat16 [512, 512], replicated
- m_gain: float32 [512], replicated
- m_shift: float32 [512], replicated
- w_up: bfloat16 [512, 512], replicated
- b_up: float32 [512], replicated
- w_down: bfloat16 [512, 512], replicated
- b_down: float32 [512], replicated
- d_out: bfloat16 [8, 2048, 512], P('dp')
Outputs:
- output 1: float32 [8, 2048, 512], P('dp')
- output 2: bfloat16 [8, 16384, 322], P('dp', 'cp')
- output 3: float32 [2048, 512], replicated
- output 4: float32 [322], replicated
- output 5: float32 [322], replicated
- output 6: float32 [512], replicated
- output 7: float32 [512], replicated
- output 8: float32 [512, 512], replicated
- output 9: float32 [322, 512], replicated
- output 10: float32 [322, 512], replicated
- output 11: float32 [512, 512], replicated
- output 12: float32 [512], replicated
- output 13: float32 [512], replicated
- output 14: float32 [512, 512], replicated
- output 15: float32 [512], replicated
- output 16: float32 [512, 512], replicated
- output 17: float32 [512], replicated
All inputs are finite; a program needn't handle non-finite values.
Results may differ from the reference program's by a relative error of at most 0.0176396.
Values sent between devices are 32-bit elements.
A program may use at most 1 GiB of HBM per device.

```python
import math
import jax
import jax.numpy as jnp
from jax import lax

BATCH = 8
INPUTS = 16384
IN_CH = 322
LATENTS = 2048
WIDTH = 512
QK_CH = 512
V_CH = 512
LN_EPS = 1e-5


def layer_norm(tensor, ln_gain, ln_shift):
    row_mean = jnp.mean(tensor, axis=-1, keepdims=True)
    centred = tensor - row_mean
    variance = jnp.mean(centred * centred, axis=-1, keepdims=True)
    return centred * lax.rsqrt(variance + LN_EPS) * ln_gain + ln_shift


def lowered(tensor):
    return tensor.astype(jnp.bfloat16).astype(jnp.float32)


def setup_inputs(seed: int = 0) -> dict:
    rng_keys = jax.random.split(jax.random.key(seed), 17)
    spread = 0.85 * math.sqrt(math.log(INPUTS / 16.0))

    def normal(key_index, dims_of, factor):
        return jax.random.normal(rng_keys[key_index], dims_of, jnp.float32) * factor

    return {
        'inputs': normal(0, (BATCH, INPUTS, IN_CH), 1.0).astype(jnp.bfloat16),
        'latents': normal(1, (LATENTS, WIDTH), 0.5),
        'x_gain': 1.0 + normal(2, (IN_CH,), 0.3),
        'x_shift': normal(3, (IN_CH,), 0.3),
        'z_gain': spread * (1.0 + normal(4, (WIDTH,), 0.2)),
        'z_shift': normal(5, (WIDTH,), 0.3 * spread),
        'w_query': normal(6, (WIDTH, QK_CH), WIDTH ** -0.5).astype(jnp.bfloat16),
        'w_key': normal(7, (IN_CH, QK_CH), IN_CH ** -0.5).astype(jnp.bfloat16),
        'w_value': normal(8, (IN_CH, V_CH), IN_CH ** -0.5).astype(jnp.bfloat16),
        'w_out': normal(9, (V_CH, WIDTH), 2.0 * V_CH ** -0.5).astype(jnp.bfloat16),
        'm_gain': 1.0 + normal(10, (WIDTH,), 0.2),
        'm_shift': normal(11, (WIDTH,), 0.2),
        'w_up': normal(12, (WIDTH, WIDTH), WIDTH ** -0.5).astype(jnp.bfloat16),
        'b_up': normal(13, (WIDTH,), 0.3),
        'w_down': normal(14, (WIDTH, WIDTH), WIDTH ** -0.5).astype(jnp.bfloat16),
        'b_down': normal(15, (WIDTH,), 0.3),
        'd_out': normal(16, (BATCH, LATENTS, WIDTH), 1.0).astype(jnp.bfloat16),
    }


def forward(inputs, latents, x_gain, x_shift, z_gain, z_shift, w_query, w_key, w_value, w_out, m_gain, m_shift, w_up, b_up, w_down, b_down):
    qk_scale = QK_CH ** -0.5
    z_norm = lowered(layer_norm(latents, z_gain, z_shift))
    queries = lowered(jnp.dot(z_norm, w_query, preferred_element_type=jnp.float32))

    def attend(x_rows):
        x_norm = lowered(layer_norm(x_rows.astype(jnp.float32), x_gain, x_shift))
        key_rows = lowered(jnp.dot(x_norm, w_key, preferred_element_type=jnp.float32))
        value_rows = lowered(jnp.dot(x_norm, w_value, preferred_element_type=jnp.float32))
        logits = jnp.dot(queries, key_rows.T, preferred_element_type=jnp.float32) * qk_scale
        attn_probs = lowered(jax.nn.softmax(logits, axis=-1))
        return lowered(jnp.dot(attn_probs, value_rows, preferred_element_type=jnp.float32))

    attn_out = lax.map(jax.checkpoint(attend), inputs)
    z_mid = latents + jnp.einsum('bnv,vd->bnd', attn_out, w_out)
    hidden = lowered(layer_norm(z_mid, m_gain, m_shift))
    pre_act = jnp.einsum('bnd,de->bne', hidden, w_up) + b_up
    act_val = lowered(jax.nn.gelu(pre_act))
    return z_mid + jnp.einsum('bne,ed->bnd', act_val, w_down) + b_down


def reference(inputs, latents, x_gain, x_shift, z_gain, z_shift, w_query, w_key, w_value, w_out, m_gain, m_shift, w_up, b_up, w_down, b_down, d_out):
    out_latents, pullback = jax.vjp(
        forward, inputs, latents, x_gain, x_shift, z_gain, z_shift,
        w_query.astype(jnp.float32), w_key.astype(jnp.float32), w_value.astype(jnp.float32), w_out.astype(jnp.float32),
        m_gain, m_shift, w_up.astype(jnp.float32), b_up, w_down.astype(jnp.float32), b_down)
    (d_inputs, d_latents, d_x_gain, d_x_shift, d_z_gain, d_z_shift, d_w_query, d_w_key, d_w_value, d_w_out,
     d_m_gain, d_m_shift, d_w_up, d_b_up, d_w_down, d_b_down) = pullback(d_out.astype(jnp.float32))
    return (out_latents, d_inputs, d_latents, d_x_gain, d_x_shift, d_z_gain, d_z_shift, d_w_query, d_w_key, d_w_value, d_w_out,
            d_m_gain, d_m_shift, d_w_up, d_b_up, d_w_down, d_b_down)
```

```python
import functools
import math

import jax
import jax.numpy as jnp
from jax import lax
from jax.experimental import pallas as pl
from jax.experimental.pallas import tpu as pltpu
from jax.sharding import PartitionSpec as P

LN_EPS = 1e-5
BF16 = jnp.bfloat16
F32 = jnp.float32
MESH_ID = pl.DeviceIdType.MESH
SIDE = 4
PLANE = SIDE * SIDE
LANES = 128
LATENT_TILE = 256
LOG2E = math.log2(math.e)
GELU_C = math.sqrt(2.0 / math.pi)
GELU_A = 0.044715
HALF_TILES = 20
STREAM_TILES = ((0, 7), (7, 14), (14, 20))
STREAM_ROWS = ((0, 32), (32, 80), (80, 128))
VMEM_LIMIT = 67043328
STREAM_AXES = ((2, 1, 0), (1, 0, 2), (0, 2, 1))


def contract(form, lhs, rhs):
    return jnp.einsum(form, lhs, rhs, preferred_element_type=F32)


def dot(lhs, rhs, dims):
    return lax.dot_general(lhs, rhs, (dims, ((), ())), preferred_element_type=F32)


NN = ((1,), (0,))
NT = ((1,), (1,))
TN = ((0,), (0,))
DOWN, ACROSS = 0, 1
HOPS = (2, 1, 3)


def mean(value, axis=ACROSS):
    return jnp.mean(value, axis=axis, keepdims=True)


def total(value, axis=DOWN):
    return jnp.sum(value, axis=axis, keepdims=True)


def zeros(*shape):
    return jnp.zeros(shape, F32)


def lanes(t):
    return pl.ds(t * LANES, LANES)


def tile_rows(i, size):
    return pl.ds(pl.multiple_of(i * size, size), size)


def norm_parts(value, axis=ACROSS):
    centred = value - mean(value, axis)
    rstd = lax.rsqrt(mean(centred * centred, axis) + LN_EPS)
    return centred * rstd, rstd


def norm_pull(d_normed, unit, rstd, gain, axis=ACROSS):
    d_unit = d_normed * gain
    return rstd * (d_unit - mean(d_unit, axis) - unit * mean(d_unit * unit, axis))


def row_pair(ref, i):
    return jnp.concatenate([ref[pl.ds(2 * i, 1), :], ref[pl.ds(2 * i + 1, 1), :]], axis=ACROSS)


def sum_slots(ref, *index):
    return ref[(0,) + index] + ref[(1,) + index] + ref[(2,) + index]


def gelu_parts(pre):
    tanh = jnp.tanh(GELU_C * (pre + GELU_A * pre * pre * pre))
    slope = 0.5 * (1.0 + tanh) + 0.5 * pre * (1.0 - tanh * tanh) * (GELU_C * (1.0 + 3.0 * GELU_A * pre * pre))
    return 0.5 * pre * (1.0 + tanh), slope


def chip_coords():
    cp = lax.axis_index('cp')
    return lax.div(cp, PLANE), lax.rem(lax.div(cp, SIDE), SIDE), lax.rem(cp, SIDE)


def chip(z, y, x):
    return {'cp': z * PLANE + y * SIDE + x}


def moved(coords, axis, offset):
    shifted = list(coords)
    shifted[axis] = lax.rem(coords[axis] + offset + SIDE, SIDE)
    return tuple(shifted)


def enter(peers):
    barrier = pltpu.get_barrier_semaphore()
    for peer in peers:
        pl.semaphore_signal(barrier, inc=1, device_id=peer, device_id_type=MESH_ID)
    pl.semaphore_wait(barrier, len(peers))


class Copies:
    def __init__(self, send_sems, recv_sems):
        self.send_sems, self.recv_sems, self.used, self.open = send_sems, recv_sems, 0, []

    def start(self, src, dst, peer):
        copy = pltpu.make_async_remote_copy(
            src_ref=src, dst_ref=dst, send_sem=self.send_sems.at[self.used], recv_sem=self.recv_sems.at[self.used],
            device_id=peer, device_id_type=MESH_ID)
        self.used += 1
        copy.start()
        self.open.append(copy)
        return copy

    def sent(self, copy):
        copy.wait_send()
        self.open = [other for other in self.open if other is not copy]

    def finish(self):
        for copy in self.open:
            copy.wait_send()


def forward_kernel(
        x_blocks, latents, x_gain, x_shift, z_gain, z_shift, w_query, w_key, w_value,
        z0, d_out, w_out, w_up, w_down, m_gain, m_shift, b_up, b_down,
        q, k, v, x_in, z_out, d_attn_all, stats_all, top_all, d_mid_out, w_grads, vec_grads,
        vt, logits, mixed, top_own, tops, sum_own, sum_parts, sums, ra1, rb1, pa1, pb1, ra2, rb2, d_attn_f32, stats_f32,
        send_sems, recv_sems):
    me = chip_coords()
    z, y, x = me
    owner = y * SIDE + x
    plane_peers = []
    for d in range(1, PLANE):
        other = lax.rem(owner + d, PLANE)
        plane_peers.append((other, chip(z, lax.div(other, SIDE), lax.rem(other, SIDE))))
    enter([device for _, device in plane_peers] + [chip(*moved(me, 0, d)) for d in HOPS])
    copies = Copies(send_sems, recv_sems)
    qk_scale = q.shape[1] ** -0.5
    to_log2 = qk_scale * LOG2E
    tiles = q.shape[0] // LATENT_TILE
    half_v = vt.shape[0] // 2
    block_rows = x_blocks.shape[-1]

    got_x = {}
    for d in HOPS:
        peer = moved(me, 0, d)
        got_x[d] = copies.start(x_blocks.at[peer[0]], x_in.at[z], chip(*peer))
    x_in[z] = x_blocks[z]
    top_own[...] = jnp.full(top_own.shape, -jnp.inf, F32)

    def query_tile(i, carry):
        rows = tile_rows(i, LATENT_TILE)
        unit, _ = norm_parts(latents[rows, :])
        z_norm = (unit * z_gain[...] + z_shift[...]).astype(BF16)
        q[rows, :] = dot(z_norm, w_query[...], NN).astype(BF16)
        return carry

    lax.fori_loop(0, tiles, query_tile, 0)

    def block_logits(j):
        rows = tile_rows(j, block_rows)
        unit, _ = norm_parts(x_in[j], DOWN)
        x_norm = (unit * x_gain[...] + x_shift[...]).astype(BF16)
        k[rows, :] = dot(x_norm, w_key[...], TN).astype(BF16)
        v[rows, :] = dot(x_norm, w_value[...], TN).astype(BF16)
        vt[:, rows] = dot(w_value[...], x_norm, TN).astype(BF16)

        def logits_tile(i, carry):
            s = dot(k[rows, :], q[tile_rows(i, LATENT_TILE), :], NT)
            logits[i, rows, :] = s
            top = jnp.max(s, axis=DOWN, keepdims=True)
            for h in range(2):
                row = pl.ds(2 * i + h, 1)
                top_own[row, :] = jnp.maximum(top_own[row, :], top[:, h * LANES:(h + 1) * LANES])
            return carry

        lax.fori_loop(0, tiles, logits_tile, 0)

    block_logits(z)
    for d in HOPS[::-1]:
        got_x[d].wait_recv()
        block_logits(moved(me, 0, -d)[0])
    top_own[...] = jnp.ceil(top_own[...] * to_log2)
    tops[owner] = top_own[...]
    top_copies = [copies.start(top_own, tops.at[owner], device) for _, device in plane_peers]

    def mix_tile(i, carry):
        top = row_pair(top_own, i)
        w = jnp.exp2(logits[i] * to_log2 - top)
        weight_sum = total(w)
        for h in range(2):
            sum_own[pl.ds(2 * i + h, 1), :] = weight_sum[:, h * LANES:(h + 1) * LANES]
        product = dot(vt[...], w.astype(BF16), NN)
        at_y, at_x = lax.div(i, 2), 2 * lax.rem(i, 2)
        for h in range(2):
            mixed[at_y, at_x + h] = product[:, h * LANES:(h + 1) * LANES]
        return carry

    lax.fori_loop(0, tiles, mix_tile, 0)
    for copy in top_copies:
        copy.wait_recv()
    top = functools.reduce(jnp.maximum, [tops[i] for i in range(PLANE)])
    top_all[...] = top
    factor = jnp.exp2(top_own[...] - top)
    scaled_sum = sum_own[...] * factor
    for i in range(PLANE):
        mixed[i // SIDE, i % SIDE] = mixed[i // SIDE, i % SIDE] * factor[i:i + 1, :]
        sum_parts[i] = jnp.broadcast_to(scaled_sum[i:i + 1, :], (8, LANES))

    first = [[], []]
    for d in HOPS:
        peer = moved(me, 2, d)
        first[0].append(copies.start(mixed.at[:, peer[2], 0:half_v, :], ra1.at[d - 1], chip(*peer)))
        peer = moved(me, 1, d)
        first[1].append(copies.start(mixed.at[peer[1], :, half_v:2 * half_v, :], rb1.at[d - 1], chip(*peer)))
    sums[owner] = sum_parts[owner]
    sum_copies = [copies.start(sum_parts.at[other], sums.at[owner], device) for other, device in plane_peers]
    for copy in first[0]:
        copy.wait_recv()
    second = [[], []]
    for i in range(SIDE):
        pa1[i] = mixed[i, x, 0:half_v, :] + sum_slots(ra1, i)
    for d in HOPS:
        peer = moved(me, 1, d)
        second[0].append(copies.start(pa1.at[peer[1]], ra2.at[d - 1], chip(*peer)))
    for copy in first[1]:
        copy.wait_recv()
    for i in range(SIDE):
        pb1[i] = mixed[y, i, half_v:2 * half_v, :] + sum_slots(rb1, i)
    for d in HOPS:
        peer = moved(me, 2, d)
        second[1].append(copies.start(pb1.at[peer[2]], rb2.at[d - 1], chip(*peer)))
    for copy in sum_copies:
        copy.wait_recv()
    inv_sum = 1.0 / functools.reduce(lambda a, b: a + b, [sums[i] for i in range(PLANE)])
    for copy in second[0] + second[1]:
        copy.wait_recv()
    upper = pa1[y] + sum_slots(ra2)
    lower = pb1[x] + sum_slots(rb2)
    attn_t = jnp.concatenate([upper, lower], axis=DOWN) * inv_sum[0:1, :]

    attn_t_low = attn_t.astype(BF16)
    attn_low = attn_t.T.astype(BF16)
    z_mid = z0[...] + dot(attn_low, w_out[...], NN)
    unit, rstd = norm_parts(z_mid)
    hidden_f32 = unit * m_gain[...] + m_shift[...]
    hidden = hidden_f32.astype(BF16)
    pre = dot(hidden, w_up[...], NN) + b_up[...]
    act_f32, slope = gelu_parts(pre)
    act = act_f32.astype(BF16)
    z_out[...] = z_mid + dot(act, w_down[...], NN) + b_down[...]

    d_out_low = d_out[...]
    d_out_f32 = d_out_low.astype(F32)
    d_act = dot(d_out_low, w_down[...], NT).astype(BF16).astype(F32)
    d_pre = d_act * slope
    d_pre_low = d_pre.astype(BF16)
    d_hidden = dot(d_pre_low, w_up[...], NT).astype(BF16).astype(F32)
    d_mid = d_out_f32 + norm_pull(d_hidden, unit, rstd, m_gain[...])
    d_mid_low = d_mid.astype(BF16)
    d_attn = dot(d_mid_low, w_out[...], NT).astype(BF16).astype(F32)
    row_dot = total(d_attn.T * attn_t)

    half_r = LANES // 2
    d_attn_f32[y, x] = d_attn
    stats_f32[owner, 0:1, :] = row_dot
    stats_f32[owner, 1:2, :] = inv_sum[0:1, :]
    up, down = pl.ds(0, half_r), pl.ds(half_r, half_r)
    first = [[], []]
    for d in HOPS:
        first[0].append(copies.start(d_attn_f32.at[y, x, up], d_attn_f32.at[y, x, up], chip(*moved(me, 1, d))))
        first[1].append(copies.start(d_attn_f32.at[y, x, down], d_attn_f32.at[y, x, down], chip(*moved(me, 2, d))))
    stat_copies = [copies.start(stats_f32.at[owner], stats_f32.at[owner], device) for _, device in plane_peers]

    d_mid_out[...] = d_mid
    w_grads[0] = dot(attn_t_low, d_mid_low, NN)
    w_grads[1] = dot(hidden_f32.T.astype(BF16), d_pre_low, NN)
    w_grads[2] = dot(act_f32.T.astype(BF16), d_out_low, NN)
    for i, value in enumerate((d_hidden * unit, d_hidden, d_pre, d_out_f32)):
        vec_grads[i:i + 1, :] = total(value)
    vec_grads[4:8, :] = zeros(4, vec_grads.shape[1])

    second = []
    for copy in first[0]:
        copy.wait_recv()
    for d in HOPS:
        second.append(copies.start(d_attn_f32.at[:, x, up], d_attn_f32.at[:, x, up], chip(*moved(me, 2, d))))
    for copy in first[1]:
        copy.wait_recv()
    for d in HOPS:
        second.append(copies.start(d_attn_f32.at[y, :, down], d_attn_f32.at[y, :, down], chip(*moved(me, 1, d))))
    for copy in stat_copies + second:
        copy.wait_recv()
    copies.finish()
    stats_all[...] = stats_f32[...]
    for i in range(PLANE):
        d_attn_all[i] = d_attn_f32[i // SIDE, i % SIDE].astype(BF16)


def forward_block(x_blocks, latents, *others, collective_id):
    latents_n, width = latents.shape
    _, channels, block_rows = x_blocks.shape
    elements = SIDE * block_rows
    chunk = latents_n // PLANE
    half = width // 2
    vmem = pl.BlockSpec(memory_space=pltpu.VMEM)
    n_copies = 3 * PLANE + 24
    shape, wide = jax.ShapeDtypeStruct, pltpu.VMEM
    stat, slots = (PLANE, 8, LANES), (3, SIDE, half, LANES)
    return pl.pallas_call(
        forward_kernel,
        out_shape=(
            shape((latents_n, width), BF16), shape((elements, width), BF16), shape((elements, width), BF16),
            shape(x_blocks.shape, F32), shape((chunk, width), F32), shape((PLANE, chunk, width), BF16),
            shape(stat, F32), shape((PLANE, LANES), F32), shape((chunk, width), F32), shape((3, width, width), F32),
            shape((8, width), F32)),
        in_specs=[vmem] * (2 + len(others)),
        out_specs=(vmem,) * 11,
        scratch_shapes=[
            wide((width, elements), BF16), wide((latents_n // LATENT_TILE, elements, LATENT_TILE), F32),
            wide((SIDE, SIDE, width, LANES), F32),
            wide((PLANE, LANES), F32), wide((PLANE, PLANE, LANES), F32), wide((PLANE, LANES), F32), wide(stat, F32), wide(stat, F32),
            wide(slots, F32), wide(slots, F32), wide(slots[1:], F32), wide(slots[1:], F32),
            wide((3, half, LANES), F32), wide((3, half, LANES), F32),
            wide((SIDE, SIDE, chunk, width), F32), wide(stat, F32),
            pltpu.SemaphoreType.DMA((n_copies,)), pltpu.SemaphoreType.DMA((n_copies,))],
        compiler_params=pltpu.CompilerParams(
            collective_id=collective_id, has_side_effects=True, vmem_limit_bytes=VMEM_LIMIT),
    )(x_blocks, latents, *others)


def at(free, coords, **other):
    index = []
    for axis, name in enumerate('zyx'):
        index.append(other[name] if name in other else (slice(None) if axis in free else coords[axis]))
    return tuple(index)


def on(axis, value):
    return {'zyx'[axis]: value}


def tile_place(t):
    return t // HALF_TILES, t % HALF_TILES


def backward_kernel(
        q, k, v, d_attn, stats, top, z_rows, d_mid, vec_grads, x_gain, x_shift, z_gain, z_shift, w_query, w_key, w_value,
        w_grads, x_in, latents_in,
        z_all, d_inputs, d_lat_out, w_out_grads, kv_out, vec_out,
        probs, d_logits, d_q, d_k, d_v, x_rows, x_norm, x_sums, d_x, d_x_in, latents, z_norm, vecs, g, core_in, *rest):
    n, per = len(STREAM_TILES), 8
    side_in = [rest[per * s:per * s + 2] for s in range(n)]
    full_in = [rest[per * s + 2:per * s + 4] for s in range(n)]
    recvs = [(None,) + rest[per * s + 4:per * s + 6] for s in range(n)]
    parts = [rest[per * s + 6:per * s + 8] for s in range(n)]
    send_sems, recv_sems, local_sems, half_free = rest[per * n:]
    me = chip_coords()
    z, y, x = me
    dp = lax.axis_index('dp')
    partner = {'dp': 1 - dp}
    qk_scale = q.shape[1] ** -0.5
    to_log2 = qk_scale * LOG2E
    width = q.shape[1]
    channels = x_rows.shape[1]
    halves = (slice(0, SIDE // 2), slice(SIDE // 2, SIDE))
    tiles = q.shape[0] // LATENT_TILE
    split = width // LANES
    chips = SIDE ** 3

    local = []

    def fetch(src, dst):
        copy = pltpu.make_async_copy(src, dst, local_sems.at[len(local)])
        copy.start()
        local.append(copy)
        return copy

    enter([partner] + [chip(*moved(me, axis, d)) for axis in range(3) for d in HOPS])
    copies = Copies(send_sems, recv_sems)

    own_z = fetch(z_rows, z_all.at[z, y, x])
    z_pending = []
    for s, (lo, hi) in enumerate(STREAM_ROWS):
        rows = pl.ds(lo, hi - lo)
        z_pending.append([
            copies.start(z_rows.at[rows], z_all.at[z, y, x, rows], chip(*moved(me, STREAM_AXES[s][0], d))) for d in HOPS])
    got_x = fetch(x_in, x_rows)
    got_latents = fetch(latents_in, latents)
    got_w = []
    for i in range(3):
        for t in range(split):
            half, slot = tile_place(20 + split * i + t)
            got_w.append(fetch(w_grads.at[i, :, :, :, :, lanes(t)], g.at[half, :, :, :, slot]))
    x_norm[...] = jnp.zeros(x_norm.shape, BF16)

    def pair(ref, i, row):
        return jnp.concatenate([ref[2 * i + h, row:row + 1, :] for h in range(2)], axis=ACROSS)

    def attend_tile(i, carry):
        rows = tile_rows(i, LATENT_TILE)
        peak = row_pair(top, i)
        row_dot, inv_sum = pair(stats, i, 0), pair(stats, i, 1)
        p = jnp.exp2(dot(k[...], q[rows, :], NT) * to_log2 - peak) * inv_sum
        probs[:, rows] = p.astype(BF16)
        d_p = dot(v[...], d_attn[rows, :], NT)
        d_s = (p * (d_p - row_dot) * qk_scale).astype(BF16)
        d_logits[:, rows] = d_s
        d_q[rows, :] = dot(d_s, k[...], TN).astype(BF16)
        return carry

    lax.fori_loop(0, tiles // 2, attend_tile, 0)
    own_z.wait()
    for s, (lo, hi) in enumerate(STREAM_ROWS):
        for copy in z_pending[s]:
            copy.wait_recv()
        first, second, _ = STREAM_AXES[s]
        ref = z_all.at[at((first,), me) + (pl.ds(lo, hi - lo),)]
        z_pending[s] = [copies.start(ref, ref, chip(*moved(me, second, d))) for d in (1, -1)]
    lax.fori_loop(tiles // 2, tiles, attend_tile, 0)

    for s, (lo, hi) in enumerate(STREAM_ROWS):
        first, second, _ = STREAM_AXES[s]
        arrived, z_pending[s] = z_pending[s], []
        for copy, d, part in zip(arrived, (1, -1), halves):
            copy.wait_recv()
            origin = on(second, moved(me, second, -d)[second])
            ref = z_all.at[at((), me, **on(first, part), **origin) + (pl.ds(lo, hi - lo),)]
            z_pending[s].append(copies.start(ref, ref, chip(*moved(me, second, d))))

    vecs[...] = zeros(*vecs.shape)
    x_sums[...] = zeros(*x_sums.shape)
    got_x.wait()

    def element_tile(i, carry):
        rows = tile_rows(i, x_rows.shape[-1])
        d_v_low = dot(probs[rows, :], d_attn[...], NN).astype(BF16)
        d_k_low = dot(d_logits[rows, :], q[...], NN).astype(BF16)
        d_v[rows, :] = d_v_low
        d_k[rows, :] = d_k_low
        unit, rstd = norm_parts(x_rows[i], DOWN)
        x_norm[0:channels, rows] = (unit * x_gain[...] + x_shift[...]).astype(BF16)
        d_normed = (dot(w_key[...], d_k_low, NT) + dot(w_value[...], d_v_low, NT)).astype(BF16).astype(F32)
        d_x[i] = norm_pull(d_normed, unit, rstd, x_gain[...], DOWN)
        for h, value in enumerate((d_normed * unit, d_normed)):
            x_sums[h] += sum(value[:, t * LANES:(t + 1) * LANES] for t in range(value.shape[1] // LANES))
        return carry

    lax.fori_loop(0, SIDE, element_tile, 0)
    x_pending = []
    for d in HOPS:
        peer = moved(me, 0, d)
        x_pending.append(copies.start(d_x.at[peer[0]], d_x_in.at[z], chip(*peer)))
    d_x_in[z] = d_x[z]

    for s, (lo, hi) in enumerate(STREAM_ROWS):
        for copy in z_pending[s]:
            copy.wait_recv()

    def z_piece(s, i, place):
        first, second, third = STREAM_AXES[s]
        lo, hi = STREAM_ROWS[s]
        return z_all.at[at((second,), me, **on(first, i), **on(third, place)) + (pl.ds(lo, hi - lo),)]

    ring = {}

    def start_ring(step):
        for s in range(n):
            third = STREAM_AXES[s][2]
            right, left = moved(me, third, 1), moved(me, third, -1)
            place = me[third]
            for way, peer, i in (('right', right, step), ('left', left, SIDE - 1 - step)):
                ref = z_piece(s, i, place)
                ring[s, way, step] = copies.start(ref, ref, chip(*peer))

    forwarded = []

    def forward_ring(step):
        for s in range(n):
            third = STREAM_AXES[s][2]
            right, left = moved(me, third, 1), moved(me, third, -1)
            for way, peer, origin, i in (('right', right, left, step), ('left', left, right, SIDE - 1 - step)):
                ring.pop((s, way, step)).wait_recv()
                ref = z_piece(s, i, origin[third])
                forwarded.append(copies.start(ref, ref, chip(*peer)))

    start_ring(0)
    start_ring(1)

    for h in range(2):
        vecs[6 + h:7 + h, 0:channels] = total(x_sums[h].T)
    got_latents.wait()

    def latent_tile(i, carry):
        rows = tile_rows(i, LATENT_TILE)
        unit, rstd = norm_parts(latents[rows, :])
        z_norm[rows, :] = (unit * z_gain[...] + z_shift[...]).astype(BF16)
        d_normed = dot(d_q[rows, :], w_query[...], NT)
        for h, value in enumerate((d_normed * unit, d_normed)):
            vecs[4 + h:5 + h, :] += total(value)
        d_lat = norm_pull(d_normed, unit, rstd, z_gain[...])
        slab, part = lax.div(i, 2), lax.rem(i, 2)
        for t in range(split):
            block = d_lat[:, t * LANES:(t + 1) * LANES].reshape(2, SIDE, SIDE, 8, LANES)
            g[0, pl.ds(2 * part, 2), :, :, slab * split + t] = block
        return carry

    lax.fori_loop(0, tiles, latent_tile, 0)
    slab, part = y, x
    for t in range(split):
        g[0, part, :, :, slab * split + t] += d_mid[:, t * LANES:(t + 1) * LANES].reshape(SIDE, SIDE, 8, LANES)

    def put(value, start):
        for t in range(value.shape[1] // LANES):
            half, slot = tile_place(start + t)
            g[half, :, :, :, slot] = value[:, t * LANES:(t + 1) * LANES].reshape(SIDE, SIDE, SIDE, 8, LANES)

    put(dot(z_norm[...], d_q[...], TN), 4 * split)
    put(dot(x_norm[...], d_k[...], NN), 8 * split)
    put(dot(x_norm[...], d_v[...], NN), 9 * split)
    vecs[0:4, :] = vec_grads[0:4, :]
    half, slot = tile_place(8 * split)
    for i in range(vecs.shape[0]):
        for t in range(split):
            g[half, SIDE - 1, i // SIDE, i % SIDE, slot, t:t + 1, :] = vecs[i:i + 1, t * LANES:(t + 1) * LANES]
    for copy in got_w:
        copy.wait()

    core_half = copies.start(g.at[1 - dp], core_in, partner)
    core_half.wait_recv()
    for i in range(SIDE):
        for j in range(SIDE):
            g[dp, i, j] += core_in[i, j]
    copies.sent(core_half)
    pl.semaphore_signal(half_free, inc=1, device_id=partner, device_id_type=MESH_ID)

    def along(s, place, part=None):
        axis = STREAM_AXES[s][0]
        others = tuple(a for a in range(3) if a != axis)
        index = at(others, me, **on(axis, place), **({} if part is None else on(others[0], part)))
        lo, hi = STREAM_TILES[s]
        return (dp,) + index + (slice(lo, hi),)

    def send(index, dst_index, dst, peer):
        return copies.start(g.at[index], g.at[dst_index] if dst is None else dst, chip(*peer))

    ways = (1, -1)
    first = []
    for s in range(n):
        axis = STREAM_AXES[s][0]
        far = moved(me, axis, 2)[axis]
        first.append([send(along(s, far, halves[w]), None, side_in[s][w], moved(me, axis, d)) for w, d in enumerate(ways)])
    start_ring(2)
    pending = []
    for s in range(n):
        axis = STREAM_AXES[s][0]
        started = []
        for w, d in enumerate(ways):
            peer = moved(me, axis, d)
            first[s][w].wait_recv()
            g[along(s, peer[axis], halves[w])] += side_in[s][w][...]
            started.append(send(along(s, peer[axis]), None, full_in[s][w], peer))
        pending.append(started)
    for phase in range(1, 3):
        for s in range(n):
            for copy in pending[s]:
                copy.wait_recv()
            before, axis = STREAM_AXES[s][phase - 1], STREAM_AXES[s][phase]
            part = parts[s][phase - 1]
            left = [a for a in range(3) if a not in STREAM_AXES[s][:phase]]
            if phase == 1:
                for copy in first[s] + pending[s]:
                    copies.sent(copy)
                for i in range(SIDE):
                    part[i] = g[along(s, me[before], i)] + full_in[s][0][i] + full_in[s][1][i]
            else:
                for i in range(SIDE):
                    index = (me[before], i) if before < left[0] else (i, me[before])
                    part[i] = parts[s][0][index] + sum_slots(recvs[s][1], i)
            started = []
            for d in HOPS:
                peer = moved(me, axis, d)
                index = tuple(peer[axis] if a == axis else slice(None) for a in left)
                started.append(copies.start(part.at[index], recvs[s][phase].at[d - 1], chip(*peer)))
            pending[s] = started
        if phase == 1:
            start_ring(3)
        else:
            forward_ring(0)
    for s, (lo, hi) in enumerate(STREAM_TILES):
        for copy in pending[s]:
            copy.wait_recv()
        got, part = recvs[s][2], parts[s][1]
        axis = STREAM_AXES[s][2]
        g[(dp,) + me + (slice(lo, hi),)] = part[me[axis]] + sum_slots(got)
        ref = g.at[(dp,) + me + (pl.ds(lo, hi - lo),)]
        pending[s] = [copies.start(ref, ref, chip(*moved(me, axis, d))) for d in HOPS]
    forward_ring(1)
    core_copies = []
    pl.semaphore_wait(half_free, 1)
    for s, (lo, hi) in enumerate(STREAM_TILES):
        for copy in pending[s]:
            copy.wait_recv()
        _, axis, last = STREAM_AXES[s]
        ref = g.at[(dp,) + at((last,), me) + (pl.ds(lo, hi - lo),)]
        pending[s] = [copies.start(ref, ref, chip(*moved(me, axis, d))) for d in HOPS]

    def to_partner(index):
        core_copies.append(copies.start(g.at[index], g.at[index], partner))

    for s in range(n):
        for copy in pending[s]:
            copy.wait_recv()
        axis = STREAM_AXES[s][0]
        index = along(s, me[axis])
        pending[s] = [send(index, index, None, moved(me, axis, d)) for d in ways]
        to_partner(index)
    for copy in x_pending:
        copy.wait_recv()
    for i in range(SIDE):
        d_inputs[i] = d_x_in[i].astype(BF16)
    last = []
    for s in range(n):
        axis = STREAM_AXES[s][0]
        for w, d in enumerate(ways):
            pending[s][w].wait_recv()
            index = along(s, moved(me, axis, -d)[axis], halves[w])
            last.append((send(index, index, None, moved(me, axis, d)), s, w))
            to_partner(along(s, moved(me, axis, -d)[axis]))
    for copy, s, w in last:
        copy.wait_recv()
        axis = STREAM_AXES[s][0]
        to_partner(along(s, moved(me, axis, 2)[axis], halves[w]))
    for copy in core_copies:
        copy.wait_recv()

    outs = []
    for t in range(16):
        outs.append(fetch(g.at[0, :, :, :, t], d_lat_out.at[t // split, :, :, :, :, lanes(t % split)]))
    for t in range(16):
        half, slot = tile_place(16 + t)
        outs.append(fetch(g.at[half, :, :, :, slot], w_out_grads.at[t // split, :, :, :, :, lanes(t % split)]))
    for t in range(2 * split):
        half, slot = tile_place(8 * split + t)
        outs.append(fetch(g.at[half, :, :, :, slot], kv_out.at[t // split, :, :, :, :, lanes(t % split)]))
    half, slot = tile_place(8 * split)
    outs.append(fetch(g.at[half, SIDE - 1, :, :, slot], vec_out))
    for copy in forwarded + list(ring.values()):
        copy.wait_recv()
    copies.finish()
    for copy in outs:
        copy.wait()


def backward_block(q, k, v, d_attn, stats, top, z_rows, *others, collective_id):
    n_latents, width = q.shape
    x_rows, latents = others[-2:]
    elements, channels = k.shape[0], x_rows.shape[1]
    vmem = pl.BlockSpec(memory_space=pltpu.VMEM)
    hbm = pl.BlockSpec(memory_space=pl.ANY)
    cube, square = (SIDE, SIDE, SIDE), (SIDE, SIDE)
    shape, wide = jax.ShapeDtypeStruct, pltpu.VMEM
    block = x_rows.shape
    scratch = [
        wide((elements, n_latents), BF16), wide((elements, n_latents), BF16),
        wide((n_latents, width), BF16), wide((elements, width), BF16), wide((elements, width), BF16),
        wide(block, F32), wide((width, elements), BF16), wide((2, channels, LANES), F32), wide(block, F32), wide(block, F32),
        wide((n_latents, width), F32), wide((n_latents, width), BF16), wide((8, width), F32),
        wide((2,) + cube + (HALF_TILES, 8, LANES), F32), wide(cube + (HALF_TILES, 8, LANES), F32)]
    for lo, hi in STREAM_TILES:
        tiles = (hi - lo, 8, LANES)
        scratch += [wide((lead + tiles), F32) for lead in (
            (SIDE // 2, SIDE), (SIDE // 2, SIDE), square, square, (3, SIDE), (3,), square, (SIDE,))]
    n_copies = 160
    slab = cube + (8, width)
    return pl.pallas_call(
        backward_kernel,
        out_shape=(shape(cube + z_rows.shape, F32), shape(block, BF16), shape((4,) + slab, F32), shape((4,) + slab, F32),
                   shape((2,) + slab, F32), shape(square + (8, LANES), F32)),
        in_specs=[vmem] * 6 + [hbm] + [vmem] * (len(others) - 3) + [hbm] * 3,
        out_specs=(hbm, vmem, hbm, hbm, hbm, hbm),
        scratch_shapes=scratch + [pltpu.SemaphoreType.DMA((n_copies,)), pltpu.SemaphoreType.DMA((n_copies,)),
                                  pltpu.SemaphoreType.DMA((64,)), pltpu.SemaphoreType.REGULAR],
        compiler_params=pltpu.CompilerParams(
            collective_id=collective_id, has_side_effects=True, vmem_limit_bytes=VMEM_LIMIT),
    )(q, k, v, d_attn, stats, top, z_rows, *others)


def solution(mesh):
    x_spec = P('dp', 'cp', None)
    row_spec = P('dp', None, None)
    vec_spec = P(None)
    mat_spec = P(None, None)
    in_specs = (x_spec, mat_spec, vec_spec, vec_spec, vec_spec, vec_spec, mat_spec, mat_spec, mat_spec, mat_spec,
                vec_spec, vec_spec, mat_spec, vec_spec, mat_spec, vec_spec, row_spec)
    out_specs = (row_spec, x_spec, mat_spec, vec_spec, vec_spec, vec_spec, vec_spec, mat_spec, mat_spec, mat_spec, mat_spec,
                 vec_spec, vec_spec, mat_spec, vec_spec, mat_spec, vec_spec)

    def local_step(inputs, latents, x_gain, x_shift, z_gain, z_shift, w_query, w_key, w_value, w_out, m_gain, m_shift, w_up, b_up, w_down, b_down, d_out):
        batch, elements, channels = inputs.shape
        n_latents, width = latents.shape
        chunk = n_latents // PLANE
        z, y, x = chip_coords()
        owner = y * SIDE + x

        x_blocks = inputs.transpose(0, 2, 1).astype(F32)
        z0_rows = lax.dynamic_slice(latents, (owner * chunk, 0), (chunk, width))
        d_out_rows = lax.dynamic_slice(d_out, (z, owner * chunk, 0), (1, chunk, width))[0]
        row, column = (lambda vec: vec.reshape(1, -1)), (lambda vec: vec.reshape(-1, 1))
        norms = (column(x_gain), column(x_shift), row(z_gain), row(z_shift), w_query, w_key, w_value)
        q, k, v, x_in, z_out_rows, d_attn, stats, top, d_mid, w_grads, vec_grads = forward_block(
            x_blocks, latents, *norms, z0_rows, d_out_rows, w_out, w_up, w_down, row(m_gain), row(m_shift), row(b_up), row(b_down),
            collective_id=0)
        z_all, d_inputs, d_lat, w_sums, kv_sums, vec_sums = backward_block(
            q, k, v, d_attn.reshape(n_latents, width), stats, top, z_out_rows, d_mid, vec_grads, *norms,
            w_grads.reshape(3, SIDE, SIDE, SIDE, 8, width), x_in, latents, collective_id=1)
        w_sums = w_sums.reshape(4, width, width)
        kv_sums = kv_sums.reshape(2, width, width)[:, :channels]
        vec_sums = vec_sums[:2, :, :width // LANES].reshape(2 * SIDE, width)
        return (z_all.reshape(batch, n_latents, width), d_inputs.transpose(0, 2, 1), d_lat.reshape(n_latents, width),
                vec_sums[6, :channels], vec_sums[7, :channels], vec_sums[4], vec_sums[5],
                w_sums[0], kv_sums[0], kv_sums[1], w_sums[1], vec_sums[0], vec_sums[1],
                w_sums[2], vec_sums[2], w_sums[3], vec_sums[3])

    return jax.shard_map(local_step, mesh=mesh, in_specs=in_specs, out_specs=out_specs, check_vma=False)
```

```python
import functools
import math

import jax
import jax.numpy as jnp
from jax import lax
from jax.experimental import pallas as pl
from jax.experimental.pallas import tpu as pltpu
from jax.sharding import PartitionSpec as P

LN_EPS = 1e-5
BF16 = jnp.bfloat16
F32 = jnp.float32
MESH_ID = pl.DeviceIdType.MESH
SIDE = 4
PLANE = SIDE * SIDE
LANES = 128
LATENT_TILE = 256
LOG2E = math.log2(math.e)
GELU_C = math.sqrt(2.0 / math.pi)
GELU_A = 0.044715
HALF_TILES = 20
STREAM_TILES = ((0, 7), (7, 14), (14, 20))
STREAM_ROWS = ((0, 32), (32, 80), (80, 128))
VMEM_LIMIT = 67043328
STREAM_AXES = ((2, 1, 0), (1, 0, 2), (0, 2, 1))


def contract(form, lhs, rhs):
    return jnp.einsum(form, lhs, rhs, preferred_element_type=F32)


def dot(lhs, rhs, dims):
    return lax.dot_general(lhs, rhs, (dims, ((), ())), preferred_element_type=F32)


NN = ((1,), (0,))
NT = ((1,), (1,))
TN = ((0,), (0,))
DOWN, ACROSS = 0, 1
HOPS = (2, 1, 3)


def mean(value, axis=ACROSS):
    return jnp.mean(value, axis=axis, keepdims=True)


def total(value, axis=DOWN):
    return jnp.sum(value, axis=axis, keepdims=True)


def zeros(*shape):
    return jnp.zeros(shape, F32)


def lanes(t):
    return pl.ds(t * LANES, LANES)


def tile_rows(i, size):
    return pl.ds(pl.multiple_of(i * size, size), size)


def norm_parts(value, axis=ACROSS):
    centred = value - mean(value, axis)
    rstd = lax.rsqrt(mean(centred * centred, axis) + LN_EPS)
    return centred * rstd, rstd


def norm_pull(d_normed, unit, rstd, gain, axis=ACROSS):
    d_unit = d_normed * gain
    return rstd * (d_unit - mean(d_unit, axis) - unit * mean(d_unit * unit, axis))


def as_column(row):
    return jnp.broadcast_to(row[...], (LANES, row.shape[1])).T[:, :1]


def row_pair(ref, i):
    return jnp.concatenate([ref[pl.ds(2 * i, 1), :], ref[pl.ds(2 * i + 1, 1), :]], axis=ACROSS)


def sum_slots(ref, *index):
    return ref[(0,) + index] + ref[(1,) + index] + ref[(2,) + index]


def gelu_parts(pre):
    tanh = jnp.tanh(GELU_C * (pre + GELU_A * pre * pre * pre))
    slope = 0.5 * (1.0 + tanh) + 0.5 * pre * (1.0 - tanh * tanh) * (GELU_C * (1.0 + 3.0 * GELU_A * pre * pre))
    return 0.5 * pre * (1.0 + tanh), slope


def chip_coords():
    cp = lax.axis_index('cp')
    return lax.div(cp, PLANE), lax.rem(lax.div(cp, SIDE), SIDE), lax.rem(cp, SIDE)


def chip(z, y, x):
    return {'cp': z * PLANE + y * SIDE + x}


def moved(coords, axis, offset):
    shifted = list(coords)
    shifted[axis] = lax.rem(coords[axis] + offset + SIDE, SIDE)
    return tuple(shifted)


def enter(peers):
    barrier = pltpu.get_barrier_semaphore()
    for peer in peers:
        pl.semaphore_signal(barrier, inc=1, device_id=peer, device_id_type=MESH_ID)
    pl.semaphore_wait(barrier, len(peers))


class Copies:
    def __init__(self, send_sems, recv_sems):
        self.send_sems, self.recv_sems, self.used, self.open = send_sems, recv_sems, 0, []

    def start(self, src, dst, peer):
        copy = pltpu.make_async_remote_copy(
            src_ref=src, dst_ref=dst, send_sem=self.send_sems.at[self.used], recv_sem=self.recv_sems.at[self.used],
            device_id=peer, device_id_type=MESH_ID)
        self.used += 1
        copy.start()
        self.open.append(copy)
        return copy

    def sent(self, copy):
        copy.wait_send()
        self.open = [other for other in self.open if other is not copy]

    def finish(self):
        for copy in self.open:
            copy.wait_send()


class LocalCopies:
    def __init__(self, sems):
        self.sems, self.used = sems, 0

    def start(self, src, dst):
        copy = pltpu.make_async_copy(src, dst, self.sems.at[self.used])
        self.used += 1
        copy.start()
        return copy


def at(free, coords, **other):
    index = []
    for axis, name in enumerate('zyx'):
        index.append(other[name] if name in other else (slice(None) if axis in free else coords[axis]))
    return tuple(index)


def on(axis, value):
    return {'zyx'[axis]: value}


def forward_kernel(
        x_blocks, latents_in, d_out_in, x_gain_row, x_shift_row, z_gain, z_shift, w_query, w_key, w_value,
        w_out, w_up, w_down, m_gain, m_shift, b_up, b_down,
        q_out, k_out, v_out, x_out, z_all, w_grads_out, d_attn_all, stats_all, top_all, d_mid_out, vec_grads,
        q, k, v, x_in, latents, d_out, z_out, w_grads,
        vt, logits, mixed, top_own, tops, sum_own, sum_parts, sums, sa, sb, fa, fb, pa1, pb1, ra2, rb2, d_attn_f32, stats_f32,
        send_sems, recv_sems, local_sems):
    me = chip_coords()
    local = LocalCopies(local_sems)
    got_latents = local.start(latents_in, latents)
    got_own = local.start(x_blocks.at[me[0]], x_in.at[me[0]])
    z, y, x = me
    owner = y * SIDE + x
    plane_peers = []
    for d in range(1, PLANE):
        other = lax.rem(owner + d, PLANE)
        plane_peers.append((other, chip(z, lax.div(other, SIDE), lax.rem(other, SIDE))))
    enter([device for _, device in plane_peers] + [chip(*moved(me, 0, d)) for d in HOPS])
    copies = Copies(send_sems, recv_sems)
    chunk = d_out.shape[0]
    got_d_out = local.start(d_out_in.at[z, pl.ds(owner * chunk, chunk), :], d_out)
    qk_scale = q.shape[1] ** -0.5
    to_log2 = qk_scale * LOG2E
    tiles = q.shape[0] // LATENT_TILE
    halves = (slice(0, SIDE // 2), slice(SIDE // 2, SIDE))
    ways = (1, -1)
    half_v = vt.shape[0] // 2
    block_rows = x_blocks.shape[-1]

    got_x = {}
    for d in HOPS:
        peer = moved(me, 0, d)
        got_x[d] = copies.start(x_blocks.at[peer[0]], x_in.at[z], chip(*peer))
    top_own[...] = jnp.full(top_own.shape, -jnp.inf, F32)
    x_gain, x_shift = as_column(x_gain_row), as_column(x_shift_row)
    got_latents.wait()

    def query_tile(i, carry):
        rows = tile_rows(i, LATENT_TILE)
        unit, _ = norm_parts(latents[rows, :])
        z_norm = (unit * z_gain[...] + z_shift[...]).astype(BF16)
        q[rows, :] = dot(z_norm, w_query[...], NN).astype(BF16)
        return carry

    lax.fori_loop(0, tiles, query_tile, 0)
    saved = [local.start(q, q_out)]
    got_own.wait()

    def block_logits(j):
        rows = tile_rows(j, block_rows)
        unit, _ = norm_parts(x_in[j], DOWN)
        x_norm = (unit * x_gain + x_shift).astype(BF16)
        k[rows, :] = dot(x_norm, w_key[...], TN).astype(BF16)
        v[rows, :] = dot(x_norm, w_value[...], TN).astype(BF16)
        vt[:, rows] = dot(w_value[...], x_norm, TN).astype(BF16)

        def logits_tile(i, carry):
            s = dot(k[rows, :], q[tile_rows(i, LATENT_TILE), :], NT)
            logits[i, rows, :] = s
            top = jnp.max(s, axis=DOWN, keepdims=True)
            for h in range(2):
                row = pl.ds(2 * i + h, 1)
                top_own[row, :] = jnp.maximum(top_own[row, :], top[:, h * LANES:(h + 1) * LANES])
            return carry

        lax.fori_loop(0, tiles, logits_tile, 0)

    block_logits(z)
    for d in HOPS[::-1]:
        got_x[d].wait_recv()
        block_logits(moved(me, 0, -d)[0])
    top_own[...] = jnp.ceil(top_own[...] * to_log2)
    saved += [local.start(k, k_out), local.start(v, v_out), local.start(x_in, x_out)]
    tops[owner] = top_own[...]
    top_copies = [copies.start(top_own, tops.at[owner], device) for _, device in plane_peers]

    def mix_tile(i, carry):
        top = row_pair(top_own, i)
        w = jnp.exp2(logits[i] * to_log2 - top)
        weight_sum = total(w)
        for h in range(2):
            sum_own[pl.ds(2 * i + h, 1), :] = weight_sum[:, h * LANES:(h + 1) * LANES]
        product = dot(vt[...], w.astype(BF16), NN)
        at_y, at_x = lax.div(i, 2), 2 * lax.rem(i, 2)
        for h in range(2):
            mixed[at_y, at_x + h] = product[:, h * LANES:(h + 1) * LANES]
        return carry

    lax.fori_loop(0, tiles, mix_tile, 0)
    for copy in top_copies:
        copy.wait_recv()
    top = functools.reduce(jnp.maximum, [tops[i] for i in range(PLANE)])
    top_all[...] = top
    factor = jnp.exp2(top_own[...] - top)
    scaled_sum = sum_own[...] * factor
    for i in range(PLANE):
        mixed[i // SIDE, i % SIDE] = mixed[i // SIDE, i % SIDE] * factor[i:i + 1, :]
        sum_parts[i] = jnp.broadcast_to(scaled_sum[i:i + 1, :], (8, LANES))

    streams = ((2, 1, pl.ds(0, half_v), sa, fa, pa1, ra2), (1, 2, pl.ds(half_v, half_v), sb, fb, pb1, rb2))

    def mixed_at(axis, place, part, cols):
        return ((part, place) if axis == 2 else (place, part)) + (cols,)

    first = []
    for axis, _, cols, side_in, _, _, _ in streams:
        far = moved(me, axis, 2)[axis]
        first.append([copies.start(mixed.at[mixed_at(axis, far, halves[w], cols)], side_in.at[w], chip(*moved(me, axis, d)))
                      for w, d in enumerate(ways)])
    sums[owner] = sum_parts[owner]
    sum_copies = [copies.start(sum_parts.at[other], sums.at[owner], device) for other, device in plane_peers]
    full = []
    for (axis, _, cols, side_in, full_in, _, _), arriving in zip(streams, first):
        started = []
        for w, d in enumerate(ways):
            peer = moved(me, axis, d)
            arriving[w].wait_recv()
            mixed[mixed_at(axis, peer[axis], halves[w], cols)] += side_in[w]
            started.append(copies.start(mixed.at[mixed_at(axis, peer[axis], slice(None), cols)], full_in.at[w], chip(*peer)))
        full.append(started)
    second = []
    for (axis, other, cols, _, full_in, part, slots), arriving in zip(streams, full):
        for copy in arriving:
            copy.wait_recv()
        for i in range(SIDE):
            part[i] = mixed[mixed_at(axis, me[axis], i, cols)] + full_in[0, i] + full_in[1, i]
        for d in HOPS:
            peer = moved(me, other, d)
            second.append(copies.start(part.at[peer[other]], slots.at[d - 1], chip(*peer)))
    for copy in sum_copies:
        copy.wait_recv()
    inv_sum = 1.0 / functools.reduce(lambda a, b: a + b, [sums[i] for i in range(PLANE)])
    for copy in second:
        copy.wait_recv()
    upper = pa1[y] + sum_slots(ra2)
    lower = pb1[x] + sum_slots(rb2)
    attn_t = jnp.concatenate([upper, lower], axis=DOWN) * inv_sum[0:1, :]

    attn_t_low = attn_t.astype(BF16)
    attn_low = attn_t.T.astype(BF16)
    z_mid = latents[tile_rows(owner, chunk), :] + dot(attn_low, w_out[...], NN)
    unit, rstd = norm_parts(z_mid)
    hidden_f32 = unit * m_gain[...] + m_shift[...]
    hidden = hidden_f32.astype(BF16)
    pre = dot(hidden, w_up[...], NN) + b_up[...]
    act_f32, slope = gelu_parts(pre)
    act = act_f32.astype(BF16)
    z_out[...] = z_mid + dot(act, w_down[...], NN) + b_down[...]

    got_d_out.wait()
    d_out_low = d_out[...]
    d_out_f32 = d_out_low.astype(F32)
    d_act = dot(d_out_low, w_down[...], NT).astype(BF16).astype(F32)
    d_pre = d_act * slope
    d_pre_low = d_pre.astype(BF16)
    d_hidden = dot(d_pre_low, w_up[...], NT).astype(BF16).astype(F32)
    d_mid = d_out_f32 + norm_pull(d_hidden, unit, rstd, m_gain[...])
    d_mid_low = d_mid.astype(BF16)
    d_attn = dot(d_mid_low, w_out[...], NT).astype(BF16).astype(F32)
    row_dot = total(d_attn.T * attn_t)

    half_r = LANES // 2
    d_attn_f32[y, x] = d_attn
    stats_f32[owner, 0:1, :] = row_dot
    stats_f32[owner, 1:2, :] = inv_sum[0:1, :]
    up, down = pl.ds(0, half_r), pl.ds(half_r, half_r)
    first = [[], []]
    for d in HOPS:
        first[0].append(copies.start(d_attn_f32.at[y, x, up], d_attn_f32.at[y, x, up], chip(*moved(me, 1, d))))
        first[1].append(copies.start(d_attn_f32.at[y, x, down], d_attn_f32.at[y, x, down], chip(*moved(me, 2, d))))
    stat_copies = [copies.start(stats_f32.at[owner], stats_f32.at[owner], device) for _, device in plane_peers]

    saved.append(local.start(z_out, z_all.at[z, y, x]))
    z_first = []
    for (lo, hi), (axis, _, _) in zip(STREAM_ROWS, STREAM_AXES):
        rows = pl.ds(lo, hi - lo)
        z_first += [copies.start(z_out.at[rows], z_all.at[z, y, x, rows], chip(*moved(me, axis, d))) for d in HOPS]

    d_mid_out[...] = d_mid
    w_grads[0] = dot(attn_t_low, d_mid_low, NN)
    w_grads[1] = dot(hidden_f32.T.astype(BF16), d_pre_low, NN)
    w_grads[2] = dot(act_f32.T.astype(BF16), d_out_low, NN)
    saved.append(local.start(w_grads, w_grads_out))
    for i, value in enumerate((d_hidden * unit, d_hidden, d_pre, d_out_f32)):
        vec_grads[i:i + 1, :] = total(value)
    vec_grads[4:8, :] = zeros(4, vec_grads.shape[1])

    gathered = []
    for axis, rows, arriving in ((2, up, first[0]), (1, down, first[1])):
        for copy in arriving:
            copy.wait_recv()
        ref = d_attn_f32.at[mixed_at(axis, me[axis], slice(None), rows)]
        gathered.append((axis, rows, [copies.start(ref, ref, chip(*moved(me, axis, d))) for d in ways]))
    last = []
    for axis, rows, arriving in gathered:
        for w, d in enumerate(ways):
            arriving[w].wait_recv()
            ref = d_attn_f32.at[mixed_at(axis, moved(me, axis, -d)[axis], halves[w], rows)]
            last.append(copies.start(ref, ref, chip(*moved(me, axis, d))))
    for copy in stat_copies + last + z_first:
        copy.wait_recv()
    copies.finish()
    stats_all[...] = stats_f32[...]
    for i in range(PLANE):
        d_attn_all[i] = d_attn_f32[i // SIDE, i % SIDE].astype(BF16)
    for copy in saved:
        copy.wait()


def forward_block(x_blocks, latents, d_out, *others, collective_id):
    latents_n, width = latents.shape
    _, channels, block_rows = x_blocks.shape
    elements = SIDE * block_rows
    chunk = latents_n // PLANE
    half = width // 2
    vmem = pl.BlockSpec(memory_space=pltpu.VMEM)
    hbm = pl.BlockSpec(memory_space=pl.ANY)
    n_copies = 90
    shape, wide = jax.ShapeDtypeStruct, pltpu.VMEM
    stat, slots = (PLANE, 8, LANES), (2, SIDE, half, LANES)
    saved = (((latents_n, width), BF16), ((elements, width), BF16), ((elements, width), BF16), (x_blocks.shape, F32))
    return pl.pallas_call(
        forward_kernel,
        out_shape=tuple(shape(*one) for one in saved) + (
            shape((SIDE, SIDE, SIDE, chunk, width), F32), shape((3, width, width), F32), shape((PLANE, chunk, width), BF16),
            shape(stat, F32), shape((PLANE, LANES), F32), shape((chunk, width), F32), shape((8, width), F32)),
        in_specs=[hbm] * 3 + [vmem] * len(others),
        out_specs=(hbm,) * 6 + (vmem,) * 5,
        scratch_shapes=[wide(*one) for one in saved] + [
            wide((latents_n, width), F32), wide((chunk, width), BF16), wide((chunk, width), F32), wide((3, width, width), F32),
            wide((width, elements), BF16), wide((latents_n // LATENT_TILE, elements, LATENT_TILE), F32),
            wide((SIDE, SIDE, width, LANES), F32),
            wide((PLANE, LANES), F32), wide((PLANE, PLANE, LANES), F32), wide((PLANE, LANES), F32), wide(stat, F32), wide(stat, F32),
            wide((2, SIDE // 2, half, LANES), F32), wide((2, SIDE // 2, half, LANES), F32), wide(slots, F32), wide(slots, F32),
            wide(slots[1:], F32), wide(slots[1:], F32), wide((3, half, LANES), F32), wide((3, half, LANES), F32),
            wide((SIDE, SIDE, chunk, width), F32), wide(stat, F32),
            pltpu.SemaphoreType.DMA((n_copies,)), pltpu.SemaphoreType.DMA((n_copies,)), pltpu.SemaphoreType.DMA((16,))],
        compiler_params=pltpu.CompilerParams(
            collective_id=collective_id, has_side_effects=True, vmem_limit_bytes=VMEM_LIMIT),
    )(x_blocks, latents, d_out, *others)


def tile_place(t):
    return t // HALF_TILES, t % HALF_TILES


def backward_kernel(
        q_in, k_in, v_in, d_attn_in, z_in, stats, top, d_mid, vec_grads, x_gain_row, x_shift_row, z_gain, z_shift,
        w_query, w_key, w_value, w_grads, x_in, latents_in,
        z_all, d_inputs, d_lat_out, w_out_grads, kv_out, vec_out,
        q, k, v, d_attn, probs, d_logits, d_q, d_k, d_v, x_rows, x_norm, x_sums, d_x, d_x_in, latents, z_norm, vecs, g, core_in, *rest):
    n, per = len(STREAM_TILES), 8
    side_in = [rest[per * s:per * s + 2] for s in range(n)]
    full_in = [rest[per * s + 2:per * s + 4] for s in range(n)]
    recvs = [(None,) + rest[per * s + 4:per * s + 6] for s in range(n)]
    parts = [rest[per * s + 6:per * s + 8] for s in range(n)]
    send_sems, recv_sems, local_sems, half_free = rest[per * n:]
    me = chip_coords()
    z, y, x = me
    dp = lax.axis_index('dp')
    partner = {'dp': 1 - dp}
    qk_scale = q.shape[1] ** -0.5
    to_log2 = qk_scale * LOG2E
    width = q.shape[1]
    channels = x_rows.shape[1]
    halves = (slice(0, SIDE // 2), slice(SIDE // 2, SIDE))
    tiles = q.shape[0] // LATENT_TILE
    split = width // LANES
    chips = SIDE ** 3

    local = LocalCopies(local_sems)
    fetch = local.start
    got_first = [fetch(*pair) for pair in ((q_in, q), (k_in, k), (v_in, v), (d_attn_in, d_attn))]
    enter([partner] + [chip(*moved(me, axis, d)) for axis in range(3) for d in HOPS])
    copies = Copies(send_sems, recv_sems)

    ways = (1, -1)
    z_pending = []
    for (lo, hi), (first, second, _) in zip(STREAM_ROWS, STREAM_AXES):
        ref = z_all.at[at((first,), me) + (pl.ds(lo, hi - lo),)]
        z_pending.append([copies.start(ref, ref, chip(*moved(me, second, d))) for d in ways])
    got_x = fetch(x_in, x_rows)
    got_latents = fetch(latents_in, latents)
    got_w = []
    for i in range(3):
        for t in range(split):
            half, slot = tile_place(20 + split * i + t)
            got_w.append(fetch(w_grads.at[i, :, :, :, :, lanes(t)], g.at[half, :, :, :, slot]))
    x_norm[...] = jnp.zeros(x_norm.shape, BF16)
    x_gain, x_shift = as_column(x_gain_row), as_column(x_shift_row)
    for copy in got_first:
        copy.wait()

    def pair(ref, i, row):
        return jnp.concatenate([ref[2 * i + h, row:row + 1, :] for h in range(2)], axis=ACROSS)

    def attend_tile(i, carry):
        rows = tile_rows(i, LATENT_TILE)
        peak = row_pair(top, i)
        row_dot, inv_sum = pair(stats, i, 0), pair(stats, i, 1)
        p = jnp.exp2(dot(k[...], q[rows, :], NT) * to_log2 - peak) * inv_sum
        probs[:, rows] = p.astype(BF16)
        d_p = dot(v[...], d_attn[rows, :], NT)
        d_s = (p * (d_p - row_dot) * qk_scale).astype(BF16)
        d_logits[:, rows] = d_s
        d_q[rows, :] = dot(d_s, k[...], TN).astype(BF16)
        return carry

    lax.fori_loop(0, tiles // 2, attend_tile, 0)
    for s, (lo, hi) in enumerate(STREAM_ROWS):
        first, second, _ = STREAM_AXES[s]
        arrived, z_pending[s] = z_pending[s], []
        for copy, d, part in zip(arrived, ways, halves):
            copy.wait_recv()
            origin = on(second, moved(me, second, -d)[second])
            ref = z_all.at[at((), me, **on(first, part), **origin) + (pl.ds(lo, hi - lo),)]
            z_pending[s].append(copies.start(ref, ref, chip(*moved(me, second, d))))

    lax.fori_loop(tiles // 2, tiles, attend_tile, 0)

    for s, (lo, hi) in enumerate(STREAM_ROWS):
        for copy in z_pending[s]:
            copy.wait_recv()

    def z_piece(s, i, place):
        first, second, third = STREAM_AXES[s]
        lo, hi = STREAM_ROWS[s]
        return z_all.at[at((second,), me, **on(first, i), **on(third, place)) + (pl.ds(lo, hi - lo),)]

    ring = {}

    def start_ring(step):
        for s in range(n):
            third = STREAM_AXES[s][2]
            right, left = moved(me, third, 1), moved(me, third, -1)
            place = me[third]
            for way, peer, i in (('right', right, step), ('left', left, SIDE - 1 - step)):
                ref = z_piece(s, i, place)
                ring[s, way, step] = copies.start(ref, ref, chip(*peer))

    forwarded = []

    def forward_ring(step):
        for s in range(n):
            third = STREAM_AXES[s][2]
            right, left = moved(me, third, 1), moved(me, third, -1)
            for way, peer, origin, i in (('right', right, left, step), ('left', left, right, SIDE - 1 - step)):
                ring.pop((s, way, step)).wait_recv()
                ref = z_piece(s, i, origin[third])
                forwarded.append(copies.start(ref, ref, chip(*peer)))

    start_ring(0)
    start_ring(1)

    vecs[...] = zeros(*vecs.shape)
    x_sums[...] = zeros(*x_sums.shape)
    got_x.wait()

    def element_tile(i, carry):
        rows = tile_rows(i, x_rows.shape[-1])
        d_v_low = dot(probs[rows, :], d_attn[...], NN).astype(BF16)
        d_k_low = dot(d_logits[rows, :], q[...], NN).astype(BF16)
        d_v[rows, :] = d_v_low
        d_k[rows, :] = d_k_low
        unit, rstd = norm_parts(x_rows[i], DOWN)
        x_norm[0:channels, rows] = (unit * x_gain + x_shift).astype(BF16)
        d_normed = (dot(w_key[...], d_k_low, NT) + dot(w_value[...], d_v_low, NT)).astype(BF16).astype(F32)
        d_x[i] = norm_pull(d_normed, unit, rstd, x_gain, DOWN)
        for h, value in enumerate((d_normed * unit, d_normed)):
            x_sums[h] += sum(value[:, t * LANES:(t + 1) * LANES] for t in range(value.shape[1] // LANES))
        return carry

    lax.fori_loop(0, SIDE, element_tile, 0)
    x_pending = []
    for d in HOPS:
        peer = moved(me, 0, d)
        x_pending.append(copies.start(d_x.at[peer[0]], d_x_in.at[z], chip(*peer)))
    d_x_in[z] = d_x[z]

    for h in range(2):
        vecs[6 + h:7 + h, 0:channels] = total(x_sums[h].T)
    got_latents.wait()

    def latent_tile(i, carry):
        rows = tile_rows(i, LATENT_TILE)
        unit, rstd = norm_parts(latents[rows, :])
        z_norm[rows, :] = (unit * z_gain[...] + z_shift[...]).astype(BF16)
        d_normed = dot(d_q[rows, :], w_query[...], NT)
        for h, value in enumerate((d_normed * unit, d_normed)):
            vecs[4 + h:5 + h, :] += total(value)
        d_lat = norm_pull(d_normed, unit, rstd, z_gain[...])
        slab, part = lax.div(i, 2), lax.rem(i, 2)
        for t in range(split):
            block = d_lat[:, t * LANES:(t + 1) * LANES].reshape(2, SIDE, SIDE, 8, LANES)
            g[0, pl.ds(2 * part, 2), :, :, slab * split + t] = block
        return carry

    lax.fori_loop(0, tiles, latent_tile, 0)
    slab, part = y, x
    for t in range(split):
        g[0, part, :, :, slab * split + t] += d_mid[:, t * LANES:(t + 1) * LANES].reshape(SIDE, SIDE, 8, LANES)

    def put(value, start):
        for t in range(value.shape[1] // LANES):
            half, slot = tile_place(start + t)
            g[half, :, :, :, slot] = value[:, t * LANES:(t + 1) * LANES].reshape(SIDE, SIDE, SIDE, 8, LANES)

    put(dot(z_norm[...], d_q[...], TN), 4 * split)
    put(dot(x_norm[...], d_k[...], NN), 8 * split)
    put(dot(x_norm[...], d_v[...], NN), 9 * split)
    vecs[0:4, :] = vec_grads[0:4, :]
    half, slot = tile_place(8 * split)
    for i in range(vecs.shape[0]):
        for t in range(split):
            g[half, SIDE - 1, i // SIDE, i % SIDE, slot, t:t + 1, :] = vecs[i:i + 1, t * LANES:(t + 1) * LANES]
    for copy in got_w:
        copy.wait()

    core_half = copies.start(g.at[1 - dp], core_in, partner)
    core_half.wait_recv()
    for i in range(SIDE):
        for j in range(SIDE):
            g[dp, i, j] += core_in[i, j]
    copies.sent(core_half)
    pl.semaphore_signal(half_free, inc=1, device_id=partner, device_id_type=MESH_ID)

    def along(s, place, part=None):
        axis = STREAM_AXES[s][0]
        others = tuple(a for a in range(3) if a != axis)
        index = at(others, me, **on(axis, place), **({} if part is None else on(others[0], part)))
        lo, hi = STREAM_TILES[s]
        return (dp,) + index + (slice(lo, hi),)

    def send(index, dst_index, dst, peer):
        return copies.start(g.at[index], g.at[dst_index] if dst is None else dst, chip(*peer))

    first = []
    for s in range(n):
        axis = STREAM_AXES[s][0]
        far = moved(me, axis, 2)[axis]
        first.append([send(along(s, far, halves[w]), None, side_in[s][w], moved(me, axis, d)) for w, d in enumerate(ways)])
    start_ring(2)
    pending = []
    for s in range(n):
        axis = STREAM_AXES[s][0]
        started = []
        for w, d in enumerate(ways):
            peer = moved(me, axis, d)
            first[s][w].wait_recv()
            g[along(s, peer[axis], halves[w])] += side_in[s][w][...]
            started.append(send(along(s, peer[axis]), None, full_in[s][w], peer))
        pending.append(started)
    for phase in range(1, 3):
        for s in range(n):
            for copy in pending[s]:
                copy.wait_recv()
            before, axis = STREAM_AXES[s][phase - 1], STREAM_AXES[s][phase]
            part = parts[s][phase - 1]
            left = [a for a in range(3) if a not in STREAM_AXES[s][:phase]]
            if phase == 1:
                for copy in first[s] + pending[s]:
                    copies.sent(copy)
                for i in range(SIDE):
                    part[i] = g[along(s, me[before], i)] + full_in[s][0][i] + full_in[s][1][i]
            else:
                for i in range(SIDE):
                    index = (me[before], i) if before < left[0] else (i, me[before])
                    part[i] = parts[s][0][index] + sum_slots(recvs[s][1], i)
            started = []
            for d in HOPS:
                peer = moved(me, axis, d)
                index = tuple(peer[axis] if a == axis else slice(None) for a in left)
                started.append(copies.start(part.at[index], recvs[s][phase].at[d - 1], chip(*peer)))
            pending[s] = started
        if phase == 1:
            start_ring(3)
        else:
            forward_ring(0)
    for s, (lo, hi) in enumerate(STREAM_TILES):
        for copy in pending[s]:
            copy.wait_recv()
        got, part = recvs[s][2], parts[s][1]
        axis = STREAM_AXES[s][2]
        g[(dp,) + me + (slice(lo, hi),)] = part[me[axis]] + sum_slots(got)
        ref = g.at[(dp,) + me + (pl.ds(lo, hi - lo),)]
        pending[s] = [copies.start(ref, ref, chip(*moved(me, axis, d))) for d in HOPS]
    forward_ring(1)
    core_copies = []
    pl.semaphore_wait(half_free, 1)
    for s, (lo, hi) in enumerate(STREAM_TILES):
        for copy in pending[s]:
            copy.wait_recv()
        _, axis, last = STREAM_AXES[s]
        ref = g.at[(dp,) + at((last,), me) + (pl.ds(lo, hi - lo),)]
        pending[s] = [copies.start(ref, ref, chip(*moved(me, axis, d))) for d in HOPS]

    def to_partner(index):
        core_copies.append(copies.start(g.at[index], g.at[index], partner))

    for s in range(n):
        for copy in pending[s]:
            copy.wait_recv()
        axis = STREAM_AXES[s][0]
        index = along(s, me[axis])
        pending[s] = [send(index, index, None, moved(me, axis, d)) for d in ways]
        to_partner(index)
    for copy in x_pending:
        copy.wait_recv()
    for i in range(SIDE):
        d_inputs[i] = d_x_in[i].astype(BF16)
    last = []
    for s in range(n):
        axis = STREAM_AXES[s][0]
        for w, d in enumerate(ways):
            pending[s][w].wait_recv()
            index = along(s, moved(me, axis, -d)[axis], halves[w])
            last.append((send(index, index, None, moved(me, axis, d)), s, w))
            to_partner(along(s, moved(me, axis, -d)[axis]))
    for copy, s, w in last:
        copy.wait_recv()
        axis = STREAM_AXES[s][0]
        to_partner(along(s, moved(me, axis, 2)[axis], halves[w]))
    for copy in core_copies:
        copy.wait_recv()

    outs = []
    for t in range(16):
        outs.append(fetch(g.at[0, :, :, :, t], d_lat_out.at[t // split, :, :, :, :, lanes(t % split)]))
    for t in range(16):
        half, slot = tile_place(16 + t)
        outs.append(fetch(g.at[half, :, :, :, slot], w_out_grads.at[t // split, :, :, :, :, lanes(t % split)]))
    for t in range(2 * split):
        half, slot = tile_place(8 * split + t)
        outs.append(fetch(g.at[half, :, :, :, slot], kv_out.at[t // split, :, :, :, :, lanes(t % split)]))
    half, slot = tile_place(8 * split)
    outs.append(fetch(g.at[half, SIDE - 1, :, :, slot], vec_out))
    for copy in forwarded + list(ring.values()):
        copy.wait_recv()
    copies.finish()
    for copy in outs:
        copy.wait()


def backward_block(q, k, v, d_attn, z_all, *others, collective_id):
    n_latents, width = q.shape
    x_rows, latents = others[-2:]
    elements, channels = k.shape[0], x_rows.shape[1]
    vmem = pl.BlockSpec(memory_space=pltpu.VMEM)
    hbm = pl.BlockSpec(memory_space=pl.ANY)
    cube, square = (SIDE, SIDE, SIDE), (SIDE, SIDE)
    shape, wide = jax.ShapeDtypeStruct, pltpu.VMEM
    block = x_rows.shape
    scratch = [
        wide(q.shape, BF16), wide(k.shape, BF16), wide(v.shape, BF16), wide(q.shape, BF16), wide((elements, n_latents), BF16), wide((elements, n_latents), BF16),
        wide((n_latents, width), BF16), wide((elements, width), BF16), wide((elements, width), BF16),
        wide(block, F32), wide((width, elements), BF16), wide((2, channels, LANES), F32), wide(block, F32), wide(block, F32),
        wide((n_latents, width), F32), wide((n_latents, width), BF16), wide((8, width), F32),
        wide((2,) + cube + (HALF_TILES, 8, LANES), F32), wide(cube + (HALF_TILES, 8, LANES), F32)]
    for lo, hi in STREAM_TILES:
        tiles = (hi - lo, 8, LANES)
        scratch += [wide((lead + tiles), F32) for lead in (
            (SIDE // 2, SIDE), (SIDE // 2, SIDE), square, square, (3, SIDE), (3,), square, (SIDE,))]
    n_copies = 160
    slab = cube + (8, width)
    return pl.pallas_call(
        backward_kernel,
        out_shape=(shape(z_all.shape, F32), shape(block, BF16), shape((4,) + slab, F32), shape((4,) + slab, F32),
                   shape((2,) + slab, F32), shape(square + (8, LANES), F32)),
        in_specs=[hbm] * 5 + [vmem] * (len(others) - 3) + [hbm] * 3,
        out_specs=(hbm, vmem, hbm, hbm, hbm, hbm),
        input_output_aliases={4: 0},
        scratch_shapes=scratch + [pltpu.SemaphoreType.DMA((n_copies,)), pltpu.SemaphoreType.DMA((n_copies,)),
                                  pltpu.SemaphoreType.DMA((64,)), pltpu.SemaphoreType.REGULAR],
        compiler_params=pltpu.CompilerParams(
            collective_id=collective_id, has_side_effects=True, vmem_limit_bytes=VMEM_LIMIT),
    )(q, k, v, d_attn, z_all, *others)


def solution(mesh):
    x_spec = P('dp', 'cp', None)
    row_spec = P('dp', None, None)
    vec_spec = P(None)
    mat_spec = P(None, None)
    in_specs = (x_spec, mat_spec, vec_spec, vec_spec, vec_spec, vec_spec, mat_spec, mat_spec, mat_spec, mat_spec,
                vec_spec, vec_spec, mat_spec, vec_spec, mat_spec, vec_spec, row_spec)
    out_specs = (row_spec, x_spec, mat_spec, vec_spec, vec_spec, vec_spec, vec_spec, mat_spec, mat_spec, mat_spec, mat_spec,
                 vec_spec, vec_spec, mat_spec, vec_spec, mat_spec, vec_spec)

    def local_step(inputs, latents, x_gain, x_shift, z_gain, z_shift, w_query, w_key, w_value, w_out, m_gain, m_shift, w_up, b_up, w_down, b_down, d_out):
        batch, elements, channels = inputs.shape
        n_latents, width = latents.shape
        chunk = n_latents // PLANE
        z, y, x = chip_coords()
        owner = y * SIDE + x

        x_blocks = inputs.transpose(0, 2, 1).astype(F32)
        row = lambda vec: vec.reshape(1, -1)
        norms = (row(x_gain), row(x_shift), row(z_gain), row(z_shift), w_query, w_key, w_value)
        q, k, v, x_in, z_all, w_grads, d_attn, stats, top, d_mid, vec_grads = forward_block(
            x_blocks, latents, d_out, *norms, w_out, w_up, w_down, row(m_gain), row(m_shift), row(b_up), row(b_down), collective_id=0)
        z_all, d_inputs, d_lat, w_sums, kv_sums, vec_sums = backward_block(
            q, k, v, d_attn.reshape(n_latents, width), z_all, stats, top, d_mid, vec_grads, *norms,
            w_grads.reshape(3, SIDE, SIDE, SIDE, 8, width), x_in, latents, collective_id=1)
        w_sums = w_sums.reshape(4, width, width)
        kv_sums = kv_sums.reshape(2, width, width)[:, :channels]
        vec_sums = vec_sums[:2, :, :width // LANES].reshape(2 * SIDE, width)
        return (z_all.reshape(batch, n_latents, width), d_inputs.transpose(0, 2, 1), d_lat.reshape(n_latents, width),
                vec_sums[6, :channels], vec_sums[7, :channels], vec_sums[4], vec_sums[5],
                w_sums[0], kv_sums[0], kv_sums[1], w_sums[1], vec_sums[0], vec_sums[1],
                w_sums[2], vec_sums[2], w_sums[3], vec_sums[3])

    return jax.shard_map(local_step, mesh=mesh, in_specs=in_specs, out_specs=out_specs, check_vma=False)
```

```python
import functools
import math

import jax
import jax.numpy as jnp
from jax import lax
from jax.experimental import pallas as pl
from jax.experimental.pallas import tpu as pltpu
from jax.sharding import PartitionSpec as P

LN_EPS = 1e-5
BF16 = jnp.bfloat16
F32 = jnp.float32
MESH_ID = pl.DeviceIdType.MESH
SIDE = 4
PLANE = SIDE * SIDE
LANES = 128
LATENT_TILE = 256
LOG2E = math.log2(math.e)
GELU_C = math.sqrt(2.0 / math.pi)
GELU_A = 0.044715
HALF_TILES = 20
STREAM_TILES = ((0, 7), (7, 14), (14, 20))
STREAM_ROWS = ((0, 32), (32, 80), (80, 128))
VMEM_LIMIT = 67043328
STREAM_AXES = ((2, 1, 0), (1, 0, 2), (0, 2, 1))


def contract(form, lhs, rhs):
    return jnp.einsum(form, lhs, rhs, preferred_element_type=F32)


def dot(lhs, rhs, dims):
    return lax.dot_general(lhs, rhs, (dims, ((), ())), preferred_element_type=F32)


NN = ((1,), (0,))
NT = ((1,), (1,))
TN = ((0,), (0,))
DOWN, ACROSS = 0, 1
HOPS = (2, 1, 3)


def mean(value, axis=ACROSS):
    return jnp.mean(value, axis=axis, keepdims=True)


def total(value, axis=DOWN):
    return jnp.sum(value, axis=axis, keepdims=True)


def zeros(*shape):
    return jnp.zeros(shape, F32)


def lanes(t):
    return pl.ds(t * LANES, LANES)


def tile_rows(i, size):
    return pl.ds(pl.multiple_of(i * size, size), size)


def norm_parts(value, axis=ACROSS):
    centred = value - mean(value, axis)
    rstd = lax.rsqrt(mean(centred * centred, axis) + LN_EPS)
    return centred * rstd, rstd


def norm_pull(d_normed, unit, rstd, gain, axis=ACROSS):
    d_unit = d_normed * gain
    return rstd * (d_unit - mean(d_unit, axis) - unit * mean(d_unit * unit, axis))


def as_column(row):
    return jnp.broadcast_to(row[...], (LANES, row.shape[1])).T[:, :1]


def row_pair(ref, i):
    return jnp.concatenate([ref[pl.ds(2 * i, 1), :], ref[pl.ds(2 * i + 1, 1), :]], axis=ACROSS)


def sum_slots(ref, *index):
    return ref[(0,) + index] + ref[(1,) + index] + ref[(2,) + index]


def gelu_parts(pre):
    tanh = jnp.tanh(GELU_C * (pre + GELU_A * pre * pre * pre))
    slope = 0.5 * (1.0 + tanh) + 0.5 * pre * (1.0 - tanh * tanh) * (GELU_C * (1.0 + 3.0 * GELU_A * pre * pre))
    return 0.5 * pre * (1.0 + tanh), slope


def chip_coords():
    cp = lax.axis_index('cp')
    return lax.div(cp, PLANE), lax.rem(lax.div(cp, SIDE), SIDE), lax.rem(cp, SIDE)


def chip(z, y, x):
    return {'cp': z * PLANE + y * SIDE + x}


def moved(coords, axis, offset):
    shifted = list(coords)
    shifted[axis] = lax.rem(coords[axis] + offset + SIDE, SIDE)
    return tuple(shifted)


def enter(peers):
    barrier = pltpu.get_barrier_semaphore()
    for peer in peers:
        pl.semaphore_signal(barrier, inc=1, device_id=peer, device_id_type=MESH_ID)
    pl.semaphore_wait(barrier, len(peers))


class Copies:
    def __init__(self, send_sems, recv_sems):
        self.send_sems, self.recv_sems, self.used, self.open = send_sems, recv_sems, 0, []

    def start(self, src, dst, peer):
        copy = pltpu.make_async_remote_copy(
            src_ref=src, dst_ref=dst, send_sem=self.send_sems.at[self.used], recv_sem=self.recv_sems.at[self.used],
            device_id=peer, device_id_type=MESH_ID)
        self.used += 1
        copy.start()
        self.open.append(copy)
        return copy

    def sent(self, copy):
        copy.wait_send()
        self.open = [other for other in self.open if other is not copy]

    def finish(self):
        for copy in self.open:
            copy.wait_send()


class LocalCopies:
    def __init__(self, sems):
        self.sems, self.used = sems, 0

    def start(self, src, dst):
        copy = pltpu.make_async_copy(src, dst, self.sems.at[self.used])
        self.used += 1
        copy.start()
        return copy


def at(free, coords, **other):
    index = []
    for axis, name in enumerate('zyx'):
        index.append(other[name] if name in other else (slice(None) if axis in free else coords[axis]))
    return tuple(index)


def on(axis, value):
    return {'zyx'[axis]: value}


def forward_kernel(
        x_blocks, latents_in, d_out_in, x_gain_row, x_shift_row, z_gain, z_shift, w_query, w_key, w_value,
        w_out, w_up, w_down, m_gain, m_shift, b_up, b_down,
        q_out, k_out, v_out, x_out, z_all, w_grads_out, d_attn_all, stats_all, top_all, d_mid_out, vec_grads,
        q, k, v, x_in, latents, d_out, z_out, w_grads,
        vt, logits, mixed, top_own, tops, sum_own, sum_parts, sums, sa, sb, fa, fb, pa1, pb1, ra2, rb2, d_attn_f32, stats_f32,
        send_sems, recv_sems, local_sems):
    me = chip_coords()
    local = LocalCopies(local_sems)
    got_latents = local.start(latents_in, latents)
    got_own = local.start(x_blocks.at[me[0]], x_in.at[me[0]])
    z, y, x = me
    owner = y * SIDE + x
    plane_peers = []
    for d in range(1, PLANE):
        other = lax.rem(owner + d, PLANE)
        plane_peers.append((other, chip(z, lax.div(other, SIDE), lax.rem(other, SIDE))))
    enter([device for _, device in plane_peers] + [chip(*moved(me, 0, d)) for d in HOPS])
    copies = Copies(send_sems, recv_sems)
    chunk = d_out.shape[0]
    got_d_out = local.start(d_out_in.at[z, pl.ds(owner * chunk, chunk), :], d_out)
    qk_scale = q.shape[1] ** -0.5
    to_log2 = qk_scale * LOG2E
    tiles = q.shape[0] // LATENT_TILE
    halves = (slice(0, SIDE // 2), slice(SIDE // 2, SIDE))
    ways = (1, -1)
    half_v = vt.shape[0] // 2
    block_rows = x_blocks.shape[-1]

    got_x = {}
    for d in HOPS:
        peer = moved(me, 0, d)
        got_x[d] = copies.start(x_blocks.at[peer[0]], x_in.at[z], chip(*peer))
    top_own[...] = jnp.full(top_own.shape, -jnp.inf, F32)
    x_gain, x_shift = as_column(x_gain_row), as_column(x_shift_row)
    got_latents.wait()

    def query_tile(i, carry):
        rows = tile_rows(i, LATENT_TILE)
        unit, _ = norm_parts(latents[rows, :])
        z_norm = (unit * z_gain[...] + z_shift[...]).astype(BF16)
        q[rows, :] = dot(z_norm, w_query[...], NN).astype(BF16)
        return carry

    lax.fori_loop(0, tiles, query_tile, 0)
    saved = [local.start(q, q_out)]
    got_own.wait()

    def block_logits(j):
        rows = tile_rows(j, block_rows)
        unit, _ = norm_parts(x_in[j], DOWN)
        x_norm = (unit * x_gain + x_shift).astype(BF16)
        k[rows, :] = dot(x_norm, w_key[...], TN).astype(BF16)
        v[rows, :] = dot(x_norm, w_value[...], TN).astype(BF16)
        vt[:, rows] = dot(w_value[...], x_norm, TN).astype(BF16)

        def logits_tile(i, carry):
            s = dot(k[rows, :], q[tile_rows(i, LATENT_TILE), :], NT)
            logits[i, rows, :] = s
            top = jnp.max(s, axis=DOWN, keepdims=True)
            for h in range(2):
                row = pl.ds(2 * i + h, 1)
                top_own[row, :] = jnp.maximum(top_own[row, :], top[:, h * LANES:(h + 1) * LANES])
            return carry

        lax.fori_loop(0, tiles, logits_tile, 0)

    block_logits(z)
    for d in HOPS[::-1]:
        got_x[d].wait_recv()
        block_logits(moved(me, 0, -d)[0])
    top_own[...] = jnp.ceil(top_own[...] * to_log2)
    saved += [local.start(k, k_out), local.start(v, v_out), local.start(x_in, x_out)]
    tops[owner] = top_own[...]
    top_copies = [copies.start(top_own, tops.at[owner], device) for _, device in plane_peers]

    def mix_tile(i, carry):
        top = row_pair(top_own, i)
        w = jnp.exp2(logits[i] * to_log2 - top)
        weight_sum = total(w)
        for h in range(2):
            sum_own[pl.ds(2 * i + h, 1), :] = weight_sum[:, h * LANES:(h + 1) * LANES]
        product = dot(vt[...], w.astype(BF16), NN)
        at_y, at_x = lax.div(i, 2), 2 * lax.rem(i, 2)
        for h in range(2):
            mixed[at_y, at_x + h] = product[:, h * LANES:(h + 1) * LANES]
        return carry

    lax.fori_loop(0, tiles, mix_tile, 0)
    for copy in top_copies:
        copy.wait_recv()
    top = functools.reduce(jnp.maximum, [tops[i] for i in range(PLANE)])
    top_all[...] = top
    factor = jnp.exp2(top_own[...] - top)
    scaled_sum = sum_own[...] * factor
    for i in range(PLANE):
        mixed[i // SIDE, i % SIDE] = mixed[i // SIDE, i % SIDE] * factor[i:i + 1, :]
        sum_parts[i] = jnp.broadcast_to(scaled_sum[i:i + 1, :], (8, LANES))

    streams = ((2, 1, pl.ds(0, half_v), sa, fa, pa1, ra2), (1, 2, pl.ds(half_v, half_v), sb, fb, pb1, rb2))

    def mixed_at(axis, place, part, cols):
        return ((part, place) if axis == 2 else (place, part)) + (cols,)

    first = []
    for axis, _, cols, side_in, _, _, _ in streams:
        far = moved(me, axis, 2)[axis]
        first.append([copies.start(mixed.at[mixed_at(axis, far, halves[w], cols)], side_in.at[w], chip(*moved(me, axis, d)))
                      for w, d in enumerate(ways)])
    sums[owner] = sum_parts[owner]
    sum_copies = [copies.start(sum_parts.at[other], sums.at[owner], device) for other, device in plane_peers]
    full = []
    for (axis, _, cols, side_in, full_in, _, _), arriving in zip(streams, first):
        started = []
        for w, d in enumerate(ways):
            peer = moved(me, axis, d)
            arriving[w].wait_recv()
            mixed[mixed_at(axis, peer[axis], halves[w], cols)] += side_in[w]
            started.append(copies.start(mixed.at[mixed_at(axis, peer[axis], slice(None), cols)], full_in.at[w], chip(*peer)))
        full.append(started)
    second = []
    for (axis, other, cols, _, full_in, part, slots), arriving in zip(streams, full):
        for copy in arriving:
            copy.wait_recv()
        for i in range(SIDE):
            part[i] = mixed[mixed_at(axis, me[axis], i, cols)] + full_in[0, i] + full_in[1, i]
        for d in HOPS:
            peer = moved(me, other, d)
            second.append(copies.start(part.at[peer[other]], slots.at[d - 1], chip(*peer)))
    for copy in sum_copies:
        copy.wait_recv()
    inv_sum = 1.0 / functools.reduce(lambda a, b: a + b, [sums[i] for i in range(PLANE)])
    for copy in second:
        copy.wait_recv()
    upper = pa1[y] + sum_slots(ra2)
    lower = pb1[x] + sum_slots(rb2)
    attn_t = jnp.concatenate([upper, lower], axis=DOWN) * inv_sum[0:1, :]

    attn_t_low = attn_t.astype(BF16)
    attn_low = attn_t.T.astype(BF16)
    z_mid = latents[tile_rows(owner, chunk), :] + dot(attn_low, w_out[...], NN)
    unit, rstd = norm_parts(z_mid)
    hidden_f32 = unit * m_gain[...] + m_shift[...]
    hidden = hidden_f32.astype(BF16)
    pre = dot(hidden, w_up[...], NN) + b_up[...]
    act_f32, slope = gelu_parts(pre)
    act = act_f32.astype(BF16)
    z_out[...] = z_mid + dot(act, w_down[...], NN) + b_down[...]

    got_d_out.wait()
    d_out_low = d_out[...]
    d_out_f32 = d_out_low.astype(F32)
    d_act = dot(d_out_low, w_down[...], NT).astype(BF16).astype(F32)
    d_pre = d_act * slope
    d_pre_low = d_pre.astype(BF16)
    d_hidden = dot(d_pre_low, w_up[...], NT).astype(BF16).astype(F32)
    d_mid = d_out_f32 + norm_pull(d_hidden, unit, rstd, m_gain[...])
    d_mid_low = d_mid.astype(BF16)
    d_attn = dot(d_mid_low, w_out[...], NT).astype(BF16).astype(F32)
    row_dot = total(d_attn.T * attn_t)

    half_r = LANES // 2
    d_attn_f32[y, x] = d_attn
    stats_f32[owner, 0:1, :] = row_dot
    stats_f32[owner, 1:2, :] = inv_sum[0:1, :]
    up, down = pl.ds(0, half_r), pl.ds(half_r, half_r)
    first = [[], []]
    for d in HOPS:
        first[0].append(copies.start(d_attn_f32.at[y, x, up], d_attn_f32.at[y, x, up], chip(*moved(me, 1, d))))
        first[1].append(copies.start(d_attn_f32.at[y, x, down], d_attn_f32.at[y, x, down], chip(*moved(me, 2, d))))
    stat_copies = [copies.start(stats_f32.at[owner], stats_f32.at[owner], device) for _, device in plane_peers]

    saved.append(local.start(z_out, z_all.at[z, y, x]))
    z_first = []
    for (lo, hi), (axis, _, _) in zip(STREAM_ROWS, STREAM_AXES):
        rows = pl.ds(lo, hi - lo)
        z_first += [copies.start(z_out.at[rows], z_all.at[z, y, x, rows], chip(*moved(me, axis, d))) for d in HOPS]

    d_mid_out[...] = d_mid
    w_grads[0] = dot(attn_t_low, d_mid_low, NN)
    w_grads[1] = dot(hidden_f32.T.astype(BF16), d_pre_low, NN)
    w_grads[2] = dot(act_f32.T.astype(BF16), d_out_low, NN)
    saved.append(local.start(w_grads, w_grads_out))
    for i, value in enumerate((d_hidden * unit, d_hidden, d_pre, d_out_f32)):
        vec_grads[i:i + 1, :] = total(value)
    vec_grads[4:8, :] = zeros(4, vec_grads.shape[1])

    gathered = []
    for axis, rows, arriving in ((2, up, first[0]), (1, down, first[1])):
        for copy in arriving:
            copy.wait_recv()
        ref = d_attn_f32.at[mixed_at(axis, me[axis], slice(None), rows)]
        gathered.append((axis, rows, [copies.start(ref, ref, chip(*moved(me, axis, d))) for d in ways]))
    last = []
    for axis, rows, arriving in gathered:
        for w, d in enumerate(ways):
            arriving[w].wait_recv()
            ref = d_attn_f32.at[mixed_at(axis, moved(me, axis, -d)[axis], halves[w], rows)]
            last.append(copies.start(ref, ref, chip(*moved(me, axis, d))))
    for copy in stat_copies + last + z_first:
        copy.wait_recv()
    copies.finish()
    stats_all[...] = stats_f32[...]
    for i in range(PLANE):
        d_attn_all[i] = d_attn_f32[i // SIDE, i % SIDE].astype(BF16)
    for copy in saved:
        copy.wait()


def forward_block(x_blocks, latents, d_out, *others, collective_id):
    latents_n, width = latents.shape
    _, channels, block_rows = x_blocks.shape
    elements = SIDE * block_rows
    chunk = latents_n // PLANE
    half = width // 2
    vmem = pl.BlockSpec(memory_space=pltpu.VMEM)
    hbm = pl.BlockSpec(memory_space=pl.ANY)
    n_copies = 90
    shape, wide = jax.ShapeDtypeStruct, pltpu.VMEM
    stat, slots = (PLANE, 8, LANES), (2, SIDE, half, LANES)
    saved = (((latents_n, width), BF16), ((elements, width), BF16), ((elements, width), BF16), (x_blocks.shape, F32))
    return pl.pallas_call(
        forward_kernel,
        out_shape=tuple(shape(*one) for one in saved) + (
            shape((SIDE, SIDE, SIDE, chunk, width), F32), shape((3, width, width), F32), shape((PLANE, chunk, width), BF16),
            shape(stat, F32), shape((PLANE, LANES), F32), shape((chunk, width), F32), shape((8, width), F32)),
        in_specs=[hbm] * 3 + [vmem] * len(others),
        out_specs=(hbm,) * 6 + (vmem,) * 5,
        scratch_shapes=[wide(*one) for one in saved] + [
            wide((latents_n, width), F32), wide((chunk, width), BF16), wide((chunk, width), F32), wide((3, width, width), F32),
            wide((width, elements), BF16), wide((latents_n // LATENT_TILE, elements, LATENT_TILE), F32),
            wide((SIDE, SIDE, width, LANES), F32),
            wide((PLANE, LANES), F32), wide((PLANE, PLANE, LANES), F32), wide((PLANE, LANES), F32), wide(stat, F32), wide(stat, F32),
            wide((2, SIDE // 2, half, LANES), F32), wide((2, SIDE // 2, half, LANES), F32), wide(slots, F32), wide(slots, F32),
            wide(slots[1:], F32), wide(slots[1:], F32), wide((3, half, LANES), F32), wide((3, half, LANES), F32),
            wide((SIDE, SIDE, chunk, width), F32), wide(stat, F32),
            pltpu.SemaphoreType.DMA((n_copies,)), pltpu.SemaphoreType.DMA((n_copies,)), pltpu.SemaphoreType.DMA((16,))],
        compiler_params=pltpu.CompilerParams(
            collective_id=collective_id, has_side_effects=True, vmem_limit_bytes=VMEM_LIMIT),
    )(x_blocks, latents, d_out, *others)


MLP_AT, LATENTS_AT, QUERY_AT, KEY_AT, VALUE_AT = 0, 3, 7, 8, 9
SLOT_GROUPS = ((0, 6), (6, 14), (14, 20))


def tile_place(matrix, t):
    return t // 2, 2 * matrix + t % 2


def backward_kernel(
        q_in, k_in, v_in, d_attn_in, z_in, stats, top, d_mid, vec_grads, x_gain_row, x_shift_row, z_gain, z_shift,
        w_query, w_key, w_value, w_grads, x_in, latents_in,
        z_all, d_inputs, d_lat_out, w_out_grads, kv_out, vec_out,
        q, k, v, d_attn, probs, d_logits, d_q, d_k, d_v, x_rows, x_norm, x_sums, d_x, d_x_in, latents, z_norm, vecs, g, core_in, *rest):
    n, per = len(STREAM_TILES), 8
    side_in = [rest[per * s:per * s + 2] for s in range(n)]
    full_in = [rest[per * s + 2:per * s + 4] for s in range(n)]
    recvs = [(None,) + rest[per * s + 4:per * s + 6] for s in range(n)]
    parts = [rest[per * s + 6:per * s + 8] for s in range(n)]
    send_sems, recv_sems, local_sems, half_free = rest[per * n:]
    me = chip_coords()
    z, y, x = me
    dp = lax.axis_index('dp')
    partner = {'dp': 1 - dp}
    qk_scale = q.shape[1] ** -0.5
    to_log2 = qk_scale * LOG2E
    width = q.shape[1]
    channels = x_rows.shape[1]
    halves = (slice(0, SIDE // 2), slice(SIDE // 2, SIDE))
    tiles = q.shape[0] // LATENT_TILE
    split = width // LANES
    chips = SIDE ** 3

    local = LocalCopies(local_sems)
    fetch = local.start
    got_first = [fetch(*pair) for pair in ((q_in, q), (k_in, k), (v_in, v), (d_attn_in, d_attn))]
    enter([partner] + [chip(*moved(me, axis, d)) for axis in range(3) for d in HOPS])
    copies = Copies(send_sems, recv_sems)

    ways = (1, -1)
    z_pending = []
    for (lo, hi), (first, second, _) in zip(STREAM_ROWS, STREAM_AXES):
        ref = z_all.at[at((first,), me) + (pl.ds(lo, hi - lo),)]
        z_pending.append([copies.start(ref, ref, chip(*moved(me, second, d))) for d in ways])
    got_x = fetch(x_in, x_rows)
    got_latents = fetch(latents_in, latents)
    got_w = []
    for i in range(3):
        for t in range(split):
            half, slot = tile_place(MLP_AT + i, t)
            got_w.append(fetch(w_grads.at[i, :, :, :, :, lanes(t)], g.at[half, :, :, :, slot]))
    x_norm[...] = jnp.zeros(x_norm.shape, BF16)
    x_gain, x_shift = as_column(x_gain_row), as_column(x_shift_row)
    for copy in got_first:
        copy.wait()

    def pair(ref, i, row):
        return jnp.concatenate([ref[2 * i + h, row:row + 1, :] for h in range(2)], axis=ACROSS)

    def attend_tile(i, carry):
        rows = tile_rows(i, LATENT_TILE)
        peak = row_pair(top, i)
        row_dot, inv_sum = pair(stats, i, 0), pair(stats, i, 1)
        p = jnp.exp2(dot(k[...], q[rows, :], NT) * to_log2 - peak) * inv_sum
        probs[:, rows] = p.astype(BF16)
        d_p = dot(v[...], d_attn[rows, :], NT)
        d_s = (p * (d_p - row_dot) * qk_scale).astype(BF16)
        d_logits[:, rows] = d_s
        d_q[rows, :] = dot(d_s, k[...], TN).astype(BF16)
        return carry

    lax.fori_loop(0, tiles // 2, attend_tile, 0)
    for s, (lo, hi) in enumerate(STREAM_ROWS):
        first, second, _ = STREAM_AXES[s]
        arrived, z_pending[s] = z_pending[s], []
        for copy, d, part in zip(arrived, ways, halves):
            copy.wait_recv()
            origin = on(second, moved(me, second, -d)[second])
            ref = z_all.at[at((), me, **on(first, part), **origin) + (pl.ds(lo, hi - lo),)]
            z_pending[s].append(copies.start(ref, ref, chip(*moved(me, second, d))))

    lax.fori_loop(tiles // 2, tiles, attend_tile, 0)

    for s, (lo, hi) in enumerate(STREAM_ROWS):
        for copy in z_pending[s]:
            copy.wait_recv()

    def z_piece(s, i, place):
        first, second, third = STREAM_AXES[s]
        lo, hi = STREAM_ROWS[s]
        return z_all.at[at((second,), me, **on(first, i), **on(third, place)) + (pl.ds(lo, hi - lo),)]

    ring = {}

    def start_ring(step):
        for s in range(n):
            third = STREAM_AXES[s][2]
            right, left = moved(me, third, 1), moved(me, third, -1)
            place = me[third]
            for way, peer, i in (('right', right, step), ('left', left, SIDE - 1 - step)):
                ref = z_piece(s, i, place)
                ring[s, way, step] = copies.start(ref, ref, chip(*peer))

    forwarded = []

    def forward_ring(step):
        for s in range(n):
            third = STREAM_AXES[s][2]
            right, left = moved(me, third, 1), moved(me, third, -1)
            for way, peer, origin, i in (('right', right, left, step), ('left', left, right, SIDE - 1 - step)):
                ring.pop((s, way, step)).wait_recv()
                ref = z_piece(s, i, origin[third])
                forwarded.append(copies.start(ref, ref, chip(*peer)))

    start_ring(0)
    start_ring(1)

    exchanged = []

    def exchange(group):
        lo, hi = SLOT_GROUPS[group]
        slots = (slice(None),) * 3 + (pl.ds(lo, hi - lo),)
        exchanged.append(copies.start(g.at[(1 - dp,) + slots], core_in.at[slots], partner))

    for copy in got_w:
        copy.wait()
    exchange(0)

    vecs[...] = zeros(*vecs.shape)
    x_sums[...] = zeros(*x_sums.shape)
    got_x.wait()

    def element_tile(i, carry):
        rows = tile_rows(i, x_rows.shape[-1])
        d_v_low = dot(probs[rows, :], d_attn[...], NN).astype(BF16)
        d_k_low = dot(d_logits[rows, :], q[...], NN).astype(BF16)
        d_v[rows, :] = d_v_low
        d_k[rows, :] = d_k_low
        unit, rstd = norm_parts(x_rows[i], DOWN)
        x_norm[0:channels, rows] = (unit * x_gain + x_shift).astype(BF16)
        d_normed = (dot(w_key[...], d_k_low, NT) + dot(w_value[...], d_v_low, NT)).astype(BF16).astype(F32)
        d_x[i] = norm_pull(d_normed, unit, rstd, x_gain, DOWN)
        for h, value in enumerate((d_normed * unit, d_normed)):
            x_sums[h] += sum(value[:, t * LANES:(t + 1) * LANES] for t in range(value.shape[1] // LANES))
        return carry

    lax.fori_loop(0, SIDE, element_tile, 0)
    x_pending = []
    for d in HOPS:
        peer = moved(me, 0, d)
        x_pending.append(copies.start(d_x.at[peer[0]], d_x_in.at[z], chip(*peer)))
    d_x_in[z] = d_x[z]

    for h in range(2):
        vecs[6 + h:7 + h, 0:channels] = total(x_sums[h].T)
    got_latents.wait()

    def latent_tile(i, carry):
        rows = tile_rows(i, LATENT_TILE)
        unit, rstd = norm_parts(latents[rows, :])
        z_norm[rows, :] = (unit * z_gain[...] + z_shift[...]).astype(BF16)
        d_normed = dot(d_q[rows, :], w_query[...], NT)
        for h, value in enumerate((d_normed * unit, d_normed)):
            vecs[4 + h:5 + h, :] += total(value)
        d_lat = norm_pull(d_normed, unit, rstd, z_gain[...])
        slab, part = lax.div(i, 2), lax.rem(i, 2)
        for t in range(split):
            block = d_lat[:, t * LANES:(t + 1) * LANES].reshape(2, SIDE, SIDE, 8, LANES)
            half, slot = tile_place(LATENTS_AT + slab, t)
            g[half, pl.ds(2 * part, 2), :, :, slot] = block
        return carry

    lax.fori_loop(0, tiles, latent_tile, 0)
    slab, part = y, x
    for t in range(split):
        half, slot = tile_place(LATENTS_AT + slab, t)
        g[half, part, :, :, slot] += d_mid[:, t * LANES:(t + 1) * LANES].reshape(SIDE, SIDE, 8, LANES)

    exchange(1)

    def put(value, matrix):
        for t in range(split):
            half, slot = tile_place(matrix, t)
            g[half, :, :, :, slot] = value[:, t * LANES:(t + 1) * LANES].reshape(SIDE, SIDE, SIDE, 8, LANES)

    put(dot(z_norm[...], d_q[...], TN), QUERY_AT)
    put(dot(x_norm[...], d_k[...], NN), KEY_AT)
    put(dot(x_norm[...], d_v[...], NN), VALUE_AT)
    vecs[0:4, :] = vec_grads[0:4, :]
    half, slot = tile_place(KEY_AT, 0)
    for i in range(vecs.shape[0]):
        for t in range(split):
            g[half, SIDE - 1, i // SIDE, i % SIDE, slot, t:t + 1, :] = vecs[i:i + 1, t * LANES:(t + 1) * LANES]
    exchange(2)
    start_ring(2)

    for copy, (lo, hi) in zip(exchanged, SLOT_GROUPS):
        copy.wait_recv()
        for i in range(SIDE):
            for j in range(SIDE):
                g[dp, i, j, :, lo:hi] += core_in[i, j, :, lo:hi]
    for copy in exchanged:
        copies.sent(copy)
    pl.semaphore_signal(half_free, inc=1, device_id=partner, device_id_type=MESH_ID)

    def along(s, place, part=None):
        axis = STREAM_AXES[s][0]
        others = tuple(a for a in range(3) if a != axis)
        index = at(others, me, **on(axis, place), **({} if part is None else on(others[0], part)))
        lo, hi = STREAM_TILES[s]
        return (dp,) + index + (slice(lo, hi),)

    def send(index, dst_index, dst, peer):
        return copies.start(g.at[index], g.at[dst_index] if dst is None else dst, chip(*peer))

    first = []
    for s in range(n):
        axis = STREAM_AXES[s][0]
        far = moved(me, axis, 2)[axis]
        first.append([send(along(s, far, halves[w]), None, side_in[s][w], moved(me, axis, d)) for w, d in enumerate(ways)])
    start_ring(3)
    pending = []
    for s in range(n):
        axis = STREAM_AXES[s][0]
        started = []
        for w, d in enumerate(ways):
            peer = moved(me, axis, d)
            first[s][w].wait_recv()
            g[along(s, peer[axis], halves[w])] += side_in[s][w][...]
            started.append(send(along(s, peer[axis]), None, full_in[s][w], peer))
        pending.append(started)
    for phase in range(1, 3):
        for s in range(n):
            for copy in pending[s]:
                copy.wait_recv()
            before, axis = STREAM_AXES[s][phase - 1], STREAM_AXES[s][phase]
            part = parts[s][phase - 1]
            left = [a for a in range(3) if a not in STREAM_AXES[s][:phase]]
            if phase == 1:
                for copy in first[s] + pending[s]:
                    copies.sent(copy)
                for i in range(SIDE):
                    part[i] = g[along(s, me[before], i)] + full_in[s][0][i] + full_in[s][1][i]
            else:
                for i in range(SIDE):
                    index = (me[before], i) if before < left[0] else (i, me[before])
                    part[i] = parts[s][0][index] + sum_slots(recvs[s][1], i)
            started = []
            for d in HOPS:
                peer = moved(me, axis, d)
                index = tuple(peer[axis] if a == axis else slice(None) for a in left)
                started.append(copies.start(part.at[index], recvs[s][phase].at[d - 1], chip(*peer)))
            pending[s] = started
        forward_ring(phase - 1)
    for s, (lo, hi) in enumerate(STREAM_TILES):
        for copy in pending[s]:
            copy.wait_recv()
        got, part = recvs[s][2], parts[s][1]
        axis = STREAM_AXES[s][2]
        g[(dp,) + me + (slice(lo, hi),)] = part[me[axis]] + sum_slots(got)
        ref = g.at[(dp,) + me + (pl.ds(lo, hi - lo),)]
        pending[s] = [copies.start(ref, ref, chip(*moved(me, axis, d))) for d in HOPS]
    core_copies = []
    pl.semaphore_wait(half_free, 1)
    for s, (lo, hi) in enumerate(STREAM_TILES):
        for copy in pending[s]:
            copy.wait_recv()
        _, axis, last = STREAM_AXES[s]
        ref = g.at[(dp,) + at((last,), me) + (pl.ds(lo, hi - lo),)]
        pending[s] = [copies.start(ref, ref, chip(*moved(me, axis, d))) for d in HOPS]

    def to_partner(index):
        core_copies.append(copies.start(g.at[index], g.at[index], partner))

    for s in range(n):
        for copy in pending[s]:
            copy.wait_recv()
        axis = STREAM_AXES[s][0]
        index = along(s, me[axis])
        pending[s] = [send(index, index, None, moved(me, axis, d)) for d in ways]
        to_partner(index)
    for copy in x_pending:
        copy.wait_recv()
    for i in range(SIDE):
        d_inputs[i] = d_x_in[i].astype(BF16)
    last = []
    for s in range(n):
        axis = STREAM_AXES[s][0]
        for w, d in enumerate(ways):
            pending[s][w].wait_recv()
            index = along(s, moved(me, axis, -d)[axis], halves[w])
            last.append((send(index, index, None, moved(me, axis, d)), s, w))
            to_partner(along(s, moved(me, axis, -d)[axis]))
    for copy, s, w in last:
        copy.wait_recv()
        axis = STREAM_AXES[s][0]
        to_partner(along(s, moved(me, axis, 2)[axis], halves[w]))
    for copy in core_copies:
        copy.wait_recv()

    outs = []
    for out, matrix, index in (
            [(d_lat_out, LATENTS_AT + i, i) for i in range(SIDE)] + [(w_out_grads, QUERY_AT, 0)]
            + [(w_out_grads, MLP_AT + i, i + 1) for i in range(3)] + [(kv_out, KEY_AT, 0), (kv_out, VALUE_AT, 1)]):
        for t in range(split):
            half, slot = tile_place(matrix, t)
            outs.append(fetch(g.at[half, :, :, :, slot], out.at[index, :, :, :, :, lanes(t)]))
    half, slot = tile_place(KEY_AT, 0)
    outs.append(fetch(g.at[half, SIDE - 1, :, :, slot], vec_out))
    for copy in forwarded + list(ring.values()):
        copy.wait_recv()
    copies.finish()
    for copy in outs:
        copy.wait()


def backward_block(q, k, v, d_attn, z_all, *others, collective_id):
    n_latents, width = q.shape
    x_rows, latents = others[-2:]
    elements, channels = k.shape[0], x_rows.shape[1]
    vmem = pl.BlockSpec(memory_space=pltpu.VMEM)
    hbm = pl.BlockSpec(memory_space=pl.ANY)
    cube, square = (SIDE, SIDE, SIDE), (SIDE, SIDE)
    shape, wide = jax.ShapeDtypeStruct, pltpu.VMEM
    block = x_rows.shape
    scratch = [
        wide(q.shape, BF16), wide(k.shape, BF16), wide(v.shape, BF16), wide(q.shape, BF16), wide((elements, n_latents), BF16), wide((elements, n_latents), BF16),
        wide((n_latents, width), BF16), wide((elements, width), BF16), wide((elements, width), BF16),
        wide(block, F32), wide((width, elements), BF16), wide((2, channels, LANES), F32), wide(block, F32), wide(block, F32),
        wide((n_latents, width), F32), wide((n_latents, width), BF16), wide((8, width), F32),
        wide((2,) + cube + (HALF_TILES, 8, LANES), F32), wide(cube + (HALF_TILES, 8, LANES), F32)]
    for lo, hi in STREAM_TILES:
        tiles = (hi - lo, 8, LANES)
        scratch += [wide((lead + tiles), F32) for lead in (
            (SIDE // 2, SIDE), (SIDE // 2, SIDE), square, square, (3, SIDE), (3,), square, (SIDE,))]
    n_copies = 160
    slab = cube + (8, width)
    return pl.pallas_call(
        backward_kernel,
        out_shape=(shape(z_all.shape, F32), shape(block, BF16), shape((4,) + slab, F32), shape((4,) + slab, F32),
                   shape((2,) + slab, F32), shape(square + (8, LANES), F32)),
        in_specs=[hbm] * 5 + [vmem] * (len(others) - 3) + [hbm] * 3,
        out_specs=(hbm, vmem, hbm, hbm, hbm, hbm),
        input_output_aliases={4: 0},
        scratch_shapes=scratch + [pltpu.SemaphoreType.DMA((n_copies,)), pltpu.SemaphoreType.DMA((n_copies,)),
                                  pltpu.SemaphoreType.DMA((64,)), pltpu.SemaphoreType.REGULAR],
        compiler_params=pltpu.CompilerParams(
            collective_id=collective_id, has_side_effects=True, vmem_limit_bytes=VMEM_LIMIT),
    )(q, k, v, d_attn, z_all, *others)


def finish_kernel(z_in, lat_in, w_in, kv_in, z_out, lat_out, wq, wo, wu, wd, wk, wv, z_buf, lat_buf, w_buf, sems):
    local = LocalCopies(sems)
    moves = []
    w_outs = (wq, wo, wu, wd)
    for i in range(z_buf.shape[0]):
        moves.append((local.start(z_in.at[i], z_buf.at[i]), z_buf.at[i], z_out.at[i]))
        if i < SIDE:
            moves.append((local.start(lat_in.at[i], lat_buf.at[i]), lat_buf.at[i], lat_out.at[i]))
            moves.append((local.start(w_in.at[i], w_buf.at[i]), w_buf.at[i], w_outs[i]))
    written = []
    for copy, src, dst in moves:
        copy.wait()
        written.append(local.start(src, dst))
    rows = wk.shape[0]
    wk[...] = kv_in[0, 0:rows, :]
    wv[...] = kv_in[1, 0:rows, :]
    for copy in written:
        copy.wait()


def finish(z_all, d_lat, w_sums, kv_sums, channels):
    vmem = pl.BlockSpec(memory_space=pltpu.VMEM)
    hbm = pl.BlockSpec(memory_space=pl.ANY)
    shape = jax.ShapeDtypeStruct
    width = w_sums.shape[-1]
    square = shape((width, width), F32)
    tall = shape((channels, width), F32)
    return pl.pallas_call(
        finish_kernel,
        out_shape=(shape(z_all.shape, F32), shape(d_lat.shape, F32), square, square, square, square, tall, tall),
        in_specs=[hbm] * 3 + [vmem],
        out_specs=(hbm,) * 6 + (vmem,) * 2,
        scratch_shapes=[pltpu.VMEM(z_all.shape, F32), pltpu.VMEM(d_lat.shape, F32), pltpu.VMEM(w_sums.shape, F32),
                        pltpu.SemaphoreType.DMA((64,))],
        compiler_params=pltpu.CompilerParams(vmem_limit_bytes=VMEM_LIMIT),
    )(z_all, d_lat, w_sums, kv_sums)


def solution(mesh):
    x_spec = P('dp', 'cp', None)
    row_spec = P('dp', None, None)
    vec_spec = P(None)
    mat_spec = P(None, None)
    in_specs = (x_spec, mat_spec, vec_spec, vec_spec, vec_spec, vec_spec, mat_spec, mat_spec, mat_spec, mat_spec,
                vec_spec, vec_spec, mat_spec, vec_spec, mat_spec, vec_spec, row_spec)
    out_specs = (row_spec, x_spec, mat_spec, vec_spec, vec_spec, vec_spec, vec_spec, mat_spec, mat_spec, mat_spec, mat_spec,
                 vec_spec, vec_spec, mat_spec, vec_spec, mat_spec, vec_spec)

    def local_step(inputs, latents, x_gain, x_shift, z_gain, z_shift, w_query, w_key, w_value, w_out, m_gain, m_shift, w_up, b_up, w_down, b_down, d_out):
        batch, elements, channels = inputs.shape
        n_latents, width = latents.shape
        chunk = n_latents // PLANE
        z, y, x = chip_coords()
        owner = y * SIDE + x

        x_blocks = inputs.transpose(0, 2, 1).astype(F32)
        row = lambda vec: vec.reshape(1, -1)
        norms = (row(x_gain), row(x_shift), row(z_gain), row(z_shift), w_query, w_key, w_value)
        q, k, v, x_in, z_all, w_grads, d_attn, stats, top, d_mid, vec_grads = forward_block(
            x_blocks, latents, d_out, *norms, w_out, w_up, w_down, row(m_gain), row(m_shift), row(b_up), row(b_down), collective_id=0)
        z_all, d_inputs, d_lat, w_sums, kv_sums, vec_sums = backward_block(
            q, k, v, d_attn.reshape(n_latents, width), z_all, stats, top, d_mid, vec_grads, *norms,
            w_grads.reshape(3, SIDE, SIDE, SIDE, 8, width), x_in, latents, collective_id=1)
        z_out, d_lat, d_w_query, d_w_out, d_w_up, d_w_down, d_w_key, d_w_value = finish(
            z_all.reshape(PLANE, -1, width), d_lat.reshape(SIDE, -1, width), w_sums.reshape(SIDE, width, width),
            kv_sums.reshape(2, width, width), channels)
        vec_sums = vec_sums[:2, :, :width // LANES].reshape(2 * SIDE, width)
        return (z_out.reshape(batch, n_latents, width), d_inputs.transpose(0, 2, 1), d_lat.reshape(n_latents, width),
                vec_sums[6, :channels], vec_sums[7, :channels], vec_sums[4], vec_sums[5],
                d_w_query, d_w_key, d_w_value, d_w_out, vec_sums[0], vec_sums[1],
                d_w_up, vec_sums[2], d_w_down, vec_sums[3])

    return jax.shard_map(local_step, mesh=mesh, in_specs=in_specs, out_specs=out_specs, check_vma=False)
```

```python
import functools
import math

import jax
import jax.numpy as jnp
from jax import lax
from jax.experimental import pallas as pl
from jax.experimental.pallas import tpu as pltpu
from jax.sharding import PartitionSpec as P

LN_EPS = 1e-5
BF16 = jnp.bfloat16
F32 = jnp.float32
MESH_ID = pl.DeviceIdType.MESH
SIDE = 4
PLANE = SIDE * SIDE
LANES = 128
LATENT_TILE = 256
RELAY_ROWS = 160
LOG2E = math.log2(math.e)
GELU_C = math.sqrt(2.0 / math.pi)
GELU_A = 0.044715
HALF_TILES = 20
STREAM_TILES = ((0, 7), (7, 14), (14, 20))
STREAM_ROWS = ((0, 32), (32, 80), (80, 128))
VMEM_LIMIT = 67043328
STREAM_AXES = ((2, 1, 0), (1, 0, 2), (0, 2, 1))


def contract(form, lhs, rhs):
    return jnp.einsum(form, lhs, rhs, preferred_element_type=F32)


def dot(lhs, rhs, dims):
    return lax.dot_general(lhs, rhs, (dims, ((), ())), preferred_element_type=F32)


NN = ((1,), (0,))
NT = ((1,), (1,))
TN = ((0,), (0,))
DOWN, ACROSS = 0, 1
HOPS = (2, 1, 3)
WAYS = (1, -1)


def mean(value, axis=ACROSS):
    return jnp.mean(value, axis=axis, keepdims=True)


def total(value, axis=DOWN):
    return jnp.sum(value, axis=axis, keepdims=True)


def zeros(*shape):
    return jnp.zeros(shape, F32)


def lanes(t):
    return pl.ds(t * LANES, LANES)


def tile_rows(i, size):
    return pl.ds(pl.multiple_of(i * size, size), size)


def norm_parts(value, axis=ACROSS):
    centred = value - mean(value, axis)
    rstd = lax.rsqrt(mean(centred * centred, axis) + LN_EPS)
    return centred * rstd, rstd


def norm_pull(d_normed, unit, rstd, gain, axis=ACROSS):
    d_unit = d_normed * gain
    return rstd * (d_unit - mean(d_unit, axis) - unit * mean(d_unit * unit, axis))


def as_columns(rows):
    turned = jnp.concatenate([rows[...], zeros(LANES - rows.shape[0], rows.shape[1])], axis=DOWN).T
    return turned[:, :1], turned[:, 1:2]


def row_pair(ref, i):
    return jnp.concatenate([ref[pl.ds(2 * i, 1), :], ref[pl.ds(2 * i + 1, 1), :]], axis=ACROSS)


def sum_slots(ref, *index):
    return ref[(0,) + index] + ref[(1,) + index] + ref[(2,) + index]


def gelu_parts(pre):
    tanh = jnp.tanh(GELU_C * (pre + GELU_A * pre * pre * pre))
    slope = 0.5 * (1.0 + tanh) + 0.5 * pre * (1.0 - tanh * tanh) * (GELU_C * (1.0 + 3.0 * GELU_A * pre * pre))
    return 0.5 * pre * (1.0 + tanh), slope


def chip_coords():
    cp = lax.axis_index('cp')
    return lax.div(cp, PLANE), lax.rem(lax.div(cp, SIDE), SIDE), lax.rem(cp, SIDE)


def chip(z, y, x):
    return {'cp': z * PLANE + y * SIDE + x}


def moved(coords, axis, offset):
    shifted = list(coords)
    shifted[axis] = lax.rem(coords[axis] + offset + SIDE, SIDE)
    return tuple(shifted)


def enter(peers):
    barrier = pltpu.get_barrier_semaphore()
    for peer in peers:
        pl.semaphore_signal(barrier, inc=1, device_id=peer, device_id_type=MESH_ID)
    pl.semaphore_wait(barrier, len(peers))


class Copies:
    def __init__(self, send_sems, recv_sems):
        self.send_sems, self.recv_sems, self.used, self.open = send_sems, recv_sems, 0, []

    def start(self, src, dst, peer):
        copy = pltpu.make_async_remote_copy(
            src_ref=src, dst_ref=dst, send_sem=self.send_sems.at[self.used], recv_sem=self.recv_sems.at[self.used],
            device_id=peer, device_id_type=MESH_ID)
        self.used += 1
        copy.start()
        self.open.append(copy)
        return copy

    def sent(self, copy):
        copy.wait_send()
        self.open = [other for other in self.open if other is not copy]

    def finish(self):
        for copy in self.open:
            copy.wait_send()


class LocalCopies:
    def __init__(self, sems):
        self.sems, self.used = sems, 0

    def start(self, src, dst):
        copy = pltpu.make_async_copy(src, dst, self.sems.at[self.used])
        self.used += 1
        copy.start()
        return copy


def at(free, coords, **other):
    index = []
    for axis, name in enumerate('zyx'):
        index.append(other[name] if name in other else (slice(None) if axis in free else coords[axis]))
    return tuple(index)


def on(axis, value):
    return {'zyx'[axis]: value}


class SwapZ:
    def __init__(self, copies, me, src, dst, relays):
        self.copies, self.me, self.dst, self.relays = copies, me, dst, relays
        far = moved(me, 0, 2)[0]
        cut = relays[0].shape[0]
        self.parts = (pl.ds(0, cut), pl.ds(cut, src.shape[1] - cut))
        self.halves = [copies.start(src.at[far, part], relay, chip(*moved(me, 0, d)))
                       for d, part, relay in zip(WAYS, self.parts, relays)]
        self.src = src

    def near(self):
        self.blocks = []
        for d in WAYS:
            peer = moved(self.me, 0, d)
            self.blocks.append(self.copies.start(self.src.at[peer[0]], self.dst.at[self.me[0]], chip(*peer)))

    def forward(self):
        self.rest = []
        for d, part, relay, half in zip(WAYS, self.parts, self.relays, self.halves):
            half.wait_recv()
            origin = moved(self.me, 0, -d)[0]
            self.rest.append(self.copies.start(relay, self.dst.at[origin, part], chip(*moved(self.me, 0, d))))


def forward_kernel(
        x_blocks, latents_in, d_out_in, x_affine, z_gain, z_shift, w_query, w_key, w_value,
        w_out_in, w_up_in, w_down_in, m_gain, m_shift, b_up, b_down,
        q_out, k_out, v_out, x_out, z_all, w_grads_out, d_attn_all, stats_all, top_all, d_mid_out, vec_grads,
        q, k, v, x_in, latents, d_out, z_out, w_grads, w_out, w_up, w_down, relay_up, relay_down,
        vt, logits, mixed, top_own, tops, sum_own, sum_parts, sums, sa, sb, fa, fb, pa1, pb1, ra2, rb2, d_attn_f32, stats_f32,
        send_sems, recv_sems, local_sems):
    me = chip_coords()
    relays = (relay_up, relay_down)
    local = LocalCopies(local_sems)
    got_latents = local.start(latents_in, latents)
    got_own = local.start(x_blocks.at[me[0]], x_in.at[me[0]])
    z, y, x = me
    owner = y * SIDE + x
    plane_peers = []
    for d in range(1, PLANE):
        other = lax.rem(owner + d, PLANE)
        plane_peers.append((other, chip(z, lax.div(other, SIDE), lax.rem(other, SIDE))))
    enter([device for _, device in plane_peers] + [chip(*moved(me, 0, d)) for d in HOPS])
    copies = Copies(send_sems, recv_sems)
    chunk = d_out.shape[0]
    got_w = [local.start(*pair) for pair in ((w_out_in, w_out), (w_up_in, w_up), (w_down_in, w_down))]
    got_d_out = local.start(d_out_in.at[z, pl.ds(owner * chunk, chunk), :], d_out)
    qk_scale = q.shape[1] ** -0.5
    to_log2 = qk_scale * LOG2E
    tiles = q.shape[0] // LATENT_TILE
    halves = (slice(0, SIDE // 2), slice(SIDE // 2, SIDE))
    half_v = vt.shape[0] // 2
    block_rows = x_blocks.shape[-1]

    swap = SwapZ(copies, me, x_blocks, x_in, relays)
    swap.near()
    top_own[...] = jnp.full(top_own.shape, -jnp.inf, F32)
    x_gain, x_shift = as_columns(x_affine)
    got_latents.wait()

    def query_tile(i, carry):
        rows = tile_rows(i, LATENT_TILE)
        unit, _ = norm_parts(latents[rows, :])
        z_norm = (unit * z_gain[...] + z_shift[...]).astype(BF16)
        q[rows, :] = dot(z_norm, w_query[...], NN).astype(BF16)
        return carry

    lax.fori_loop(0, tiles, query_tile, 0)
    saved = [local.start(q, q_out)]
    got_own.wait()

    def block_logits(j):
        rows = tile_rows(j, block_rows)
        unit, _ = norm_parts(x_in[j], DOWN)
        x_norm = (unit * x_gain + x_shift).astype(BF16)
        k[rows, :] = dot(x_norm, w_key[...], TN).astype(BF16)
        v[rows, :] = dot(x_norm, w_value[...], TN).astype(BF16)
        vt[:, rows] = dot(w_value[...], x_norm, TN).astype(BF16)

        def logits_tile(i, carry):
            s = dot(k[rows, :], q[tile_rows(i, LATENT_TILE), :], NT)
            logits[i, rows, :] = s
            top = jnp.max(s, axis=DOWN, keepdims=True)
            for h in range(2):
                row = pl.ds(2 * i + h, 1)
                top_own[row, :] = jnp.maximum(top_own[row, :], top[:, h * LANES:(h + 1) * LANES])
            return carry

        lax.fori_loop(0, tiles, logits_tile, 0)

    block_logits(z)
    swap.forward()
    for d, copy in zip(WAYS, swap.blocks):
        copy.wait_recv()
        block_logits(moved(me, 0, -d)[0])
    for copy in swap.rest:
        copy.wait_recv()
    block_logits(moved(me, 0, 2)[0])
    top_own[...] = jnp.ceil(top_own[...] * to_log2)
    saved += [local.start(k, k_out), local.start(v, v_out), local.start(x_in, x_out)]
    tops[owner] = top_own[...]
    top_copies = [copies.start(top_own, tops.at[owner], device) for _, device in plane_peers]

    def mix_tile(i, carry):
        top = row_pair(top_own, i)
        w = jnp.exp2(logits[i] * to_log2 - top)
        weight_sum = total(w)
        for h in range(2):
            sum_own[pl.ds(2 * i + h, 1), :] = weight_sum[:, h * LANES:(h + 1) * LANES]
        product = dot(vt[...], w.astype(BF16), NN)
        at_y, at_x = lax.div(i, 2), 2 * lax.rem(i, 2)
        for h in range(2):
            mixed[at_y, at_x + h] = product[:, h * LANES:(h + 1) * LANES]
        return carry

    lax.fori_loop(0, tiles, mix_tile, 0)
    for copy in top_copies:
        copy.wait_recv()
    top = functools.reduce(jnp.maximum, [tops[i] for i in range(PLANE)])
    top_all[...] = top
    factor = jnp.exp2(top_own[...] - top)
    scaled_sum = sum_own[...] * factor
    for i in range(PLANE):
        mixed[i // SIDE, i % SIDE] = mixed[i // SIDE, i % SIDE] * factor[i:i + 1, :]
        sum_parts[i] = jnp.broadcast_to(scaled_sum[i:i + 1, :], (8, LANES))

    streams = ((2, 1, pl.ds(0, half_v), sa, fa, pa1, ra2), (1, 2, pl.ds(half_v, half_v), sb, fb, pb1, rb2))

    def mixed_at(axis, place, part, cols):
        return ((part, place) if axis == 2 else (place, part)) + (cols,)

    first = []
    for axis, _, cols, side_in, _, _, _ in streams:
        far = moved(me, axis, 2)[axis]
        first.append([copies.start(mixed.at[mixed_at(axis, far, halves[w], cols)], side_in.at[w], chip(*moved(me, axis, d)))
                      for w, d in enumerate(WAYS)])
    sums[owner] = sum_parts[owner]
    sum_copies = [copies.start(sum_parts.at[other], sums.at[owner], device) for other, device in plane_peers]
    full = []
    for (axis, _, cols, side_in, full_in, _, _), arriving in zip(streams, first):
        started = []
        for w, d in enumerate(WAYS):
            peer = moved(me, axis, d)
            arriving[w].wait_recv()
            mixed[mixed_at(axis, peer[axis], halves[w], cols)] += side_in[w]
            started.append(copies.start(mixed.at[mixed_at(axis, peer[axis], slice(None), cols)], full_in.at[w], chip(*peer)))
        full.append(started)
    second = []
    for (axis, other, cols, _, full_in, part, slots), arriving in zip(streams, full):
        for copy in arriving:
            copy.wait_recv()
        for i in range(SIDE):
            part[i] = mixed[mixed_at(axis, me[axis], i, cols)] + full_in[0, i] + full_in[1, i]
        for d in HOPS:
            peer = moved(me, other, d)
            second.append(copies.start(part.at[peer[other]], slots.at[d - 1], chip(*peer)))
    for copy in sum_copies:
        copy.wait_recv()
    inv_sum = 1.0 / functools.reduce(lambda a, b: a + b, [sums[i] for i in range(PLANE)])
    for copy in second:
        copy.wait_recv()
    upper = pa1[y] + sum_slots(ra2)
    lower = pb1[x] + sum_slots(rb2)
    attn_t = jnp.concatenate([upper, lower], axis=DOWN) * inv_sum[0:1, :]

    attn_t_low = attn_t.astype(BF16)
    for copy in got_w:
        copy.wait()
    attn_low = attn_t.T.astype(BF16)
    z_mid = latents[tile_rows(owner, chunk), :] + dot(attn_low, w_out[...], NN)
    unit, rstd = norm_parts(z_mid)
    hidden_f32 = unit * m_gain[...] + m_shift[...]
    hidden = hidden_f32.astype(BF16)
    pre = dot(hidden, w_up[...], NN) + b_up[...]
    act_f32, slope = gelu_parts(pre)
    act = act_f32.astype(BF16)
    z_out[...] = z_mid + dot(act, w_down[...], NN) + b_down[...]

    got_d_out.wait()
    d_out_low = d_out[...]
    d_out_f32 = d_out_low.astype(F32)
    d_act = dot(d_out_low, w_down[...], NT).astype(BF16).astype(F32)
    d_pre = d_act * slope
    d_pre_low = d_pre.astype(BF16)
    d_hidden = dot(d_pre_low, w_up[...], NT).astype(BF16).astype(F32)
    d_mid = d_out_f32 + norm_pull(d_hidden, unit, rstd, m_gain[...])
    d_mid_low = d_mid.astype(BF16)
    d_attn = dot(d_mid_low, w_out[...], NT).astype(BF16).astype(F32)
    row_dot = total(d_attn.T * attn_t)

    half_r = LANES // 2
    d_attn_f32[y, x] = d_attn
    stats_f32[owner, 0:1, :] = row_dot
    stats_f32[owner, 1:2, :] = inv_sum[0:1, :]
    up, down = pl.ds(0, half_r), pl.ds(half_r, half_r)
    first = [[], []]
    for d in HOPS:
        first[0].append(copies.start(d_attn_f32.at[y, x, up], d_attn_f32.at[y, x, up], chip(*moved(me, 1, d))))
        first[1].append(copies.start(d_attn_f32.at[y, x, down], d_attn_f32.at[y, x, down], chip(*moved(me, 2, d))))
    stat_copies = [copies.start(stats_f32.at[owner], stats_f32.at[owner], device) for _, device in plane_peers]

    saved.append(local.start(z_out, z_all.at[z, y, x]))
    z_first = []
    for (lo, hi), (axis, _, _) in zip(STREAM_ROWS, STREAM_AXES):
        rows = pl.ds(lo, hi - lo)
        z_first += [copies.start(z_out.at[rows], z_all.at[z, y, x, rows], chip(*moved(me, axis, d))) for d in HOPS]

    d_mid_out[...] = d_mid
    w_grads[0] = dot(attn_t_low, d_mid_low, NN)
    w_grads[1] = dot(hidden_f32.T.astype(BF16), d_pre_low, NN)
    w_grads[2] = dot(act_f32.T.astype(BF16), d_out_low, NN)
    saved.append(local.start(w_grads, w_grads_out))
    for i, value in enumerate((d_hidden * unit, d_hidden, d_pre, d_out_f32)):
        vec_grads[i:i + 1, :] = total(value)
    vec_grads[4:8, :] = zeros(4, vec_grads.shape[1])

    gathered = []
    for axis, rows, arriving in ((2, up, first[0]), (1, down, first[1])):
        for copy in arriving:
            copy.wait_recv()
        ref = d_attn_f32.at[mixed_at(axis, me[axis], slice(None), rows)]
        gathered.append((axis, rows, [copies.start(ref, ref, chip(*moved(me, axis, d))) for d in WAYS]))
    last = []
    for axis, rows, arriving in gathered:
        for w, d in enumerate(WAYS):
            arriving[w].wait_recv()
            ref = d_attn_f32.at[mixed_at(axis, moved(me, axis, -d)[axis], halves[w], rows)]
            last.append(copies.start(ref, ref, chip(*moved(me, axis, d))))
    for copy in stat_copies + last + z_first:
        copy.wait_recv()
    copies.finish()
    stats_all[...] = stats_f32[...]
    for i in range(PLANE):
        d_attn_all[i] = d_attn_f32[i // SIDE, i % SIDE].astype(BF16)
    for copy in saved:
        copy.wait()


def forward_block(x_blocks, latents, d_out, *others, collective_id):
    latents_n, width = latents.shape
    _, channels, block_rows = x_blocks.shape
    elements = SIDE * block_rows
    chunk = latents_n // PLANE
    half = width // 2
    vmem = pl.BlockSpec(memory_space=pltpu.VMEM)
    hbm = pl.BlockSpec(memory_space=pl.ANY)
    n_copies = 90
    shape, wide = jax.ShapeDtypeStruct, pltpu.VMEM
    stat, slots = (PLANE, 8, LANES), (2, SIDE, half, LANES)
    saved = (((latents_n, width), BF16), ((elements, width), BF16), ((elements, width), BF16), (x_blocks.shape, F32))
    return pl.pallas_call(
        forward_kernel,
        out_shape=tuple(shape(*one) for one in saved) + (
            shape((SIDE, SIDE, SIDE, chunk, width), F32), shape((3, width, width), F32), shape((PLANE, chunk, width), BF16),
            shape(stat, F32), shape((PLANE, LANES), F32), shape((chunk, width), F32), shape((8, width), F32)),
        in_specs=[hbm] * 3 + [vmem] * (len(others) - 7) + [hbm] * 3 + [vmem] * 4,
        out_specs=(hbm,) * 6 + (vmem,) * 5,
        scratch_shapes=[wide(*one) for one in saved] + [
            wide((latents_n, width), F32), wide((chunk, width), BF16), wide((chunk, width), F32), wide((3, width, width), F32),
            wide((width, width), BF16), wide((width, width), BF16), wide((width, width), BF16),
            wide((RELAY_ROWS, block_rows), F32), wide((channels - RELAY_ROWS, block_rows), F32),
            wide((width, elements), BF16), wide((latents_n // LATENT_TILE, elements, LATENT_TILE), F32),
            wide((SIDE, SIDE, width, LANES), F32),
            wide((PLANE, LANES), F32), wide((PLANE, PLANE, LANES), F32), wide((PLANE, LANES), F32), wide(stat, F32), wide(stat, F32),
            wide((2, SIDE // 2, half, LANES), F32), wide((2, SIDE // 2, half, LANES), F32), wide(slots, F32), wide(slots, F32),
            wide(slots[1:], F32), wide(slots[1:], F32), wide((3, half, LANES), F32), wide((3, half, LANES), F32),
            wide((SIDE, SIDE, chunk, width), F32), wide(stat, F32),
            pltpu.SemaphoreType.DMA((n_copies,)), pltpu.SemaphoreType.DMA((n_copies,)), pltpu.SemaphoreType.DMA((16,))],
        compiler_params=pltpu.CompilerParams(
            collective_id=collective_id, has_side_effects=True, vmem_limit_bytes=VMEM_LIMIT),
    )(x_blocks, latents, d_out, *others)


MLP_AT, LATENTS_AT, QUERY_AT, KEY_AT, VALUE_AT = 0, 3, 7, 8, 9
SLOT_GROUPS = ((0, 6), (6, 14), (14, 20))


def tile_place(matrix, t):
    return t // 2, 2 * matrix + t % 2


def backward_kernel(
        q_in, k_in, v_in, d_attn_in, z_in, stats, top, d_mid, vec_grads, x_affine, z_gain, z_shift,
        w_query, w_key, w_value, w_grads, x_in, latents_in,
        z_all, d_inputs, d_lat_out, w_out_grads, kv_out, vec_out,
        q, k, v, d_attn, probs, d_logits, d_q, d_k, d_v, x_rows, x_norm, x_sums, d_x, d_x_in, relay_up, relay_down, latents, z_norm, vecs, g, core_in, *rest):
    relays = (relay_up, relay_down)
    n, per = len(STREAM_TILES), 8
    side_in = [rest[per * s:per * s + 2] for s in range(n)]
    full_in = [rest[per * s + 2:per * s + 4] for s in range(n)]
    recvs = [(None,) + rest[per * s + 4:per * s + 6] for s in range(n)]
    parts = [rest[per * s + 6:per * s + 8] for s in range(n)]
    send_sems, recv_sems, local_sems, half_free = rest[per * n:]
    me = chip_coords()
    z, y, x = me
    dp = lax.axis_index('dp')
    partner = {'dp': 1 - dp}
    qk_scale = q.shape[1] ** -0.5
    to_log2 = qk_scale * LOG2E
    width = q.shape[1]
    channels = x_rows.shape[1]
    halves = (slice(0, SIDE // 2), slice(SIDE // 2, SIDE))
    tiles = q.shape[0] // LATENT_TILE
    split = width // LANES
    chips = SIDE ** 3

    local = LocalCopies(local_sems)
    fetch = local.start
    got_first = [fetch(*pair) for pair in ((q_in, q), (k_in, k), (v_in, v), (d_attn_in, d_attn))]
    enter([partner] + [chip(*moved(me, axis, d)) for axis in range(3) for d in HOPS])
    copies = Copies(send_sems, recv_sems)

    z_pending = []
    for (lo, hi), (first, second, _) in zip(STREAM_ROWS, STREAM_AXES):
        ref = z_all.at[at((first,), me) + (pl.ds(lo, hi - lo),)]
        z_pending.append([copies.start(ref, ref, chip(*moved(me, second, d))) for d in WAYS])
    got_x = fetch(x_in, x_rows)
    got_latents = fetch(latents_in, latents)
    got_w = []
    for i in range(3):
        for t in range(split):
            half, slot = tile_place(MLP_AT + i, t)
            got_w.append(fetch(w_grads.at[i, :, :, :, :, lanes(t)], g.at[half, :, :, :, slot]))
    x_norm[...] = jnp.zeros(x_norm.shape, BF16)
    x_gain, x_shift = as_columns(x_affine)
    for copy in got_first:
        copy.wait()

    def pair(ref, i, row):
        return jnp.concatenate([ref[2 * i + h, row:row + 1, :] for h in range(2)], axis=ACROSS)

    def attend_tile(i, carry):
        rows = tile_rows(i, LATENT_TILE)
        peak = row_pair(top, i)
        row_dot, inv_sum = pair(stats, i, 0), pair(stats, i, 1)
        p = jnp.exp2(dot(k[...], q[rows, :], NT) * to_log2 - peak) * inv_sum
        probs[:, rows] = p.astype(BF16)
        d_p = dot(v[...], d_attn[rows, :], NT)
        d_s = (p * (d_p - row_dot) * qk_scale).astype(BF16)
        d_logits[:, rows] = d_s
        d_q[rows, :] = dot(d_s, k[...], TN).astype(BF16)
        return carry

    lax.fori_loop(0, tiles // 2, attend_tile, 0)
    for s, (lo, hi) in enumerate(STREAM_ROWS):
        first, second, _ = STREAM_AXES[s]
        arrived, z_pending[s] = z_pending[s], []
        for copy, d, part in zip(arrived, WAYS, halves):
            copy.wait_recv()
            origin = on(second, moved(me, second, -d)[second])
            ref = z_all.at[at((), me, **on(first, part), **origin) + (pl.ds(lo, hi - lo),)]
            z_pending[s].append(copies.start(ref, ref, chip(*moved(me, second, d))))

    lax.fori_loop(tiles // 2, tiles, attend_tile, 0)

    for s, (lo, hi) in enumerate(STREAM_ROWS):
        for copy in z_pending[s]:
            copy.wait_recv()

    def z_piece(s, i, place):
        first, second, third = STREAM_AXES[s]
        lo, hi = STREAM_ROWS[s]
        return z_all.at[at((second,), me, **on(first, i), **on(third, place)) + (pl.ds(lo, hi - lo),)]

    ring = {}

    def start_ring(step):
        for s in range(n):
            third = STREAM_AXES[s][2]
            right, left = moved(me, third, 1), moved(me, third, -1)
            place = me[third]
            for way, peer, i in (('right', right, step), ('left', left, SIDE - 1 - step)):
                ref = z_piece(s, i, place)
                ring[s, way, step] = copies.start(ref, ref, chip(*peer))

    forwarded = []

    def forward_ring(step):
        for s in range(n):
            third = STREAM_AXES[s][2]
            right, left = moved(me, third, 1), moved(me, third, -1)
            for way, peer, origin, i in (('right', right, left, step), ('left', left, right, SIDE - 1 - step)):
                ring.pop((s, way, step)).wait_recv()
                ref = z_piece(s, i, origin[third])
                forwarded.append(copies.start(ref, ref, chip(*peer)))

    start_ring(0)
    start_ring(1)

    exchanged = []

    def exchange(group):
        lo, hi = SLOT_GROUPS[group]
        slots = (slice(None),) * 3 + (pl.ds(lo, hi - lo),)
        exchanged.append(copies.start(g.at[(1 - dp,) + slots], core_in.at[slots], partner))

    for copy in got_w:
        copy.wait()
    exchange(0)

    vecs[...] = zeros(*vecs.shape)
    x_sums[...] = zeros(*x_sums.shape)
    got_x.wait()

    def element_tile(i, carry):
        rows = tile_rows(i, x_rows.shape[-1])
        d_v_low = dot(probs[rows, :], d_attn[...], NN).astype(BF16)
        d_k_low = dot(d_logits[rows, :], q[...], NN).astype(BF16)
        d_v[rows, :] = d_v_low
        d_k[rows, :] = d_k_low
        unit, rstd = norm_parts(x_rows[i], DOWN)
        x_norm[0:channels, rows] = (unit * x_gain + x_shift).astype(BF16)
        d_normed = (dot(w_key[...], d_k_low, NT) + dot(w_value[...], d_v_low, NT)).astype(BF16).astype(F32)
        d_x[i] = norm_pull(d_normed, unit, rstd, x_gain, DOWN)
        for h, value in enumerate((d_normed * unit, d_normed)):
            x_sums[h] += sum(value[:, t * LANES:(t + 1) * LANES] for t in range(value.shape[1] // LANES))
        return carry

    lax.fori_loop(0, SIDE, element_tile, 0)
    swap = SwapZ(copies, me, d_x, d_x_in, relays)
    d_x_in[z] = d_x[z]

    for h in range(2):
        vecs[6 + h:7 + h, 0:channels] = total(x_sums[h].T)
    got_latents.wait()

    def latent_tile(i, carry):
        rows = tile_rows(i, LATENT_TILE)
        unit, rstd = norm_parts(latents[rows, :])
        z_norm[rows, :] = (unit * z_gain[...] + z_shift[...]).astype(BF16)
        d_normed = dot(d_q[rows, :], w_query[...], NT)
        for h, value in enumerate((d_normed * unit, d_normed)):
            vecs[4 + h:5 + h, :] += total(value)
        d_lat = norm_pull(d_normed, unit, rstd, z_gain[...])
        slab, part = lax.div(i, 2), lax.rem(i, 2)
        for t in range(split):
            block = d_lat[:, t * LANES:(t + 1) * LANES].reshape(2, SIDE, SIDE, 8, LANES)
            half, slot = tile_place(LATENTS_AT + slab, t)
            g[half, pl.ds(2 * part, 2), :, :, slot] = block
        return carry

    lax.fori_loop(0, tiles, latent_tile, 0)
    slab, part = y, x
    for t in range(split):
        half, slot = tile_place(LATENTS_AT + slab, t)
        g[half, part, :, :, slot] += d_mid[:, t * LANES:(t + 1) * LANES].reshape(SIDE, SIDE, 8, LANES)

    exchange(1)

    def put(value, matrix):
        for t in range(split):
            half, slot = tile_place(matrix, t)
            g[half, :, :, :, slot] = value[:, t * LANES:(t + 1) * LANES].reshape(SIDE, SIDE, SIDE, 8, LANES)

    put(dot(z_norm[...], d_q[...], TN), QUERY_AT)
    put(dot(x_norm[...], d_k[...], NN), KEY_AT)
    put(dot(x_norm[...], d_v[...], NN), VALUE_AT)
    vecs[0:4, :] = vec_grads[0:4, :]
    half, slot = tile_place(KEY_AT, 0)
    for i in range(vecs.shape[0]):
        for t in range(split):
            g[half, SIDE - 1, i // SIDE, i % SIDE, slot, t:t + 1, :] = vecs[i:i + 1, t * LANES:(t + 1) * LANES]
    exchange(2)

    for copy, (lo, hi) in zip(exchanged, SLOT_GROUPS):
        copy.wait_recv()
        for i in range(SIDE):
            for j in range(SIDE):
                g[dp, i, j, :, lo:hi] += core_in[i, j, :, lo:hi]
    for copy in exchanged:
        copies.sent(copy)
    pl.semaphore_signal(half_free, inc=1, device_id=partner, device_id_type=MESH_ID)

    def along(s, place, part=None):
        axis = STREAM_AXES[s][0]
        others = tuple(a for a in range(3) if a != axis)
        index = at(others, me, **on(axis, place), **({} if part is None else on(others[0], part)))
        lo, hi = STREAM_TILES[s]
        return (dp,) + index + (slice(lo, hi),)

    def send(index, dst_index, dst, peer):
        return copies.start(g.at[index], g.at[dst_index] if dst is None else dst, chip(*peer))

    first = []
    for s in range(n):
        axis = STREAM_AXES[s][0]
        far = moved(me, axis, 2)[axis]
        first.append([send(along(s, far, halves[w]), None, side_in[s][w], moved(me, axis, d)) for w, d in enumerate(WAYS)])
    swap.near()
    start_ring(2)
    pending = []
    for s in range(n):
        axis = STREAM_AXES[s][0]
        started = []
        for w, d in enumerate(WAYS):
            peer = moved(me, axis, d)
            first[s][w].wait_recv()
            g[along(s, peer[axis], halves[w])] += side_in[s][w][...]
            started.append(send(along(s, peer[axis]), None, full_in[s][w], peer))
        pending.append(started)
    start_ring(3)
    for phase in range(1, 3):
        for s in range(n):
            for copy in pending[s]:
                copy.wait_recv()
            before, axis = STREAM_AXES[s][phase - 1], STREAM_AXES[s][phase]
            part = parts[s][phase - 1]
            left = [a for a in range(3) if a not in STREAM_AXES[s][:phase]]
            if phase == 1:
                for copy in first[s] + pending[s]:
                    copies.sent(copy)
                for i in range(SIDE):
                    part[i] = g[along(s, me[before], i)] + full_in[s][0][i] + full_in[s][1][i]
            else:
                for i in range(SIDE):
                    index = (me[before], i) if before < left[0] else (i, me[before])
                    part[i] = parts[s][0][index] + sum_slots(recvs[s][1], i)
            started = []
            for d in HOPS:
                peer = moved(me, axis, d)
                index = tuple(peer[axis] if a == axis else slice(None) for a in left)
                started.append(copies.start(part.at[index], recvs[s][phase].at[d - 1], chip(*peer)))
            pending[s] = started
        if phase == 1:
            swap.forward()
        forward_ring(phase - 1)
    for s, (lo, hi) in enumerate(STREAM_TILES):
        for copy in pending[s]:
            copy.wait_recv()
        got, part = recvs[s][2], parts[s][1]
        axis = STREAM_AXES[s][2]
        g[(dp,) + me + (slice(lo, hi),)] = part[me[axis]] + sum_slots(got)
        ref = g.at[(dp,) + me + (pl.ds(lo, hi - lo),)]
        pending[s] = [copies.start(ref, ref, chip(*moved(me, axis, d))) for d in HOPS]
    core_copies = []
    pl.semaphore_wait(half_free, 1)
    for s, (lo, hi) in enumerate(STREAM_TILES):
        for copy in pending[s]:
            copy.wait_recv()
        _, axis, last = STREAM_AXES[s]
        ref = g.at[(dp,) + at((last,), me) + (pl.ds(lo, hi - lo),)]
        pending[s] = [copies.start(ref, ref, chip(*moved(me, axis, d))) for d in HOPS]

    def to_partner(index):
        core_copies.append(copies.start(g.at[index], g.at[index], partner))

    for s in range(n):
        for copy in pending[s]:
            copy.wait_recv()
        axis = STREAM_AXES[s][0]
        index = along(s, me[axis])
        pending[s] = [send(index, index, None, moved(me, axis, d)) for d in WAYS]
        to_partner(index)
    for copy in swap.blocks + swap.rest:
        copy.wait_recv()
    for i in range(SIDE):
        d_inputs[i] = d_x_in[i].astype(BF16)
    last = []
    for s in range(n):
        axis = STREAM_AXES[s][0]
        for w, d in enumerate(WAYS):
            pending[s][w].wait_recv()
            index = along(s, moved(me, axis, -d)[axis], halves[w])
            last.append((send(index, index, None, moved(me, axis, d)), s, w))
            to_partner(along(s, moved(me, axis, -d)[axis]))
    for copy, s, w in last:
        copy.wait_recv()
        axis = STREAM_AXES[s][0]
        to_partner(along(s, moved(me, axis, 2)[axis], halves[w]))
    for copy in core_copies:
        copy.wait_recv()

    outs = []
    for out, matrix, index in (
            [(d_lat_out, LATENTS_AT + i, i) for i in range(SIDE)] + [(w_out_grads, QUERY_AT, 0)]
            + [(w_out_grads, MLP_AT + i, i + 1) for i in range(3)] + [(kv_out, KEY_AT, 0), (kv_out, VALUE_AT, 1)]):
        for t in range(split):
            half, slot = tile_place(matrix, t)
            outs.append(fetch(g.at[half, :, :, :, slot], out.at[index, :, :, :, :, lanes(t)]))
    half, slot = tile_place(KEY_AT, 0)
    outs.append(fetch(g.at[half, SIDE - 1, :, :, slot], vec_out))
    for copy in forwarded + list(ring.values()):
        copy.wait_recv()
    copies.finish()
    for copy in outs:
        copy.wait()


def backward_block(q, k, v, d_attn, z_all, *others, collective_id):
    n_latents, width = q.shape
    x_rows, latents = others[-2:]
    elements, channels = k.shape[0], x_rows.shape[1]
    vmem = pl.BlockSpec(memory_space=pltpu.VMEM)
    hbm = pl.BlockSpec(memory_space=pl.ANY)
    cube, square = (SIDE, SIDE, SIDE), (SIDE, SIDE)
    shape, wide = jax.ShapeDtypeStruct, pltpu.VMEM
    block = x_rows.shape
    scratch = [
        wide(q.shape, BF16), wide(k.shape, BF16), wide(v.shape, BF16), wide(q.shape, BF16), wide((elements, n_latents), BF16), wide((elements, n_latents), BF16),
        wide((n_latents, width), BF16), wide((elements, width), BF16), wide((elements, width), BF16),
        wide(block, F32), wide((width, elements), BF16), wide((2, channels, LANES), F32), wide(block, F32), wide(block, F32),
        wide((RELAY_ROWS, block[-1]), F32), wide((channels - RELAY_ROWS, block[-1]), F32),
        wide((n_latents, width), F32), wide((n_latents, width), BF16), wide((8, width), F32),
        wide((2,) + cube + (HALF_TILES, 8, LANES), F32), wide(cube + (HALF_TILES, 8, LANES), F32)]
    for lo, hi in STREAM_TILES:
        tiles = (hi - lo, 8, LANES)
        scratch += [wide((lead + tiles), F32) for lead in (
            (SIDE // 2, SIDE), (SIDE // 2, SIDE), square, square, (3, SIDE), (3,), square, (SIDE,))]
    n_copies = 160
    slab = cube + (8, width)
    return pl.pallas_call(
        backward_kernel,
        out_shape=(shape(z_all.shape, F32), shape(block, BF16), shape((4,) + slab, F32), shape((4,) + slab, F32),
                   shape((2,) + slab, F32), shape(square + (8, LANES), F32)),
        in_specs=[hbm] * 5 + [vmem] * (len(others) - 3) + [hbm] * 3,
        out_specs=(hbm, vmem, hbm, hbm, hbm, hbm),
        input_output_aliases={4: 0},
        scratch_shapes=scratch + [pltpu.SemaphoreType.DMA((n_copies,)), pltpu.SemaphoreType.DMA((n_copies,)),
                                  pltpu.SemaphoreType.DMA((64,)), pltpu.SemaphoreType.REGULAR],
        compiler_params=pltpu.CompilerParams(
            collective_id=collective_id, has_side_effects=True, vmem_limit_bytes=VMEM_LIMIT),
    )(q, k, v, d_attn, z_all, *others)


def finish_kernel(z_in, lat_in, w_in, kv_in, x_in, vec_in,
                  z_out, lat_out, wq, wo, wu, wd, wk, wv, x_out, *rest):
    vec_outs, (z_buf, lat_buf, w_buf, sems) = rest[:-SIDE], rest[-SIDE:]
    local = LocalCopies(sems)
    moves = []
    w_outs = (wq, wo, wu, wd)
    for i in range(z_buf.shape[0]):
        moves.append((local.start(z_in.at[i], z_buf.at[i]), z_buf.at[i], z_out.at[i]))
        if i < SIDE:
            moves.append((local.start(lat_in.at[i], lat_buf.at[i]), lat_buf.at[i], lat_out.at[i]))
            moves.append((local.start(w_in.at[i], w_buf.at[i]), w_buf.at[i], w_outs[i]))
    written = []
    for copy, src, dst in moves:
        copy.wait()
        written.append(local.start(src, dst))
    rows = wk.shape[0]
    for i in range(SIDE):
        x_out[:, i, :] = x_in[i]
    for i, out in enumerate(vec_outs):
        line = jnp.concatenate([vec_in[i // SIDE, i % SIDE, t:t + 1, :] for t in range(wk.shape[1] // LANES)], axis=ACROSS)
        out[...] = line[:, :out.shape[1]]
    wk[...] = kv_in[0, 0:rows, :]
    wv[...] = kv_in[1, 0:rows, :]
    for copy in written:
        copy.wait()


def finish(z_all, d_lat, w_sums, kv_sums, d_x, vec_sums):
    vmem = pl.BlockSpec(memory_space=pltpu.VMEM)
    hbm = pl.BlockSpec(memory_space=pl.ANY)
    shape = jax.ShapeDtypeStruct
    width = w_sums.shape[-1]
    square = shape((width, width), F32)
    _, channels, columns = d_x.shape
    tall = shape((channels, width), F32)
    line, x_line = shape((1, width), F32), shape((1, channels), F32)
    return pl.pallas_call(
        finish_kernel,
        out_shape=(shape(z_all.shape, F32), shape(d_lat.shape, F32), square, square, square, square, tall, tall,
                   shape((channels, SIDE, columns), BF16)) + (line,) * 6 + (x_line,) * 2,
        in_specs=[hbm] * 3 + [vmem] * 3,
        out_specs=(hbm,) * 6 + (vmem,) * 11,
        scratch_shapes=[pltpu.VMEM(z_all.shape, F32), pltpu.VMEM(d_lat.shape, F32), pltpu.VMEM(w_sums.shape, F32),
                        pltpu.SemaphoreType.DMA((64,))],
        compiler_params=pltpu.CompilerParams(vmem_limit_bytes=VMEM_LIMIT),
    )(z_all, d_lat, w_sums, kv_sums, d_x, vec_sums)


def solution(mesh):
    x_spec = P('dp', 'cp', None)
    row_spec = P('dp', None, None)
    vec_spec = P(None)
    mat_spec = P(None, None)
    in_specs = (x_spec, mat_spec, vec_spec, vec_spec, vec_spec, vec_spec, mat_spec, mat_spec, mat_spec, mat_spec,
                vec_spec, vec_spec, mat_spec, vec_spec, mat_spec, vec_spec, row_spec)
    out_specs = (row_spec, x_spec, mat_spec, vec_spec, vec_spec, vec_spec, vec_spec, mat_spec, mat_spec, mat_spec, mat_spec,
                 vec_spec, vec_spec, mat_spec, vec_spec, mat_spec, vec_spec)

    def local_step(inputs, latents, x_gain, x_shift, z_gain, z_shift, w_query, w_key, w_value, w_out, m_gain, m_shift, w_up, b_up, w_down, b_down, d_out):
        batch, elements, channels = inputs.shape
        n_latents, width = latents.shape
        chunk = n_latents // PLANE
        z, y, x = chip_coords()
        owner = y * SIDE + x

        x_blocks = inputs.transpose(0, 2, 1).astype(F32)
        row = lambda vec: vec.reshape(1, -1)
        norms = (jnp.stack([x_gain, x_shift]), row(z_gain), row(z_shift), w_query, w_key, w_value)
        q, k, v, x_in, z_all, w_grads, d_attn, stats, top, d_mid, vec_grads = forward_block(
            x_blocks, latents, d_out, *norms, w_out, w_up, w_down, row(m_gain), row(m_shift), row(b_up), row(b_down), collective_id=0)
        z_all, d_inputs, d_lat, w_sums, kv_sums, vec_sums = backward_block(
            q, k, v, d_attn.reshape(n_latents, width), z_all, stats, top, d_mid, vec_grads, *norms,
            w_grads.reshape(3, SIDE, SIDE, SIDE, 8, width), x_in, latents, collective_id=1)
        z_out, d_lat, d_w_query, d_w_out, d_w_up, d_w_down, d_w_key, d_w_value, d_inputs, *vectors = finish(
            z_all.reshape(PLANE, -1, width), d_lat.reshape(SIDE, -1, width), w_sums.reshape(SIDE, width, width),
            kv_sums.reshape(2, width, width), d_inputs, vec_sums)
        d_m_gain, d_m_shift, d_b_up, d_b_down, d_z_gain, d_z_shift, d_x_gain, d_x_shift = [v.reshape(-1) for v in vectors]
        return (z_out.reshape(batch, n_latents, width), d_inputs.transpose(1, 2, 0), d_lat.reshape(n_latents, width),
                d_x_gain, d_x_shift, d_z_gain, d_z_shift, d_w_query, d_w_key, d_w_value, d_w_out, d_m_gain, d_m_shift,
                d_w_up, d_b_up, d_w_down, d_b_down)

    return jax.shard_map(local_step, mesh=mesh, in_specs=in_specs, out_specs=out_specs, check_vma=False)
```

```python
import functools
import math

import jax
import jax.numpy as jnp
from jax import lax
from jax.experimental import pallas as pl
from jax.experimental.pallas import tpu as pltpu
from jax.sharding import PartitionSpec as P

LN_EPS = 1e-5
BF16 = jnp.bfloat16
F32 = jnp.float32
MESH_ID = pl.DeviceIdType.MESH
SIDE = 4
PLANE = SIDE * SIDE
LANES = 128
LATENT_TILE = 256
RELAY_ROWS = 160
LOG2E = math.log2(math.e)
GELU_C = math.sqrt(2.0 / math.pi)
GELU_A = 0.044715
HALF_TILES = 20
STREAM_TILES = ((0, 7), (7, 14), (14, 20))
STREAM_ROWS = ((0, 32), (32, 80), (80, 128))
VMEM_LIMIT = 67043328
STREAM_AXES = ((2, 1, 0), (1, 0, 2), (0, 2, 1))


def contract(form, lhs, rhs):
    return jnp.einsum(form, lhs, rhs, preferred_element_type=F32)


def dot(lhs, rhs, dims):
    return lax.dot_general(lhs, rhs, (dims, ((), ())), preferred_element_type=F32)


NN = ((1,), (0,))
NT = ((1,), (1,))
TN = ((0,), (0,))
DOWN, ACROSS = 0, 1
HOPS = (2, 1, 3)
WAYS = (1, -1)


def mean(value, axis=ACROSS):
    return jnp.mean(value, axis=axis, keepdims=True)


def total(value, axis=DOWN):
    return jnp.sum(value, axis=axis, keepdims=True)


def zeros(*shape):
    return jnp.zeros(shape, F32)


def lanes(t):
    return pl.ds(t * LANES, LANES)


def tile_rows(i, size):
    return pl.ds(pl.multiple_of(i * size, size), size)


def norm_parts(value, axis=ACROSS):
    centred = value - mean(value, axis)
    rstd = lax.rsqrt(mean(centred * centred, axis) + LN_EPS)
    return centred * rstd, rstd


def norm_pull(d_normed, unit, rstd, gain, axis=ACROSS):
    d_unit = d_normed * gain
    return rstd * (d_unit - mean(d_unit, axis) - unit * mean(d_unit * unit, axis))


def as_columns(rows):
    turned = jnp.concatenate([rows[...], zeros(LANES - rows.shape[0], rows.shape[1])], axis=DOWN).T
    return turned[:, :1], turned[:, 1:2]


def row_pair(ref, i):
    return jnp.concatenate([ref[pl.ds(2 * i, 1), :], ref[pl.ds(2 * i + 1, 1), :]], axis=ACROSS)


def sum_slots(ref, *index):
    return ref[(0,) + index] + ref[(1,) + index] + ref[(2,) + index]


def gelu_parts(pre):
    tanh = jnp.tanh(GELU_C * (pre + GELU_A * pre * pre * pre))
    slope = 0.5 * (1.0 + tanh) + 0.5 * pre * (1.0 - tanh * tanh) * (GELU_C * (1.0 + 3.0 * GELU_A * pre * pre))
    return 0.5 * pre * (1.0 + tanh), slope


def chip_coords():
    cp = lax.axis_index('cp')
    return lax.div(cp, PLANE), lax.rem(lax.div(cp, SIDE), SIDE), lax.rem(cp, SIDE)


def chip(z, y, x):
    return {'cp': z * PLANE + y * SIDE + x}


def moved(coords, axis, offset):
    shifted = list(coords)
    shifted[axis] = lax.rem(coords[axis] + offset + SIDE, SIDE)
    return tuple(shifted)


def enter(peers):
    barrier = pltpu.get_barrier_semaphore()
    for peer in peers:
        pl.semaphore_signal(barrier, inc=1, device_id=peer, device_id_type=MESH_ID)
    pl.semaphore_wait(barrier, len(peers))


class Copies:
    def __init__(self, send_sems, recv_sems):
        self.send_sems, self.recv_sems, self.used, self.open = send_sems, recv_sems, 0, []

    def start(self, src, dst, peer):
        copy = pltpu.make_async_remote_copy(
            src_ref=src, dst_ref=dst, send_sem=self.send_sems.at[self.used], recv_sem=self.recv_sems.at[self.used],
            device_id=peer, device_id_type=MESH_ID)
        self.used += 1
        copy.start()
        self.open.append(copy)
        return copy

    def sent(self, copy):
        copy.wait_send()
        self.open = [other for other in self.open if other is not copy]

    def finish(self):
        for copy in self.open:
            copy.wait_send()


class LocalCopies:
    def __init__(self, sems):
        self.sems, self.used = sems, 0

    def start(self, src, dst):
        copy = pltpu.make_async_copy(src, dst, self.sems.at[self.used])
        self.used += 1
        copy.start()
        return copy


def at(free, coords, **other):
    index = []
    for axis, name in enumerate('zyx'):
        index.append(other[name] if name in other else (slice(None) if axis in free else coords[axis]))
    return tuple(index)


def on(axis, value):
    return {'zyx'[axis]: value}


class SwapZ:
    def __init__(self, copies, me, src, dst, relays):
        self.copies, self.me, self.dst, self.relays = copies, me, dst, relays
        far = moved(me, 0, 2)[0]
        cut = relays[0].shape[0]
        self.parts = (pl.ds(0, cut), pl.ds(cut, src.shape[1] - cut))
        self.halves = [copies.start(src.at[far, part], relay, chip(*moved(me, 0, d)))
                       for d, part, relay in zip(WAYS, self.parts, relays)]
        self.src = src

    def near(self):
        self.blocks = []
        for d in WAYS:
            peer = moved(self.me, 0, d)
            self.blocks.append(self.copies.start(self.src.at[peer[0]], self.dst.at[self.me[0]], chip(*peer)))

    def forward(self):
        self.rest = []
        for d, part, relay, half in zip(WAYS, self.parts, self.relays, self.halves):
            half.wait_recv()
            origin = moved(self.me, 0, -d)[0]
            self.rest.append(self.copies.start(relay, self.dst.at[origin, part], chip(*moved(self.me, 0, d))))


def forward_kernel(
        x_blocks, latents_in, d_out_in, x_affine, z_gain, z_shift, w_query, w_key, w_value,
        w_out_in, w_up_in, w_down_in, m_gain, m_shift, b_up, b_down,
        q_out, k_out, v_out, x_out, z_all, w_grads_out, d_attn_all, stats_all, top_all, d_mid_out, vec_grads,
        q, k, v, x_in, latents, d_out, z_out, w_grads, w_out, w_up, w_down, relay_up, relay_down,
        vt, logits, mixed, top_own, tops, sum_own, sum_parts, sums, sa, sb, fa, fb, pa1, pb1, ra2, rb2, d_attn_f32, stats_f32,
        send_sems, recv_sems, local_sems):
    me = chip_coords()
    relays = (relay_up, relay_down)
    local = LocalCopies(local_sems)
    got_latents = local.start(latents_in, latents)
    got_own = local.start(x_blocks.at[me[0]], x_in.at[me[0]])
    z, y, x = me
    owner = y * SIDE + x
    plane_peers = []
    for d in range(1, PLANE):
        other = lax.rem(owner + d, PLANE)
        plane_peers.append((other, chip(z, lax.div(other, SIDE), lax.rem(other, SIDE))))
    enter([device for _, device in plane_peers] + [chip(*moved(me, 0, d)) for d in HOPS])
    copies = Copies(send_sems, recv_sems)
    chunk = d_out.shape[0]
    got_w = [local.start(*pair) for pair in ((w_out_in, w_out), (w_up_in, w_up), (w_down_in, w_down))]
    got_d_out = local.start(d_out_in.at[z, pl.ds(owner * chunk, chunk), :], d_out)
    qk_scale = q.shape[1] ** -0.5
    to_log2 = qk_scale * LOG2E
    tiles = q.shape[0] // LATENT_TILE
    halves = (slice(0, SIDE // 2), slice(SIDE // 2, SIDE))
    half_v = vt.shape[0] // 2
    block_rows = x_blocks.shape[-1]

    swap = SwapZ(copies, me, x_blocks, x_in, relays)
    swap.near()
    top_own[...] = jnp.full(top_own.shape, -jnp.inf, F32)
    x_gain, x_shift = as_columns(x_affine)
    got_latents.wait()

    def query_tile(i, carry):
        rows = tile_rows(i, LATENT_TILE)
        unit, _ = norm_parts(latents[rows, :])
        z_norm = (unit * z_gain[...] + z_shift[...]).astype(BF16)
        q[rows, :] = dot(z_norm, w_query[...], NN).astype(BF16)
        return carry

    lax.fori_loop(0, tiles, query_tile, 0)
    saved = [local.start(q, q_out)]
    got_own.wait()

    def block_logits(j):
        rows = tile_rows(j, block_rows)
        unit, _ = norm_parts(x_in[j], DOWN)
        x_norm = (unit * x_gain + x_shift).astype(BF16)
        k[rows, :] = dot(x_norm, w_key[...], TN).astype(BF16)
        v[rows, :] = dot(x_norm, w_value[...], TN).astype(BF16)
        vt[:, rows] = dot(w_value[...], x_norm, TN).astype(BF16)

        def logits_tile(i, carry):
            s = dot(k[rows, :], q[tile_rows(i, LATENT_TILE), :], NT)
            logits[i, rows, :] = s
            top = jnp.max(s, axis=DOWN, keepdims=True)
            for h in range(2):
                row = pl.ds(2 * i + h, 1)
                top_own[row, :] = jnp.maximum(top_own[row, :], top[:, h * LANES:(h + 1) * LANES])
            return carry

        lax.fori_loop(0, tiles, logits_tile, 0)

    block_logits(z)
    swap.forward()
    for d, copy in zip(WAYS, swap.blocks):
        copy.wait_recv()
        block_logits(moved(me, 0, -d)[0])
    for copy in swap.rest:
        copy.wait_recv()
    block_logits(moved(me, 0, 2)[0])
    top_own[...] = jnp.ceil(top_own[...] * to_log2)
    saved += [local.start(k, k_out), local.start(v, v_out), local.start(x_in, x_out)]
    tops[owner] = top_own[...]
    top_copies = [copies.start(top_own, tops.at[owner], device) for _, device in plane_peers]

    def mix_tile(i, carry):
        top = row_pair(top_own, i)
        w = jnp.exp2(logits[i] * to_log2 - top)
        weight_sum = total(w)
        for h in range(2):
            sum_own[pl.ds(2 * i + h, 1), :] = weight_sum[:, h * LANES:(h + 1) * LANES]
        product = dot(vt[...], w.astype(BF16), NN)
        at_y, at_x = lax.div(i, 2), 2 * lax.rem(i, 2)
        for h in range(2):
            mixed[at_y, at_x + h] = product[:, h * LANES:(h + 1) * LANES]
        return carry

    lax.fori_loop(0, tiles, mix_tile, 0)
    for copy in top_copies:
        copy.wait_recv()
    top = functools.reduce(jnp.maximum, [tops[i] for i in range(PLANE)])
    top_all[...] = top
    factor = jnp.exp2(top_own[...] - top)
    scaled_sum = sum_own[...] * factor
    for i in range(PLANE):
        mixed[i // SIDE, i % SIDE] = mixed[i // SIDE, i % SIDE] * factor[i:i + 1, :]
        sum_parts[i] = jnp.broadcast_to(scaled_sum[i:i + 1, :], (8, LANES))

    streams = ((2, 1, pl.ds(0, half_v), sa, fa, pa1, ra2), (1, 2, pl.ds(half_v, half_v), sb, fb, pb1, rb2))

    def mixed_at(axis, place, part, cols):
        return ((part, place) if axis == 2 else (place, part)) + (cols,)

    first = []
    for axis, _, cols, side_in, _, _, _ in streams:
        far = moved(me, axis, 2)[axis]
        first.append([copies.start(mixed.at[mixed_at(axis, far, halves[w], cols)], side_in.at[w], chip(*moved(me, axis, d)))
                      for w, d in enumerate(WAYS)])
    sums[owner] = sum_parts[owner]
    sum_copies = [copies.start(sum_parts.at[other], sums.at[owner], device) for other, device in plane_peers]
    full = []
    for (axis, _, cols, side_in, full_in, _, _), arriving in zip(streams, first):
        started = []
        for w, d in enumerate(WAYS):
            peer = moved(me, axis, d)
            arriving[w].wait_recv()
            mixed[mixed_at(axis, peer[axis], halves[w], cols)] += side_in[w]
            started.append(copies.start(mixed.at[mixed_at(axis, peer[axis], slice(None), cols)], full_in.at[w], chip(*peer)))
        full.append(started)
    second = []
    for (axis, other, cols, _, full_in, part, slots), arriving in zip(streams, full):
        for copy in arriving:
            copy.wait_recv()
        for i in range(SIDE):
            part[i] = mixed[mixed_at(axis, me[axis], i, cols)] + full_in[0, i] + full_in[1, i]
        for d in HOPS:
            peer = moved(me, other, d)
            second.append(copies.start(part.at[peer[other]], slots.at[d - 1], chip(*peer)))
    for copy in sum_copies:
        copy.wait_recv()
    inv_sum = 1.0 / functools.reduce(lambda a, b: a + b, [sums[i] for i in range(PLANE)])
    for copy in second:
        copy.wait_recv()
    upper = pa1[y] + sum_slots(ra2)
    lower = pb1[x] + sum_slots(rb2)
    attn_t = jnp.concatenate([upper, lower], axis=DOWN) * inv_sum[0:1, :]

    attn_t_low = attn_t.astype(BF16)
    for copy in got_w:
        copy.wait()
    attn_low = attn_t.T.astype(BF16)
    z_mid = latents[tile_rows(owner, chunk), :] + dot(attn_low, w_out[...], NN)
    unit, rstd = norm_parts(z_mid)
    hidden_f32 = unit * m_gain[...] + m_shift[...]
    hidden = hidden_f32.astype(BF16)
    pre = dot(hidden, w_up[...], NN) + b_up[...]
    act_f32, slope = gelu_parts(pre)
    act = act_f32.astype(BF16)
    z_out[...] = z_mid + dot(act, w_down[...], NN) + b_down[...]

    got_d_out.wait()
    d_out_low = d_out[...]
    d_out_f32 = d_out_low.astype(F32)
    d_act = dot(d_out_low, w_down[...], NT).astype(BF16).astype(F32)
    d_pre = d_act * slope
    d_pre_low = d_pre.astype(BF16)
    d_hidden = dot(d_pre_low, w_up[...], NT).astype(BF16).astype(F32)
    d_mid = d_out_f32 + norm_pull(d_hidden, unit, rstd, m_gain[...])
    d_mid_low = d_mid.astype(BF16)
    d_attn = dot(d_mid_low, w_out[...], NT).astype(BF16).astype(F32)
    row_dot = total(d_attn.T * attn_t)

    half_r = LANES // 2
    d_attn_f32[y, x] = d_attn
    stats_f32[owner, 0:1, :] = row_dot
    stats_f32[owner, 1:2, :] = inv_sum[0:1, :]
    up, down = pl.ds(0, half_r), pl.ds(half_r, half_r)
    first = [[], []]
    for d in HOPS:
        first[0].append(copies.start(d_attn_f32.at[y, x, up], d_attn_f32.at[y, x, up], chip(*moved(me, 1, d))))
        first[1].append(copies.start(d_attn_f32.at[y, x, down], d_attn_f32.at[y, x, down], chip(*moved(me, 2, d))))
    stat_copies = [copies.start(stats_f32.at[owner], stats_f32.at[owner], device) for _, device in plane_peers]

    saved.append(local.start(z_out, z_all.at[z, y, x]))
    z_first = []
    for (lo, hi), (axis, _, _) in zip(STREAM_ROWS, STREAM_AXES):
        rows = pl.ds(lo, hi - lo)
        z_first += [copies.start(z_out.at[rows], z_all.at[z, y, x, rows], chip(*moved(me, axis, d))) for d in HOPS]

    d_mid_out[...] = d_mid
    w_grads[0] = dot(attn_t_low, d_mid_low, NN)
    w_grads[1] = dot(hidden_f32.T.astype(BF16), d_pre_low, NN)
    w_grads[2] = dot(act_f32.T.astype(BF16), d_out_low, NN)
    saved.append(local.start(w_grads, w_grads_out))
    for i, value in enumerate((d_hidden * unit, d_hidden, d_pre, d_out_f32)):
        vec_grads[i:i + 1, :] = total(value)
    vec_grads[4:8, :] = zeros(4, vec_grads.shape[1])

    gathered = []
    for axis, rows, arriving in ((2, up, first[0]), (1, down, first[1])):
        for copy in arriving:
            copy.wait_recv()
        ref = d_attn_f32.at[mixed_at(axis, me[axis], slice(None), rows)]
        gathered.append((axis, rows, [copies.start(ref, ref, chip(*moved(me, axis, d))) for d in WAYS]))
    last = []
    for axis, rows, arriving in gathered:
        for w, d in enumerate(WAYS):
            arriving[w].wait_recv()
            ref = d_attn_f32.at[mixed_at(axis, moved(me, axis, -d)[axis], halves[w], rows)]
            last.append(copies.start(ref, ref, chip(*moved(me, axis, d))))
    for copy in stat_copies + last + z_first:
        copy.wait_recv()
    copies.finish()
    stats_all[...] = stats_f32[...]
    for i in range(PLANE):
        d_attn_all[i] = d_attn_f32[i // SIDE, i % SIDE].astype(BF16)
    for copy in saved:
        copy.wait()


def forward_block(x_blocks, latents, d_out, *others, collective_id):
    latents_n, width = latents.shape
    _, channels, block_rows = x_blocks.shape
    elements = SIDE * block_rows
    chunk = latents_n // PLANE
    half = width // 2
    vmem = pl.BlockSpec(memory_space=pltpu.VMEM)
    hbm = pl.BlockSpec(memory_space=pl.ANY)
    n_copies = 90
    shape, wide = jax.ShapeDtypeStruct, pltpu.VMEM
    stat, slots = (PLANE, 8, LANES), (2, SIDE, half, LANES)
    saved = (((latents_n, width), BF16), ((elements, width), BF16), ((elements, width), BF16), (x_blocks.shape, F32))
    return pl.pallas_call(
        forward_kernel,
        out_shape=tuple(shape(*one) for one in saved) + (
            shape((SIDE, SIDE, SIDE, chunk, width), F32), shape((3, width, width), F32), shape((PLANE, chunk, width), BF16),
            shape(stat, F32), shape((PLANE, LANES), F32), shape((chunk, width), F32), shape((8, width), F32)),
        in_specs=[hbm] * 3 + [vmem] * (len(others) - 7) + [hbm] * 3 + [vmem] * 4,
        out_specs=(hbm,) * 6 + (vmem,) * 5,
        scratch_shapes=[wide(*one) for one in saved] + [
            wide((latents_n, width), F32), wide((chunk, width), BF16), wide((chunk, width), F32), wide((3, width, width), F32),
            wide((width, width), BF16), wide((width, width), BF16), wide((width, width), BF16),
            wide((RELAY_ROWS, block_rows), F32), wide((channels - RELAY_ROWS, block_rows), F32),
            wide((width, elements), BF16), wide((latents_n // LATENT_TILE, elements, LATENT_TILE), F32),
            wide((SIDE, SIDE, width, LANES), F32),
            wide((PLANE, LANES), F32), wide((PLANE, PLANE, LANES), F32), wide((PLANE, LANES), F32), wide(stat, F32), wide(stat, F32),
            wide((2, SIDE // 2, half, LANES), F32), wide((2, SIDE // 2, half, LANES), F32), wide(slots, F32), wide(slots, F32),
            wide(slots[1:], F32), wide(slots[1:], F32), wide((3, half, LANES), F32), wide((3, half, LANES), F32),
            wide((SIDE, SIDE, chunk, width), F32), wide(stat, F32),
            pltpu.SemaphoreType.DMA((n_copies,)), pltpu.SemaphoreType.DMA((n_copies,)), pltpu.SemaphoreType.DMA((16,))],
        compiler_params=pltpu.CompilerParams(
            collective_id=collective_id, has_side_effects=True, vmem_limit_bytes=VMEM_LIMIT),
    )(x_blocks, latents, d_out, *others)


MLP_AT, LATENTS_AT, QUERY_AT, KEY_AT, VALUE_AT = 0, 3, 7, 8, 9
SLOT_GROUPS = ((0, 6), (6, 14), (14, 20))


def tile_place(matrix, t):
    return t // 2, 2 * matrix + t % 2


def backward_kernel(
        q_in, k_in, v_in, d_attn_in, z_in, stats, top, d_mid, vec_grads, x_affine, z_gain, z_shift,
        w_query, w_key, w_value, w_grads, x_in, latents_in,
        z_all, d_inputs, d_lat_out, w_out_grads, kv_out, vec_out,
        q, k, v, d_attn, probs, d_logits, d_q, d_k, d_v, x_rows, x_norm, x_sums, d_x, d_x_in, relay_up, relay_down, latents, z_norm, vecs, g, core_in, *rest):
    relays = (relay_up, relay_down)
    n, per = len(STREAM_TILES), 8
    side_in = [rest[per * s:per * s + 2] for s in range(n)]
    full_in = [rest[per * s + 2:per * s + 4] for s in range(n)]
    recvs = [(None,) + rest[per * s + 4:per * s + 6] for s in range(n)]
    parts = [rest[per * s + 6:per * s + 8] for s in range(n)]
    send_sems, recv_sems, local_sems, half_free = rest[per * n:]
    me = chip_coords()
    z, y, x = me
    dp = lax.axis_index('dp')
    partner = {'dp': 1 - dp}
    qk_scale = q.shape[1] ** -0.5
    to_log2 = qk_scale * LOG2E
    width = q.shape[1]
    channels = x_rows.shape[1]
    halves = (slice(0, SIDE // 2), slice(SIDE // 2, SIDE))
    tiles = q.shape[0] // LATENT_TILE
    split = width // LANES
    chips = SIDE ** 3

    local = LocalCopies(local_sems)
    fetch = local.start
    got_first = [fetch(*pair) for pair in ((q_in, q), (k_in, k), (v_in, v), (d_attn_in, d_attn))]
    enter([partner] + [chip(*moved(me, axis, d)) for axis in range(3) for d in HOPS])
    copies = Copies(send_sems, recv_sems)

    z_pending = []
    for (lo, hi), (first, second, _) in zip(STREAM_ROWS, STREAM_AXES):
        ref = z_all.at[at((first,), me) + (pl.ds(lo, hi - lo),)]
        z_pending.append([copies.start(ref, ref, chip(*moved(me, second, d))) for d in WAYS])
    got_x = fetch(x_in, x_rows)
    got_latents = fetch(latents_in, latents)
    got_w = []
    for i in range(3):
        for t in range(split):
            half, slot = tile_place(MLP_AT + i, t)
            got_w.append(fetch(w_grads.at[i, :, :, :, :, lanes(t)], g.at[half, :, :, :, slot]))
    x_norm[...] = jnp.zeros(x_norm.shape, BF16)
    x_gain, x_shift = as_columns(x_affine)
    for copy in got_first:
        copy.wait()

    def pair(ref, i, row):
        return jnp.concatenate([ref[2 * i + h, row:row + 1, :] for h in range(2)], axis=ACROSS)

    def attend_tile(i, carry):
        rows = tile_rows(i, LATENT_TILE)
        peak = row_pair(top, i)
        row_dot, inv_sum = pair(stats, i, 0), pair(stats, i, 1)
        p = jnp.exp2(dot(k[...], q[rows, :], NT) * to_log2 - peak) * inv_sum
        probs[:, rows] = p.astype(BF16)
        d_p = dot(v[...], d_attn[rows, :], NT)
        d_s = (p * (d_p - row_dot) * qk_scale).astype(BF16)
        d_logits[:, rows] = d_s
        d_q[rows, :] = dot(d_s, k[...], TN).astype(BF16)
        return carry

    lax.fori_loop(0, tiles // 2, attend_tile, 0)
    for s, (lo, hi) in enumerate(STREAM_ROWS):
        first, second, _ = STREAM_AXES[s]
        arrived, z_pending[s] = z_pending[s], []
        for copy, d, part in zip(arrived, WAYS, halves):
            copy.wait_recv()
            origin = on(second, moved(me, second, -d)[second])
            ref = z_all.at[at((), me, **on(first, part), **origin) + (pl.ds(lo, hi - lo),)]
            z_pending[s].append(copies.start(ref, ref, chip(*moved(me, second, d))))

    lax.fori_loop(tiles // 2, tiles, attend_tile, 0)

    for s, (lo, hi) in enumerate(STREAM_ROWS):
        for copy in z_pending[s]:
            copy.wait_recv()

    def z_piece(s, i, place):
        first, second, third = STREAM_AXES[s]
        lo, hi = STREAM_ROWS[s]
        return z_all.at[at((second,), me, **on(first, i), **on(third, place)) + (pl.ds(lo, hi - lo),)]

    ring = {}

    def start_ring(step):
        for s in range(n):
            third = STREAM_AXES[s][2]
            right, left = moved(me, third, 1), moved(me, third, -1)
            place = me[third]
            for way, peer, i in (('right', right, step), ('left', left, SIDE - 1 - step)):
                ref = z_piece(s, i, place)
                ring[s, way, step] = copies.start(ref, ref, chip(*peer))

    forwarded = []

    def forward_ring(step):
        for s in range(n):
            third = STREAM_AXES[s][2]
            right, left = moved(me, third, 1), moved(me, third, -1)
            for way, peer, origin, i in (('right', right, left, step), ('left', left, right, SIDE - 1 - step)):
                ring.pop((s, way, step)).wait_recv()
                ref = z_piece(s, i, origin[third])
                forwarded.append(copies.start(ref, ref, chip(*peer)))

    start_ring(0)
    start_ring(1)

    exchanged = []

    def exchange(group):
        lo, hi = SLOT_GROUPS[group]
        slots = (slice(None),) * 3 + (pl.ds(lo, hi - lo),)
        exchanged.append(copies.start(g.at[(1 - dp,) + slots], core_in.at[slots], partner))

    for copy in got_w:
        copy.wait()
    exchange(0)

    vecs[...] = zeros(*vecs.shape)
    x_sums[...] = zeros(*x_sums.shape)
    got_x.wait()

    def element_tile(i, carry):
        rows = tile_rows(i, x_rows.shape[-1])
        d_v_low = dot(probs[rows, :], d_attn[...], NN).astype(BF16)
        d_k_low = dot(d_logits[rows, :], q[...], NN).astype(BF16)
        d_v[rows, :] = d_v_low
        d_k[rows, :] = d_k_low
        unit, rstd = norm_parts(x_rows[i], DOWN)
        x_norm[0:channels, rows] = (unit * x_gain + x_shift).astype(BF16)
        d_normed = (dot(w_key[...], d_k_low, NT) + dot(w_value[...], d_v_low, NT)).astype(BF16).astype(F32)
        d_x[i] = norm_pull(d_normed, unit, rstd, x_gain, DOWN)
        for h, value in enumerate((d_normed * unit, d_normed)):
            x_sums[h] += sum(value[:, t * LANES:(t + 1) * LANES] for t in range(value.shape[1] // LANES))
        return carry

    lax.fori_loop(0, SIDE, element_tile, 0)
    swap = SwapZ(copies, me, d_x, d_x_in, relays)
    swap.near()
    d_x_in[z] = d_x[z]

    for h in range(2):
        vecs[6 + h:7 + h, 0:channels] = total(x_sums[h].T)
    got_latents.wait()

    def latent_tile(i, carry):
        rows = tile_rows(i, LATENT_TILE)
        unit, rstd = norm_parts(latents[rows, :])
        z_norm[rows, :] = (unit * z_gain[...] + z_shift[...]).astype(BF16)
        d_normed = dot(d_q[rows, :], w_query[...], NT)
        for h, value in enumerate((d_normed * unit, d_normed)):
            vecs[4 + h:5 + h, :] += total(value)
        d_lat = norm_pull(d_normed, unit, rstd, z_gain[...])
        slab, part = lax.div(i, 2), lax.rem(i, 2)
        for t in range(split):
            block = d_lat[:, t * LANES:(t + 1) * LANES].reshape(2, SIDE, SIDE, 8, LANES)
            half, slot = tile_place(LATENTS_AT + slab, t)
            g[half, pl.ds(2 * part, 2), :, :, slot] = block
        return carry

    lax.fori_loop(0, tiles, latent_tile, 0)
    slab, part = y, x
    for t in range(split):
        half, slot = tile_place(LATENTS_AT + slab, t)
        g[half, part, :, :, slot] += d_mid[:, t * LANES:(t + 1) * LANES].reshape(SIDE, SIDE, 8, LANES)

    exchange(1)

    def put(value, matrix):
        for t in range(split):
            half, slot = tile_place(matrix, t)
            g[half, :, :, :, slot] = value[:, t * LANES:(t + 1) * LANES].reshape(SIDE, SIDE, SIDE, 8, LANES)

    put(dot(z_norm[...], d_q[...], TN), QUERY_AT)
    put(dot(x_norm[...], d_k[...], NN), KEY_AT)
    put(dot(x_norm[...], d_v[...], NN), VALUE_AT)
    vecs[0:4, :] = vec_grads[0:4, :]
    half, slot = tile_place(KEY_AT, 0)
    for i in range(vecs.shape[0]):
        for t in range(split):
            g[half, SIDE - 1, i // SIDE, i % SIDE, slot, t:t + 1, :] = vecs[i:i + 1, t * LANES:(t + 1) * LANES]
    exchange(2)
    start_ring(2)

    for copy, (lo, hi) in zip(exchanged, SLOT_GROUPS):
        copy.wait_recv()
        for i in range(SIDE):
            for j in range(SIDE):
                g[dp, i, j, :, lo:hi] += core_in[i, j, :, lo:hi]
    for copy in exchanged:
        copies.sent(copy)
    pl.semaphore_signal(half_free, inc=1, device_id=partner, device_id_type=MESH_ID)

    def along(s, place, part=None):
        axis = STREAM_AXES[s][0]
        others = tuple(a for a in range(3) if a != axis)
        index = at(others, me, **on(axis, place), **({} if part is None else on(others[0], part)))
        lo, hi = STREAM_TILES[s]
        return (dp,) + index + (slice(lo, hi),)

    def send(index, dst_index, dst, peer):
        return copies.start(g.at[index], g.at[dst_index] if dst is None else dst, chip(*peer))

    first = []
    for s in range(n):
        axis = STREAM_AXES[s][0]
        far = moved(me, axis, 2)[axis]
        first.append([send(along(s, far, halves[w]), None, side_in[s][w], moved(me, axis, d)) for w, d in enumerate(WAYS)])
    start_ring(3)
    pending = []
    for s in range(n):
        axis = STREAM_AXES[s][0]
        started = []
        for w, d in enumerate(WAYS):
            peer = moved(me, axis, d)
            first[s][w].wait_recv()
            g[along(s, peer[axis], halves[w])] += side_in[s][w][...]
            started.append(send(along(s, peer[axis]), None, full_in[s][w], peer))
        pending.append(started)
    for phase in range(1, 3):
        for s in range(n):
            for copy in pending[s]:
                copy.wait_recv()
            before, axis = STREAM_AXES[s][phase - 1], STREAM_AXES[s][phase]
            part = parts[s][phase - 1]
            left = [a for a in range(3) if a not in STREAM_AXES[s][:phase]]
            if phase == 1:
                for copy in first[s] + pending[s]:
                    copies.sent(copy)
                for i in range(SIDE):
                    part[i] = g[along(s, me[before], i)] + full_in[s][0][i] + full_in[s][1][i]
            else:
                for i in range(SIDE):
                    index = (me[before], i) if before < left[0] else (i, me[before])
                    part[i] = parts[s][0][index] + sum_slots(recvs[s][1], i)
            started = []
            for d in HOPS:
                peer = moved(me, axis, d)
                index = tuple(peer[axis] if a == axis else slice(None) for a in left)
                started.append(copies.start(part.at[index], recvs[s][phase].at[d - 1], chip(*peer)))
            pending[s] = started
        if phase == 1:
            swap.forward()
        forward_ring(phase - 1)
    for s, (lo, hi) in enumerate(STREAM_TILES):
        for copy in pending[s]:
            copy.wait_recv()
        got, part = recvs[s][2], parts[s][1]
        axis = STREAM_AXES[s][2]
        g[(dp,) + me + (slice(lo, hi),)] = part[me[axis]] + sum_slots(got)
        ref = g.at[(dp,) + me + (pl.ds(lo, hi - lo),)]
        pending[s] = [copies.start(ref, ref, chip(*moved(me, axis, d))) for d in HOPS]
    core_copies = []
    pl.semaphore_wait(half_free, 1)
    for s, (lo, hi) in enumerate(STREAM_TILES):
        for copy in pending[s]:
            copy.wait_recv()
        _, axis, last = STREAM_AXES[s]
        ref = g.at[(dp,) + at((last,), me) + (pl.ds(lo, hi - lo),)]
        pending[s] = [copies.start(ref, ref, chip(*moved(me, axis, d))) for d in HOPS]

    def to_partner(index):
        core_copies.append(copies.start(g.at[index], g.at[index], partner))

    for s in range(n):
        for copy in pending[s]:
            copy.wait_recv()
        axis = STREAM_AXES[s][0]
        index = along(s, me[axis])
        pending[s] = [send(index, index, None, moved(me, axis, d)) for d in WAYS]
        to_partner(index)
    for copy in swap.blocks + swap.rest:
        copy.wait_recv()
    for i in range(SIDE):
        d_inputs[i] = d_x_in[i].astype(BF16)
    last = []
    for s in range(n):
        axis = STREAM_AXES[s][0]
        for w, d in enumerate(WAYS):
            pending[s][w].wait_recv()
            index = along(s, moved(me, axis, -d)[axis], halves[w])
            last.append((send(index, index, None, moved(me, axis, d)), s, w))
            to_partner(along(s, moved(me, axis, -d)[axis]))
    for copy, s, w in last:
        copy.wait_recv()
        axis = STREAM_AXES[s][0]
        to_partner(along(s, moved(me, axis, 2)[axis], halves[w]))
    for copy in core_copies:
        copy.wait_recv()

    outs = []
    for out, matrix, index in (
            [(d_lat_out, LATENTS_AT + i, i) for i in range(SIDE)] + [(w_out_grads, QUERY_AT, 0)]
            + [(w_out_grads, MLP_AT + i, i + 1) for i in range(3)] + [(kv_out, KEY_AT, 0), (kv_out, VALUE_AT, 1)]):
        for t in range(split):
            half, slot = tile_place(matrix, t)
            outs.append(fetch(g.at[half, :, :, :, slot], out.at[index, :, :, :, :, lanes(t)]))
    half, slot = tile_place(KEY_AT, 0)
    outs.append(fetch(g.at[half, SIDE - 1, :, :, slot], vec_out))
    for copy in forwarded + list(ring.values()):
        copy.wait_recv()
    copies.finish()
    for copy in outs:
        copy.wait()


def backward_block(q, k, v, d_attn, z_all, *others, collective_id):
    n_latents, width = q.shape
    x_rows, latents = others[-2:]
    elements, channels = k.shape[0], x_rows.shape[1]
    vmem = pl.BlockSpec(memory_space=pltpu.VMEM)
    hbm = pl.BlockSpec(memory_space=pl.ANY)
    cube, square = (SIDE, SIDE, SIDE), (SIDE, SIDE)
    shape, wide = jax.ShapeDtypeStruct, pltpu.VMEM
    block = x_rows.shape
    scratch = [
        wide(q.shape, BF16), wide(k.shape, BF16), wide(v.shape, BF16), wide(q.shape, BF16), wide((elements, n_latents), BF16), wide((elements, n_latents), BF16),
        wide((n_latents, width), BF16), wide((elements, width), BF16), wide((elements, width), BF16),
        wide(block, F32), wide((width, elements), BF16), wide((2, channels, LANES), F32), wide(block, F32), wide(block, F32),
        wide((RELAY_ROWS, block[-1]), F32), wide((channels - RELAY_ROWS, block[-1]), F32),
        wide((n_latents, width), F32), wide((n_latents, width), BF16), wide((8, width), F32),
        wide((2,) + cube + (HALF_TILES, 8, LANES), F32), wide(cube + (HALF_TILES, 8, LANES), F32)]
    for lo, hi in STREAM_TILES:
        tiles = (hi - lo, 8, LANES)
        scratch += [wide((lead + tiles), F32) for lead in (
            (SIDE // 2, SIDE), (SIDE // 2, SIDE), square, square, (3, SIDE), (3,), square, (SIDE,))]
    n_copies = 160
    slab = cube + (8, width)
    return pl.pallas_call(
        backward_kernel,
        out_shape=(shape(z_all.shape, F32), shape(block, BF16), shape((4,) + slab, F32), shape((4,) + slab, F32),
                   shape((2,) + slab, F32), shape(square + (8, LANES), F32)),
        in_specs=[hbm] * 5 + [vmem] * (len(others) - 3) + [hbm] * 3,
        out_specs=(hbm, vmem, hbm, hbm, hbm, hbm),
        input_output_aliases={4: 0},
        scratch_shapes=scratch + [pltpu.SemaphoreType.DMA((n_copies,)), pltpu.SemaphoreType.DMA((n_copies,)),
                                  pltpu.SemaphoreType.DMA((64,)), pltpu.SemaphoreType.REGULAR],
        compiler_params=pltpu.CompilerParams(
            collective_id=collective_id, has_side_effects=True, vmem_limit_bytes=VMEM_LIMIT),
    )(q, k, v, d_attn, z_all, *others)


def finish_kernel(z_in, lat_in, w_in, kv_in, x_in, vec_in,
                  z_out, lat_out, wq, wo, wu, wd, wk, wv, x_out, *rest):
    vec_outs, (z_buf, lat_buf, w_buf, sems) = rest[:-SIDE], rest[-SIDE:]
    local = LocalCopies(sems)
    moves = []
    w_outs = (wq, wo, wu, wd)
    for i in range(z_buf.shape[0]):
        moves.append((local.start(z_in.at[i], z_buf.at[i]), z_buf.at[i], z_out.at[i]))
        if i < SIDE:
            moves.append((local.start(lat_in.at[i], lat_buf.at[i]), lat_buf.at[i], lat_out.at[i]))
            moves.append((local.start(w_in.at[i], w_buf.at[i]), w_buf.at[i], w_outs[i]))
    written = []
    for copy, src, dst in moves:
        copy.wait()
        written.append(local.start(src, dst))
    rows = wk.shape[0]
    for i in range(SIDE):
        x_out[:, i, :] = x_in[i]
    for i, out in enumerate(vec_outs):
        line = jnp.concatenate([vec_in[i // SIDE, i % SIDE, t:t + 1, :] for t in range(wk.shape[1] // LANES)], axis=ACROSS)
        out[...] = line[:, :out.shape[1]]
    wk[...] = kv_in[0, 0:rows, :]
    wv[...] = kv_in[1, 0:rows, :]
    for copy in written:
        copy.wait()


def finish(z_all, d_lat, w_sums, kv_sums, d_x, vec_sums):
    vmem = pl.BlockSpec(memory_space=pltpu.VMEM)
    hbm = pl.BlockSpec(memory_space=pl.ANY)
    shape = jax.ShapeDtypeStruct
    width = w_sums.shape[-1]
    square = shape((width, width), F32)
    _, channels, columns = d_x.shape
    tall = shape((channels, width), F32)
    line, x_line = shape((1, width), F32), shape((1, channels), F32)
    return pl.pallas_call(
        finish_kernel,
        out_shape=(shape(z_all.shape, F32), shape(d_lat.shape, F32), square, square, square, square, tall, tall,
                   shape((channels, SIDE, columns), BF16)) + (line,) * 6 + (x_line,) * 2,
        in_specs=[hbm] * 3 + [vmem] * 3,
        out_specs=(hbm,) * 6 + (vmem,) * 11,
        scratch_shapes=[pltpu.VMEM(z_all.shape, F32), pltpu.VMEM(d_lat.shape, F32), pltpu.VMEM(w_sums.shape, F32),
                        pltpu.SemaphoreType.DMA((64,))],
        compiler_params=pltpu.CompilerParams(vmem_limit_bytes=VMEM_LIMIT),
    )(z_all, d_lat, w_sums, kv_sums, d_x, vec_sums)


def solution(mesh):
    x_spec = P('dp', 'cp', None)
    row_spec = P('dp', None, None)
    vec_spec = P(None)
    mat_spec = P(None, None)
    in_specs = (x_spec, mat_spec, vec_spec, vec_spec, vec_spec, vec_spec, mat_spec, mat_spec, mat_spec, mat_spec,
                vec_spec, vec_spec, mat_spec, vec_spec, mat_spec, vec_spec, row_spec)
    out_specs = (row_spec, x_spec, mat_spec, vec_spec, vec_spec, vec_spec, vec_spec, mat_spec, mat_spec, mat_spec, mat_spec,
                 vec_spec, vec_spec, mat_spec, vec_spec, mat_spec, vec_spec)

    def local_step(inputs, latents, x_gain, x_shift, z_gain, z_shift, w_query, w_key, w_value, w_out, m_gain, m_shift, w_up, b_up, w_down, b_down, d_out):
        batch, elements, channels = inputs.shape
        n_latents, width = latents.shape
        chunk = n_latents // PLANE
        z, y, x = chip_coords()
        owner = y * SIDE + x

        x_blocks = inputs.transpose(0, 2, 1).astype(F32)
        row = lambda vec: vec.reshape(1, -1)
        norms = (jnp.stack([x_gain, x_shift]), row(z_gain), row(z_shift), w_query, w_key, w_value)
        q, k, v, x_in, z_all, w_grads, d_attn, stats, top, d_mid, vec_grads = forward_block(
            x_blocks, latents, d_out, *norms, w_out, w_up, w_down, row(m_gain), row(m_shift), row(b_up), row(b_down), collective_id=0)
        z_all, d_inputs, d_lat, w_sums, kv_sums, vec_sums = backward_block(
            q, k, v, d_attn.reshape(n_latents, width), z_all, stats, top, d_mid, vec_grads, *norms,
            w_grads.reshape(3, SIDE, SIDE, SIDE, 8, width), x_in, latents, collective_id=1)
        z_out, d_lat, d_w_query, d_w_out, d_w_up, d_w_down, d_w_key, d_w_value, d_inputs, *vectors = finish(
            z_all.reshape(PLANE, -1, width), d_lat.reshape(SIDE, -1, width), w_sums.reshape(SIDE, width, width),
            kv_sums.reshape(2, width, width), d_inputs, vec_sums)
        d_m_gain, d_m_shift, d_b_up, d_b_down, d_z_gain, d_z_shift, d_x_gain, d_x_shift = [v.reshape(-1) for v in vectors]
        return (z_out.reshape(batch, n_latents, width), d_inputs.transpose(1, 2, 0), d_lat.reshape(n_latents, width),
                d_x_gain, d_x_shift, d_z_gain, d_z_shift, d_w_query, d_w_key, d_w_value, d_w_out, d_m_gain, d_m_shift,
                d_w_up, d_b_up, d_w_down, d_b_down)

    return jax.shard_map(local_step, mesh=mesh, in_specs=in_specs, out_specs=out_specs, check_vma=False)
```
